128 devices in a mesh: seq: 16 (over z, x), exp: 8 (over y, core).
Axes of the slice: x: 4, y: 4, z: 4, core: 2. Of those that a mesh axis runs over, the one named last changes fastest.
Arguments:
- tokens: bfloat16 [8, 2048, 4096], P('exp', 'seq'), may hold values from -6 to 6
- out_grad: bfloat16 [8, 2048, 4096], P('exp', 'seq'), may hold values from -0.59765625 to 0.59765625
- router_weight: bfloat16 [4096, 128], replicated, may hold values from -8 to 8
- gate_weight: bfloat16 [128, 4096, 768], P(('seq', 'exp')), may hold values from -0.09375 to 0.09375
- up_weight: bfloat16 [128, 4096, 768], P(('seq', 'exp')), may hold values from -0.09375 to 0.09375
- down_weight: bfloat16 [128, 768, 4096], P(('seq', 'exp')), may hold values from -0.21875 to 0.21875
- saved_gate: bfloat16 [128, 2048, 768], P(('seq', 'exp')), may hold values from -6 to 6
- saved_up: bfloat16 [128, 2048, 768], P(('seq', 'exp')), may hold values from -6 to 6
- expert_ids: int32 [8, 2048, 8], P('exp', 'seq'), may hold values from 0 to 127, as said below
- aux_weight: float32 [1], replicated, may hold values from 2 to 6
Outputs:
- token_grad: bfloat16 [8, 2048, 4096], P('exp', 'seq')
- combine_grad: float32 [8, 2048, 8], P('exp', 'seq')
- router_grad: float32 [4096, 128], P(('seq', 'exp'))
The draws below stay inside these ranges and needn't reach their ends.
Inputs may be any that keep to these rules, and one draw needn't show every extreme that they name: `expert_ids`: among the rows of one device (128 tokens) each expert is named at most 16 times, and some expert exactly 16 times; a token's 8 experts differ.
All inputs are finite; a program needn't handle non-finite values.
Results may differ from the reference program's by a relative error of at most 0.013.
Values may be sent and summed in bfloat16 or wider, within the bound.
A program may use at most 192 MiB of HBM per device.

```python
import math
import jax
import jax.numpy as jnp
from jax import lax

D = 4096
FF = 768
TOP = 8
TOK_DEV = 128
EXPERTS = 128
CAP = 16
SLOTS = 2048
GROUPS = 8
GROUP_TOK = 2048
N_SEQ = 16
N_EXP = 8


def draw_router_weight(key, part):
    drawn = jax.random.normal(key, (D, EXPERTS), jnp.float32) / math.sqrt(D)
    return jnp.clip(drawn, -8.0, 8.0).astype(jnp.bfloat16)


def draw_expert_ids(key, part):
    block_count = GROUPS * (GROUP_TOK // TOK_DEV)
    block_keys = jax.random.split(jax.random.fold_in(key, 11), block_count)
    full_count = TOK_DEV * TOP // CAP

    def one_block(block_key):
        order = jax.random.permutation(block_key, EXPERTS).astype(jnp.int32)
        picked = order[:full_count]
        items = jnp.repeat(picked, CAP, total_repeat_length=TOK_DEV * TOP)
        return items.reshape(TOP, TOK_DEV).T
    drawn = jax.vmap(one_block)(block_keys)
    return drawn.reshape(GROUPS, GROUP_TOK, TOP).astype(jnp.int32)


def shard_levels(rng, dims, pieces, low, largest):
    level, own = 1.0, jax.random.fold_in(rng, 6)
    for dim, parts in pieces:
        draws = jnp.exp(jax.random.uniform(jax.random.fold_in(own, dim), (parts,), jnp.float32, low / len(pieces), largest / len(pieces)))
        level = level * jnp.repeat(draws, dims[dim] // parts).reshape([-1 if axis == dim else 1 for axis in range(len(dims))])
    return level


def noise(stream_key, extent, deviation, most, cuts=(), kind=jnp.bfloat16):
    entries = jax.random.normal(stream_key, extent, jnp.float32) * deviation
    if len(cuts) > 0:
        entries = shard_levels(stream_key, extent, cuts, -0.22, 0.18) * entries
    return jnp.clip(entries, min=-most, max=most).astype(kind)


def setup_inputs(seed: int = 0) -> dict:
    seeds = jax.random.split(jax.random.key(seed), 11)
    return {
        "tokens": noise(seeds[0], (GROUPS, GROUP_TOK, D), 1.0, 6.0, ((0, 8), (1, 16))),
        "out_grad": noise(seeds[1], (GROUPS, GROUP_TOK, D), 0.1, 0.59765625, ((0, 8), (1, 16))),
        "router_weight": draw_router_weight(jax.random.fold_in(seeds[10], 71), 0),
        "gate_weight": noise(seeds[3], (EXPERTS, D, FF), D ** -0.5, 0.09375, ((0, 128),)),
        "up_weight": noise(seeds[4], (EXPERTS, D, FF), D ** -0.5, 0.09375, ((0, 128),)),
        "down_weight": noise(seeds[5], (EXPERTS, FF, D), FF ** -0.5, 0.21875, ((0, 128),)),
        "saved_gate": noise(seeds[6], (EXPERTS, SLOTS, FF), 1.0, 6.0, ((0, 128),)),
        "saved_up": noise(seeds[7], (EXPERTS, SLOTS, FF), 1.0, 6.0, ((0, 128),)),
        "expert_ids": draw_expert_ids(jax.random.fold_in(seeds[10], 71), 0),
        "aux_weight": jnp.clip(jax.random.uniform(seeds[9], (1,), jnp.float32, 2.0, 6.0), 2.0, 6.0),
    }


def expert_backward(grad_rows, gate_rows, w_gate, w_up, w_down, pre_gate, pre_up):
    upstream = jnp.einsum("rd,fd->rf", grad_rows, w_down, preferred_element_type=jnp.float32)
    first = pre_gate.astype(jnp.float32)
    second = pre_up.astype(jnp.float32)
    gate_sig = jax.nn.sigmoid(first)
    gate_act = first * gate_sig
    hidden = gate_act * second
    slot_combine = jnp.sum(upstream * hidden, axis=-1).astype(jnp.bfloat16)
    scaled = gate_rows.astype(jnp.float32)[:, None] * upstream
    grad_first = (scaled * second * gate_sig * (1.0 + first * (1.0 - gate_sig))).astype(jnp.bfloat16)
    grad_second = (scaled * gate_act).astype(jnp.bfloat16)
    back_rows = jnp.einsum("rf,df->rd", grad_first, w_gate, preferred_element_type=jnp.float32)
    back_rows = back_rows + jnp.einsum("rf,df->rd", grad_second, w_up, preferred_element_type=jnp.float32)
    return back_rows.astype(jnp.bfloat16), slot_combine


def reference(tokens, out_grad, router_weight, gate_weight, up_weight, down_weight, saved_gate, saved_up, expert_ids, aux_weight):
    groups, group_tok, model_width = tokens.shape
    experts = router_weight.shape[1]
    slot_count = saved_gate.shape[1]
    capacity = slot_count // (N_SEQ * N_EXP)
    total_rows = groups * group_tok
    inputs = tokens.reshape(total_rows, model_width)
    upstream_grad = out_grad.reshape(total_rows, model_width)
    chosen_ids = expert_ids.reshape(total_rows, TOP)
    logits = jnp.dot(inputs, router_weight, preferred_element_type=jnp.float32)
    router_probs = jax.nn.softmax(logits, axis=-1)
    chosen = jnp.take_along_axis(router_probs, chosen_ids, axis=1)
    chosen_sum = jnp.sum(chosen, axis=1, keepdims=True)
    gate_vals = chosen / chosen_sum
    onehot = (chosen_ids[:, :, None] == jnp.arange(experts, dtype=jnp.int32)[None, None, :]).astype(jnp.int32)
    blocks = total_rows // TOK_DEV
    per_block = onehot.reshape(blocks, TOK_DEV * TOP, experts)
    rank_before = jnp.cumsum(per_block, axis=1) - per_block
    slot_pos = jnp.sum(rank_before * per_block, axis=-1).reshape(total_rows, TOP)
    row_index = jnp.arange(total_rows, dtype=jnp.int32)
    group_of = row_index // group_tok
    within = row_index % group_tok
    source = (within // TOK_DEV) * N_EXP + group_of
    slot_index = (chosen_ids * slot_count + source[:, None] * capacity + slot_pos).astype(jnp.int32).reshape(-1)
    slot_token = jnp.full((experts * slot_count,), total_rows, jnp.int32).at[slot_index].set(jnp.repeat(row_index, TOP))
    gate_slots = jnp.zeros((experts * slot_count,), jnp.bfloat16).at[slot_index].set(gate_vals.reshape(-1).astype(jnp.bfloat16))
    grad_padded = jnp.concatenate([upstream_grad, jnp.zeros((1, model_width), jnp.bfloat16)], axis=0)

    def one_expert(accumulated, expert):
        own_rows = lax.dynamic_slice_in_dim(slot_token, expert * slot_count, slot_count)
        own_gates = lax.dynamic_slice_in_dim(gate_slots, expert * slot_count, slot_count)
        back_rows, slot_combine = expert_backward(grad_padded[own_rows], own_gates, gate_weight[expert], up_weight[expert], down_weight[expert], saved_gate[expert], saved_up[expert])
        accumulated = accumulated.at[own_rows].add(back_rows.astype(jnp.float32))
        return accumulated, slot_combine

    expert_sum, all_combine = lax.scan(one_expert, jnp.zeros((total_rows + 1, model_width), jnp.float32), jnp.arange(experts, dtype=jnp.int32))
    combine_grad = all_combine.reshape(-1)[slot_index].reshape(total_rows, TOP).astype(jnp.float32)
    prob_sel = (combine_grad - jnp.sum(gate_vals * combine_grad, axis=1, keepdims=True)) / chosen_sum
    prob_grad = jnp.einsum("tk,tke->te", prob_sel, onehot.astype(jnp.float32))
    chosen_count = jnp.sum(onehot, axis=1).astype(jnp.float32)
    seq_counts = jnp.sum(chosen_count.reshape(groups, group_tok, experts), axis=1)
    fraction = experts * seq_counts / (TOP * group_tok)
    prob_grad = prob_grad + aux_weight[0] * jnp.repeat(fraction, group_tok, axis=0)
    dlogits = router_probs * (prob_grad - jnp.sum(router_probs * prob_grad, axis=1, keepdims=True))
    logit_grad = dlogits.astype(jnp.bfloat16)
    token_grad = expert_sum[:total_rows] + jnp.einsum("te,de->td", logit_grad, router_weight, preferred_element_type=jnp.float32)
    router_grad = jnp.einsum("td,te->de", inputs, logit_grad, preferred_element_type=jnp.float32)
    return (token_grad.astype(jnp.bfloat16).reshape(groups, group_tok, model_width), combine_grad.reshape(groups, group_tok, TOP), router_grad)
```

```python
import functools

import jax
import jax.numpy as jnp
from jax import lax
from jax.experimental import pallas as pl
from jax.experimental.pallas import tpu as pltpu
from jax.sharding import Mesh
from jax.sharding import PartitionSpec as P

SEQ = ("seq_0", "seq_1")
EXP = ("exp_0", "exp_1")
AXES = ("seq_0", "seq_1", "exp_0", "exp_1")
MESH = pl.DeviceIdType.MESH
RING = 4
LANES = 128
ORDERS = ((0, 1, 2), (1, 2, 0), (2, 0, 1))


def column_parts(width):
    tiles = width // LANES
    sizes = [(tiles + 2 - p) // 3 * LANES for p in range(3)]
    starts = [0, sizes[0], sizes[0] + sizes[1]]
    return list(zip(starts, sizes))


class Wires:
    def __init__(self, send_sems, recv_sems):
        self.send_sems, self.recv_sems = send_sems, recv_sems
        self.sent, self.names = [], {}

    def slot(self, name):
        return self.recv_sems.at[self.names.setdefault(name, len(self.names))]

    def send(self, src, dst, device, name):
        copy = pltpu.make_async_remote_copy(
            src, dst, self.send_sems.at[len(self.sent)], self.slot(name), device, MESH
        )
        copy.start()
        self.sent.append(copy)

    def arrived(self, ref, name, device):
        pltpu.make_async_remote_copy(
            ref, ref, self.send_sems.at[0], self.slot(name), device, MESH
        ).wait_recv()

    def drain(self):
        for copy in self.sent:
            copy.wait_send()


class Place:
    def __init__(self):
        self.at = [lax.axis_index(name) for name in AXES]
        self.core = self.at[3]

    def along(self, axis, step):
        return lax.rem(self.at[axis] + (step + RING), RING)

    def near(self, axis, step, other_core=0):
        coords = list(self.at)
        coords[axis] = self.along(axis, step)
        if other_core:
            coords[3] = 1 - self.core
        return tuple(coords)

    def partner(self):
        return (self.at[0], self.at[1], self.at[2], 1 - self.core)

    def greet(self):
        barrier = pltpu.get_barrier_semaphore()
        peers = [self.partner()]
        for axis in range(3):
            for step in (1, -1):
                for other in (0, 1):
                    peers.append(self.near(axis, step, other))
        for peer in peers:
            pl.semaphore_signal(barrier, inc=1, device_id=peer, device_id_type=MESH)
        pl.semaphore_wait(barrier, len(peers))


def slots_of(ref, order, b_index, s_index, c_index, start, size):
    a, b, s = order
    where = [None] * 3
    where[a], where[b], where[s] = slice(None), b_index, s_index
    return ref.at[where[0], where[1], where[2], c_index, :, pl.ds(start, size)]


def line_row(table, line):
    rows = table.astype(jnp.float32)
    index = lax.broadcasted_iota(jnp.int32, rows.shape, 0)
    return jnp.sum(jnp.where(index == line, rows, 0.0), axis=0, keepdims=True)


def dispatch_kernel(
    parts, grad, maps, slots, maps_out, g0, g1, g2, o0, o1, o2, l0, l1, l2, seen, ss, rs, ls
):
    held, outgoing, relay = (g0, g1, g2), (o0, o1, o2), (l0, l1, l2)
    here = Place()
    wires = Wires(ss, rs)
    tokens = grad.shape[0]
    half = tokens // 2
    local = []

    def keep(src, dst):
        copy = pltpu.make_async_copy(src, dst, ls.at[len(local)])
        copy.start()
        local.append(copy)

    for p, (a, b, s) in enumerate(ORDERS):
        start, size = parts[p]
        keep(grad.at[:, pl.ds(start, size)], held[p].at[here.at[b], here.at[a]])
        keep(maps.at[p], seen.at[p, here.at[b], here.at[a]])
    here.greet()
    for copy in local:
        copy.wait()

    def pass_on(p, k, step):
        a, b, s = ORDERS[p]
        block = held[p].at[here.at[b], here.along(a, step)]
        wires.send(block, block, here.near(b, 1), (p, "m2", 1, k))
        wires.send(block, block, here.near(b, -1), (p, "m2", -1, k))

    def relay_on(p, k, step):
        a, b, s = ORDERS[p]
        for way, rows in ((1, pl.ds(0, half)), (-1, pl.ds(half, half))):
            block = held[p].at[here.along(b, -way), here.along(a, step)]
            wires.arrived(block, (p, "m2", way, k), here.near(b, -way))
            piece = held[p].at[here.along(b, -way), here.along(a, step), rows]
            wires.send(piece, piece, here.near(b, way), (p, "m2far", way, k))

    def far_in(p, k, step):
        a, b, s = ORDERS[p]
        for way, rows in ((1, pl.ds(0, half)), (-1, pl.ds(half, half))):
            piece = held[p].at[here.along(b, 2), here.along(a, step), rows]
            wires.arrived(piece, (p, "m2far", way, k), here.near(b, -way))

    for p, (a, b, s) in enumerate(ORDERS):
        table = seen.at[p, here.at[b], here.at[a]]
        block = held[p].at[here.at[b], here.at[a]]
        for way in (1, -1):
            wires.send(table, table, here.near(a, way), (p, "t1", way))
        for way in (1, -1):
            wires.send(block, block, here.near(a, way), (p, "m1", way))
    for p in range(3):
        pass_on(p, 0, 0)
    for p, (a, b, s) in enumerate(ORDERS):
        table = seen.at[p, here.at[b], here.along(a, -1)]
        wires.arrived(table, (p, "t1", 1), here.near(a, -1))
        wires.send(table, table, here.near(a, 1), (p, "t1far"))
        wires.arrived(
            seen.at[p, here.at[b], here.along(a, 1)], (p, "t1", -1), here.near(a, 1)
        )
    for p, (a, b, s) in enumerate(ORDERS):
        for way, rows in ((1, pl.ds(0, half)), (-1, pl.ds(half, half))):
            block = held[p].at[here.at[b], here.along(a, -way)]
            wires.arrived(block, (p, "m1", way), here.near(a, -way))
            piece = held[p].at[here.at[b], here.along(a, -way), rows]
            wires.send(piece, piece, here.near(a, way), (p, "m1far", way))
    for p, (a, b, s) in enumerate(ORDERS):
        wires.arrived(
            seen.at[p, here.at[b], here.along(a, 2)], (p, "t1far"), here.near(a, -1)
        )
        table = seen.at[p, here.at[b]]
        for way in (1, -1):
            wires.send(table, table, here.near(b, way), (p, "t2", way))
    for p in range(3):
        pass_on(p, 1, -1)
        pass_on(p, 2, 1)
    for p, (a, b, s) in enumerate(ORDERS):
        table = seen.at[p, here.along(b, -1)]
        wires.arrived(table, (p, "t2", 1), here.near(b, -1))
        wires.send(table, table, here.near(b, 1), (p, "t2far"))
        wires.arrived(seen.at[p, here.along(b, 1)], (p, "t2", -1), here.near(b, 1))
    for p, (a, b, s) in enumerate(ORDERS):
        for way, rows in ((1, pl.ds(0, half)), (-1, pl.ds(half, half))):
            piece = held[p].at[here.at[b], here.along(a, 2), rows]
            wires.arrived(piece, (p, "m1far", way), here.near(a, -way))
        pass_on(p, 3, 2)

    def select(p, k, b_step):
        a, b, s = ORDERS[p]
        b_index = here.along(b, b_step)
        line = here.at[b] * RING + here.at[a]
        size = parts[p][1]

        def one(a_index, carry):
            token_of = line_row(seen[p, b_index, a_index, pl.ds(0, 16), :], line)
            token = lax.broadcasted_iota(jnp.int32, (tokens, LANES), 0).astype(jnp.float32)
            pick = jnp.where(token == token_of, 1.0, 0.0).astype(jnp.bfloat16)
            rows = lax.dot_general(
                pick,
                held[p][b_index, a_index],
                (((0,), (0,)), ((), ())),
                preferred_element_type=jnp.float32,
            )
            outgoing[p][k, :, a_index] = rows.astype(jnp.bfloat16).reshape(8, 16, size)
            return carry

        lax.fori_loop(0, RING, one, 0)

    def deliver(p, k, b_step):
        order = ORDERS[p]
        a, b, s = order
        start, size = parts[p]
        b_index = here.along(b, b_step)
        mine = slots_of(slots, order, b_index, here.at[s], here.core, start, size)
        way = 1 if k % 2 == 0 else -1
        wires.send(
            outgoing[p].at[k, pl.ds(here.along(s, 2) * 2, 2)],
            relay[p].at[k],
            here.near(s, way),
            (p, "relay", k),
        )
        for step in (1, -1):
            for other in (0, 1):
                core = 1 - here.core if other else here.core
                wires.send(
                    outgoing[p].at[k, here.along(s, step) * 2 + core],
                    mine,
                    here.near(s, step, other),
                    (p, "near", step, other, k),
                )
        wires.send(
            outgoing[p].at[k, here.at[s] * 2 + (1 - here.core)],
            mine,
            here.partner(),
            (p, "chip", k),
        )
        keep(outgoing[p].at[k, here.at[s] * 2 + here.core], mine)

    def forward(p, k, b_step):
        order = ORDERS[p]
        a, b, s = order
        start, size = parts[p]
        b_index = here.along(b, b_step)
        way = 1 if k % 2 == 0 else -1
        wires.arrived(relay[p].at[k], (p, "relay", k), here.near(s, -way))
        theirs = slots_of(slots, order, b_index, here.along(s, -way), here.core, start, size)
        for other in (0, 1):
            core = 1 - here.core if other else here.core
            wires.send(
                relay[p].at[k, core], theirs, here.near(s, way, other), (p, "far", other, k)
            )

    def received(p, k, b_step):
        order = ORDERS[p]
        a, b, s = order
        start, size = parts[p]
        b_index = here.along(b, b_step)
        way = 1 if k % 2 == 0 else -1
        for other in (0, 1):
            core = 1 - here.core if other else here.core
            for step in (1, -1):
                wires.arrived(
                    slots_of(slots, order, b_index, here.along(s, -step), core, start, size),
                    (p, "near", step, other, k),
                    here.near(s, -step, other),
                )
            wires.arrived(
                slots_of(slots, order, b_index, here.along(s, 2), core, start, size),
                (p, "far", other, k),
                here.near(s, -way, other),
            )
        wires.arrived(
            slots_of(slots, order, b_index, here.at[s], 1 - here.core, start, size),
            (p, "chip", k),
            here.partner(),
        )

    turns = (0, -1, 1, 2)
    for p in range(3):
        relay_on(p, 0, 0)
    for p in range(3):
        select(p, 0, 0)
        deliver(p, 0, 0)
    for k, step in ((1, -1), (2, 1), (3, 2)):
        for p in range(3):
            relay_on(p, k, step)
    for k in (1, 2):
        for p in range(3):
            select(p, k, turns[k])
            deliver(p, k, turns[k])
    for p in range(3):
        forward(p, 0, 0)
    for p in range(3):
        for k, step in ((0, 0), (1, -1), (2, 1), (3, 2)):
            far_in(p, k, step)
    for p, (a, b, s) in enumerate(ORDERS):
        wires.arrived(seen.at[p, here.along(b, 2)], (p, "t2far"), here.near(b, -1))
    for p in range(3):
        select(p, 3, 2)
        deliver(p, 3, 2)
    maps_out[...] = seen[...]
    for k in (1, 2, 3):
        for p in range(3):
            forward(p, k, turns[k])
    for k in range(4):
        for p in range(3):
            received(p, k, turns[k])
    for copy in local[6:]:
        copy.wait()
    wires.drain()


def dispatch(parts, grad, maps):
    tokens, width = grad.shape
    rows = [pltpu.VMEM((RING, RING, tokens, size), jnp.bfloat16) for _, size in parts]
    outs = [pltpu.VMEM((RING, 8, RING, 16, size), jnp.bfloat16) for _, size in parts]
    relays = [pltpu.VMEM((RING, 2, RING, 16, size), jnp.bfloat16) for _, size in parts]
    table = (3, RING, RING, 32, LANES)
    return pl.pallas_call(
        functools.partial(dispatch_kernel, parts),
        out_shape=(
            jax.ShapeDtypeStruct((RING, RING, RING, 2, 16, width), jnp.bfloat16),
            jax.ShapeDtypeStruct(table, jnp.bfloat16),
        ),
        in_specs=[
            pl.BlockSpec(memory_space=pltpu.HBM),
            pl.BlockSpec(memory_space=pltpu.HBM),
        ],
        out_specs=(
            pl.BlockSpec(memory_space=pltpu.HBM),
            pl.BlockSpec(memory_space=pltpu.VMEM),
        ),
        scratch_shapes=rows
        + outs
        + relays
        + [
            pltpu.VMEM(table, jnp.bfloat16),
            pltpu.SemaphoreType.DMA((192,)),
            pltpu.SemaphoreType.DMA((192,)),
            pltpu.SemaphoreType.DMA((32,)),
        ],
        compiler_params=pltpu.CompilerParams(
            collective_id=0, has_side_effects=True, vmem_limit_bytes=60 * 2**20
        ),
    )(grad, maps)


def combine_kernel(
    parts, back, tables, out, q0, q1, q2, l0, l1, l2, x0, x1, x2, y0, y1, y2,
    u0, u1, u2, v0, v1, v2, ss, rs, ls,
):
    rows, relay = (q0, q1, q2), (l0, l1, l2)
    halves2, whole2 = (x0, x1, x2), (y0, y1, y2)
    halves1, whole1 = (u0, u1, u2), (v0, v1, v2)
    here = Place()
    wires = Wires(ss, rs)
    tokens = out.shape[0]
    local = []
    here.greet()

    def pieces(p, b_index, s_index, c_index):
        start, size = parts[p]
        return slots_of(back, ORDERS[p], b_index, s_index, c_index, start, size)

    def give(p, k, b_step):
        a, b, s = ORDERS[p]
        b_index = here.along(b, b_step)
        mine = rows[p].at[b_index, :, here.at[s] * 2 + here.core]
        way = 1 if k % 2 == 0 else -1
        wires.send(
            pieces(p, b_index, here.along(s, 2), slice(None)),
            relay[p].at[k],
            here.near(s, way),
            (p, "relay", k),
        )
        for step in (1, -1):
            for other in (0, 1):
                core = 1 - here.core if other else here.core
                wires.send(
                    pieces(p, b_index, here.along(s, step), core),
                    mine,
                    here.near(s, step, other),
                    (p, "near", step, other, k),
                )
        wires.send(
            pieces(p, b_index, here.at[s], 1 - here.core), mine, here.partner(), (p, "chip", k)
        )
        copy = pltpu.make_async_copy(
            pieces(p, b_index, here.at[s], here.core), mine, ls.at[len(local)]
        )
        copy.start()
        local.append(copy)

    def forward(p, k, b_step):
        a, b, s = ORDERS[p]
        b_index = here.along(b, b_step)
        way = 1 if k % 2 == 0 else -1
        wires.arrived(relay[p].at[k], (p, "relay", k), here.near(s, -way))
        theirs = rows[p].at[b_index, :, here.along(s, -way) * 2 + here.core]
        for other in (0, 1):
            core = 1 - here.core if other else here.core
            wires.send(
                relay[p].at[k, :, core], theirs, here.near(s, way, other), (p, "far", other, k)
            )

    def gathered(p, k, b_step):
        a, b, s = ORDERS[p]
        b_index = here.along(b, b_step)
        way = 1 if k % 2 == 0 else -1
        for other in (0, 1):
            core = 1 - here.core if other else here.core
            for step in (1, -1):
                wires.arrived(
                    rows[p].at[b_index, :, here.along(s, -step) * 2 + core],
                    (p, "near", step, other, k),
                    here.near(s, -step, other),
                )
            wires.arrived(
                rows[p].at[b_index, :, here.along(s, 2) * 2 + core],
                (p, "far", other, k),
                here.near(s, -way, other),
            )
        wires.arrived(
            rows[p].at[b_index, :, here.at[s] * 2 + (1 - here.core)],
            (p, "chip", k),
            here.partner(),
        )
        local[k * 3 + p].wait()

    def add_up(p, b_step):
        a, b, s = ORDERS[p]
        b_index = here.along(b, b_step)
        line = here.at[b] * RING + here.at[a]
        size = parts[p][1]

        def one(a_index, carry):
            token_of = line_row(tables[p, b_index, a_index, pl.ds(0, 16), :], line)
            gate_of = line_row(tables[p, b_index, a_index, pl.ds(16, 16), :], line)
            token = lax.broadcasted_iota(jnp.int32, (tokens, LANES), 0).astype(jnp.float32)
            weigh = jnp.where(token == token_of, gate_of, 0.0).astype(jnp.bfloat16)
            total = jnp.dot(
                weigh,
                rows[p][b_index, a_index].reshape(LANES, size),
                preferred_element_type=jnp.float32,
            )
            rows[p][b_index, a_index] = total.astype(jnp.bfloat16).reshape(8, 16, size)
            return carry

        lax.fori_loop(0, RING, one, 0)

    def plus(*terms):
        total = terms[0].astype(jnp.float32)
        for term in terms[1:]:
            total = total + term.astype(jnp.float32)
        return total

    def fold2(p, way):
        a, b, s = ORDERS[p]
        b_index = here.along(b, way)
        slot = 0 if way == 1 else 1
        groups = pl.ds(0, 4) if way == 1 else pl.ds(4, 4)
        wires.arrived(halves2[p].at[slot], (p, "half2", way), here.near(b, -way))

        def one(a_index, carry):
            rows[p][b_index, a_index, groups] = plus(
                rows[p][b_index, a_index, groups], halves2[p][slot, a_index]
            ).astype(jnp.bfloat16)
            return carry

        lax.fori_loop(0, RING, one, 0)
        for k, step in enumerate((2, 1, -1, 0)):
            wires.send(
                rows[p].at[b_index, here.along(a, step)],
                whole2[p].at[slot, k],
                here.near(b, way),
                (p, "whole2", way, k),
            )

    def settle2(p, k, step):
        a, b, s = ORDERS[p]
        for way in (1, -1):
            slot = 0 if way == 1 else 1
            wires.arrived(whole2[p].at[slot, k], (p, "whole2", way, k), here.near(b, -way))
        own = rows[p].at[here.at[b], here.along(a, step)]
        return plus(own[...], whole2[p][0, k], whole2[p][1, k])

    order = (2, 1, -1, 0)
    for k, step in enumerate(order):
        for p in range(3):
            give(p, k, step)
    for k, step in enumerate(order):
        for p in range(3):
            forward(p, k, step)
    for p, (a, b, s) in enumerate(ORDERS):
        gathered(p, 0, 2)
        add_up(p, 2)
        far = here.along(b, 2)
        for way, groups in ((1, pl.ds(0, 4)), (-1, pl.ds(4, 4))):
            wires.send(
                rows[p].at[far, :, groups],
                halves2[p].at[0 if way == 1 else 1],
                here.near(b, way),
                (p, "half2", way),
            )
    for k, way in ((1, 1), (2, -1)):
        for p in range(3):
            gathered(p, k, way)
            add_up(p, way)
            fold2(p, way)
    for p in range(3):
        gathered(p, 3, 0)
        add_up(p, 0)
    for p, (a, b, s) in enumerate(ORDERS):
        block = rows[p].at[here.at[b], here.along(a, 2)]
        block[...] = settle2(p, 0, 2).astype(jnp.bfloat16)
        for way, groups in ((1, pl.ds(0, 4)), (-1, pl.ds(4, 4))):
            wires.send(
                rows[p].at[here.at[b], here.along(a, 2), groups],
                halves1[p].at[0 if way == 1 else 1],
                here.near(a, way),
                (p, "half1", way),
            )
    for k, way in ((1, 1), (2, -1)):
        for p, (a, b, s) in enumerate(ORDERS):
            slot = 0 if way == 1 else 1
            groups = pl.ds(0, 4) if way == 1 else pl.ds(4, 4)
            block = rows[p].at[here.at[b], here.along(a, way)]
            block[...] = settle2(p, k, way).astype(jnp.bfloat16)
            wires.arrived(halves1[p].at[slot], (p, "half1", way), here.near(a, -way))
            part = rows[p].at[here.at[b], here.along(a, way), groups]
            part[...] = plus(part[...], halves1[p][slot]).astype(jnp.bfloat16)
            wires.send(block, whole1[p].at[slot], here.near(a, way), (p, "whole1", way))
    for p, (a, b, s) in enumerate(ORDERS):
        start, size = parts[p]
        total = settle2(p, 3, 0)
        for way in (1, -1):
            slot = 0 if way == 1 else 1
            wires.arrived(whole1[p].at[slot], (p, "whole1", way), here.near(a, -way))
        total = plus(total, whole1[p][0], whole1[p][1])
        out[:, pl.ds(start, size)] = total.reshape(tokens, size)
    wires.drain()


def combine(parts, back, tables, tokens):
    width = back.shape[-1]

    def buffers(*lead):
        return [pltpu.VMEM((*lead, size), jnp.bfloat16) for _, size in parts]

    return pl.pallas_call(
        functools.partial(combine_kernel, parts),
        out_shape=jax.ShapeDtypeStruct((tokens, width), jnp.float32),
        in_specs=[
            pl.BlockSpec(memory_space=pltpu.HBM),
            pl.BlockSpec(memory_space=pltpu.VMEM),
        ],
        out_specs=pl.BlockSpec(memory_space=pltpu.VMEM),
        scratch_shapes=buffers(RING, RING, 8, 16)
        + buffers(RING, RING, 2, 16)
        + buffers(2, RING, 4, 16)
        + buffers(2, RING, 8, 16)
        + buffers(2, 4, 16)
        + buffers(2, 8, 16)
        + [
            pltpu.SemaphoreType.DMA((192,)),
            pltpu.SemaphoreType.DMA((192,)),
            pltpu.SemaphoreType.DMA((16,)),
        ],
        compiler_params=pltpu.CompilerParams(
            collective_id=1, has_side_effects=True, vmem_limit_bytes=60 * 2**20
        ),
    )(back, tables)


def in_blocks(shard, dim, size):
    shape = shard.shape
    parts = shard.reshape(*shape[:dim], size, shape[dim] // size, *shape[dim + 1 :])
    return jnp.moveaxis(parts, dim, 0)


def summed_on_arrival(shard, axis, dim):
    size = lax.axis_size(axis)
    parts = lax.all_to_all(in_blocks(shard, dim, size), axis, 0, 0, tiled=True)
    return jnp.sum(parts, axis=0)


def expert_backward(grad_rows, w_gate, w_up, w_down, pre_gate, pre_up):
    upstream = jnp.einsum("rd,fd->rf", grad_rows, w_down, preferred_element_type=jnp.float32)
    first = pre_gate.astype(jnp.float32)
    second = pre_up.astype(jnp.float32)
    gate_sig = jax.nn.sigmoid(first)
    gate_act = first * gate_sig
    hidden = gate_act * second
    slot_combine = jnp.sum(upstream * hidden, axis=-1).astype(jnp.bfloat16)
    grad_first = (upstream * second * gate_sig * (1.0 + first * (1.0 - gate_sig))).astype(
        jnp.bfloat16
    )
    grad_second = (upstream * gate_act).astype(jnp.bfloat16)
    back_rows = jnp.einsum("rf,df->rd", grad_first, w_gate, preferred_element_type=jnp.float32)
    back_rows = back_rows + jnp.einsum(
        "rf,df->rd", grad_second, w_up, preferred_element_type=jnp.float32
    )
    return (back_rows.astype(jnp.bfloat16), slot_combine)


def shards(
    tokens,
    out_grad,
    router_weight,
    gate_weight,
    up_weight,
    down_weight,
    saved_gate,
    saved_up,
    expert_ids,
    aux_weight,
):
    devices = lax.axis_size(AXES)
    seq_size = lax.axis_size(SEQ)
    inputs, upstream_grad, chosen_ids = tokens[0], out_grad[0], expert_ids[0]
    tok_rows, top_count = chosen_ids.shape
    model_width = inputs.shape[1]
    experts = router_weight.shape[1]
    capacity = saved_gate.shape[1] // devices
    parts = column_parts(model_width)

    logits = jnp.dot(inputs, router_weight, preferred_element_type=jnp.float32)
    probs = jax.nn.softmax(logits, axis=-1)
    expert = jnp.arange(experts, dtype=jnp.int32)
    mask = jnp.sum((chosen_ids[:, :, None] == expert).astype(jnp.float32), axis=1)
    chosen_sum = jnp.sum(probs * mask, axis=1, keepdims=True)
    gates = probs * mask / chosen_sum
    position = jnp.arange(tok_rows)
    before = (position[:, None] > position[None, :]).astype(jnp.bfloat16)
    slot_pos = jnp.dot(before, mask.astype(jnp.bfloat16), preferred_element_type=jnp.float32)
    slot = jnp.arange(capacity, dtype=jnp.float32)
    filled = jnp.where(
        (slot_pos[:, None, :] == slot[None, :, None]) & (mask[:, None, :] > 0), 1.0, 0.0
    )
    offset = (position - tok_rows).astype(jnp.float32)
    slot_token = jnp.sum(filled * offset[:, None, None], axis=0) + tok_rows
    slot_gate = jnp.sum(filled * gates[:, None, :], axis=0)
    tables = []
    for a, b, s in ORDERS:
        both = jnp.stack([slot_token, slot_gate]).reshape(2, capacity, RING, RING, RING, 2)
        both = both.transpose(0, 2 + b, 2 + a, 2 + s, 5, 1)
        tables.append(both.reshape(2 * RING * RING, LANES))
    tables = jnp.stack(tables).astype(jnp.bfloat16)

    received, seen = dispatch(parts, upstream_grad, tables)

    back_rows, slot_combine = expert_backward(
        received.reshape(-1, model_width),
        gate_weight[0],
        up_weight[0],
        down_weight[0],
        saved_gate[0],
        saved_up[0],
    )
    combine_back = lax.all_to_all(
        slot_combine.reshape(1, devices, capacity), AXES, split_axis=1, concat_axis=0, tiled=True
    ).reshape(experts, capacity)
    expert_sum = combine(parts, back_rows.reshape(received.shape), seen, tok_rows)

    in_seq = seen[0, :, :, : RING * RING].astype(jnp.float32)
    used = jnp.sum((in_seq < tok_rows).astype(jnp.float32), axis=(0, 1))
    used = jnp.sum(used.reshape(RING, RING, RING, 2, capacity), axis=-1)
    seq_counts = used.transpose(1, 0, 2, 3).reshape(experts)

    combine_dense = jnp.sum(filled * combine_back.T.astype(jnp.float32)[None], axis=1)
    combine_grad = jnp.sum(
        jnp.where(chosen_ids[:, :, None] == expert, combine_dense[:, None, :], 0.0), axis=-1
    )
    prob_sel = (
        combine_dense - jnp.sum(gates * combine_dense, axis=1, keepdims=True)
    ) / chosen_sum
    fraction = experts * seq_counts / (top_count * tok_rows * seq_size)
    prob_grad = prob_sel * mask + aux_weight[0] * fraction[None, :]
    dlogits = probs * (prob_grad - jnp.sum(probs * prob_grad, axis=1, keepdims=True))
    logit_grad = dlogits.astype(jnp.bfloat16)
    token_grad = expert_sum + jnp.einsum(
        "te,de->td", logit_grad, router_weight, preferred_element_type=jnp.float32
    )
    router = jnp.einsum("td,te->de", inputs, logit_grad, preferred_element_type=jnp.float32)
    for axis in AXES:
        router = summed_on_arrival(router, axis, 0)
    return (token_grad.astype(jnp.bfloat16)[None], combine_grad[None], router)


def solution(mesh):
    torus = Mesh(mesh.devices.reshape(RING, RING, RING, 2), AXES)
    return jax.shard_map(
        shards,
        mesh=torus,
        in_specs=(
            P(EXP, SEQ, None),
            P(EXP, SEQ, None),
            P(),
            P(AXES, None, None),
            P(AXES, None, None),
            P(AXES, None, None),
            P(AXES, None, None),
            P(AXES, None, None),
            P(EXP, SEQ, None),
            P(),
        ),
        out_specs=(P(EXP, SEQ, None), P(EXP, SEQ, None), P(AXES, None)),
        check_vma=False,
    )
```

```python
import functools

import jax
import jax.numpy as jnp
from jax import lax
from jax.experimental import pallas as pl
from jax.experimental.pallas import tpu as pltpu
from jax.sharding import Mesh
from jax.sharding import PartitionSpec as P

SEQ = ("seq_0", "seq_1")
EXP = ("exp_0", "exp_1")
AXES = ("seq_0", "seq_1", "exp_0", "exp_1")
MESH = pl.DeviceIdType.MESH
RING = 4
LANES = 128
ORDERS = ((0, 1, 2), (1, 2, 0), (2, 0, 1))


def column_parts(width):
    tiles = width // LANES
    sizes = [(tiles + 2 - p) // 3 * LANES for p in range(3)]
    starts = [0, sizes[0], sizes[0] + sizes[1]]
    return list(zip(starts, sizes))


class Wires:
    def __init__(self, send_sems, recv_sems):
        self.send_sems, self.recv_sems = send_sems, recv_sems
        self.sent, self.names = [], {}

    def slot(self, name):
        return self.recv_sems.at[self.names.setdefault(name, len(self.names))]

    def send(self, src, dst, device, name):
        copy = pltpu.make_async_remote_copy(
            src, dst, self.send_sems.at[len(self.sent)], self.slot(name), device, MESH
        )
        copy.start()
        self.sent.append(copy)

    def arrived(self, ref, name, device):
        pltpu.make_async_remote_copy(
            ref, ref, self.send_sems.at[0], self.slot(name), device, MESH
        ).wait_recv()

    def drain(self):
        for copy in self.sent:
            copy.wait_send()


class Place:
    def __init__(self):
        self.at = [lax.axis_index(name) for name in AXES]
        self.core = self.at[3]

    def along(self, axis, step):
        return lax.rem(self.at[axis] + (step + RING), RING)

    def near(self, axis, step, other_core=0):
        coords = list(self.at)
        coords[axis] = self.along(axis, step)
        if other_core:
            coords[3] = 1 - self.core
        return tuple(coords)

    def partner(self):
        return (self.at[0], self.at[1], self.at[2], 1 - self.core)

    def greet(self):
        barrier = pltpu.get_barrier_semaphore()
        peers = [self.partner()]
        for axis in range(3):
            for step in (1, -1):
                for other in (0, 1):
                    peers.append(self.near(axis, step, other))
        for peer in peers:
            pl.semaphore_signal(barrier, inc=1, device_id=peer, device_id_type=MESH)
        pl.semaphore_wait(barrier, len(peers))


def slots_of(ref, order, b_index, s_index, c_index, start, size):
    a, b, s = order
    where = [None] * 3
    where[a], where[b], where[s] = slice(None), b_index, s_index
    return ref.at[where[0], where[1], where[2], c_index, :, pl.ds(start, size)]


def line_row(table, line):
    rows = table.astype(jnp.float32)
    index = lax.broadcasted_iota(jnp.int32, rows.shape, 0)
    return jnp.sum(jnp.where(index == line, rows, 0.0), axis=0, keepdims=True)


def fixed_b(order, b_index):
    where = [slice(None)] * 3
    where[order[1]] = b_index
    return tuple(where)


def dispatch_kernel(
    parts, grad, maps, down, slots, maps_out, upstream,
    g0, g1, g2, o0, o1, o2, l0, l1, l2, seen, weight, batch, ss, rs, ls, bs,
):
    held, outgoing, relay = (g0, g1, g2), (o0, o1, o2), (l0, l1, l2)
    here = Place()
    wires = Wires(ss, rs)
    tokens = grad.shape[0]
    half = tokens // 2
    local = []

    def keep(src, dst):
        copy = pltpu.make_async_copy(src, dst, ls.at[len(local)])
        copy.start()
        local.append(copy)

    for p, (a, b, s) in enumerate(ORDERS):
        start, size = parts[p]
        keep(grad.at[:, pl.ds(start, size)], held[p].at[here.at[b], here.at[a]])
        keep(maps.at[p], seen.at[p, here.at[b], here.at[a]])
    fetch = pltpu.make_async_copy(down, weight, bs.at[2])
    fetch.start()
    here.greet()
    for copy in local:
        copy.wait()

    def pass_on(p, k, step):
        a, b, s = ORDERS[p]
        block = held[p].at[here.at[b], here.along(a, step)]
        wires.send(block, block, here.near(b, 1), (p, "m2", 1, k))
        wires.send(block, block, here.near(b, -1), (p, "m2", -1, k))

    def relay_on(p, k, step):
        a, b, s = ORDERS[p]
        for way, rows in ((1, pl.ds(0, half)), (-1, pl.ds(half, half))):
            block = held[p].at[here.along(b, -way), here.along(a, step)]
            wires.arrived(block, (p, "m2", way, k), here.near(b, -way))
            piece = held[p].at[here.along(b, -way), here.along(a, step), rows]
            wires.send(piece, piece, here.near(b, way), (p, "m2far", way, k))

    def far_in(p, k, step):
        a, b, s = ORDERS[p]
        for way, rows in ((1, pl.ds(0, half)), (-1, pl.ds(half, half))):
            piece = held[p].at[here.along(b, 2), here.along(a, step), rows]
            wires.arrived(piece, (p, "m2far", way, k), here.near(b, -way))

    for p, (a, b, s) in enumerate(ORDERS):
        table = seen.at[p, here.at[b], here.at[a]]
        block = held[p].at[here.at[b], here.at[a]]
        for way in (1, -1):
            wires.send(table, table, here.near(a, way), (p, "t1", way))
        for way in (1, -1):
            wires.send(block, block, here.near(a, way), (p, "m1", way))
    for p in range(3):
        pass_on(p, 0, 0)
    for p, (a, b, s) in enumerate(ORDERS):
        table = seen.at[p, here.at[b], here.along(a, -1)]
        wires.arrived(table, (p, "t1", 1), here.near(a, -1))
        wires.send(table, table, here.near(a, 1), (p, "t1far"))
        wires.arrived(
            seen.at[p, here.at[b], here.along(a, 1)], (p, "t1", -1), here.near(a, 1)
        )
    for p, (a, b, s) in enumerate(ORDERS):
        for way, rows in ((1, pl.ds(0, half)), (-1, pl.ds(half, half))):
            block = held[p].at[here.at[b], here.along(a, -way)]
            wires.arrived(block, (p, "m1", way), here.near(a, -way))
            piece = held[p].at[here.at[b], here.along(a, -way), rows]
            wires.send(piece, piece, here.near(a, way), (p, "m1far", way))
    for p, (a, b, s) in enumerate(ORDERS):
        wires.arrived(
            seen.at[p, here.at[b], here.along(a, 2)], (p, "t1far"), here.near(a, -1)
        )
        table = seen.at[p, here.at[b]]
        for way in (1, -1):
            wires.send(table, table, here.near(b, way), (p, "t2", way))
    for p in range(3):
        pass_on(p, 1, -1)
        pass_on(p, 2, 1)
    for p, (a, b, s) in enumerate(ORDERS):
        table = seen.at[p, here.along(b, -1)]
        wires.arrived(table, (p, "t2", 1), here.near(b, -1))
        wires.send(table, table, here.near(b, 1), (p, "t2far"))
        wires.arrived(seen.at[p, here.along(b, 1)], (p, "t2", -1), here.near(b, 1))
    for p, (a, b, s) in enumerate(ORDERS):
        for way, rows in ((1, pl.ds(0, half)), (-1, pl.ds(half, half))):
            piece = held[p].at[here.at[b], here.along(a, 2), rows]
            wires.arrived(piece, (p, "m1far", way), here.near(a, -way))
        pass_on(p, 3, 2)

    def select(p, k, b_step):
        a, b, s = ORDERS[p]
        b_index = here.along(b, b_step)
        line = here.at[b] * RING + here.at[a]
        size = parts[p][1]

        def one(a_index, carry):
            token_of = line_row(seen[p, b_index, a_index, pl.ds(0, 16), :], line)
            token = lax.broadcasted_iota(jnp.int32, (tokens, LANES), 0).astype(jnp.float32)
            pick = jnp.where(token == token_of, 1.0, 0.0).astype(jnp.bfloat16)
            rows = lax.dot_general(
                pick,
                held[p][b_index, a_index],
                (((0,), (0,)), ((), ())),
                preferred_element_type=jnp.float32,
            )
            outgoing[p][k, :, a_index] = rows.astype(jnp.bfloat16).reshape(8, 16, size)
            return carry

        lax.fori_loop(0, RING, one, 0)

    def deliver(p, k, b_step):
        order = ORDERS[p]
        a, b, s = order
        start, size = parts[p]
        b_index = here.along(b, b_step)
        mine = slots_of(slots, order, b_index, here.at[s], here.core, start, size)
        way = 1 if k % 2 == 0 else -1
        wires.send(
            outgoing[p].at[k, pl.ds(here.along(s, 2) * 2, 2)],
            relay[p].at[k],
            here.near(s, way),
            (p, "relay", k),
        )
        for step in (1, -1):
            for other in (0, 1):
                core = 1 - here.core if other else here.core
                wires.send(
                    outgoing[p].at[k, here.along(s, step) * 2 + core],
                    mine,
                    here.near(s, step, other),
                    (p, "near", step, other, k),
                )
        wires.send(
            outgoing[p].at[k, here.at[s] * 2 + (1 - here.core)],
            mine,
            here.partner(),
            (p, "chip", k),
        )
        keep(outgoing[p].at[k, here.at[s] * 2 + here.core], mine)

    def forward(p, k, b_step):
        order = ORDERS[p]
        a, b, s = order
        start, size = parts[p]
        b_index = here.along(b, b_step)
        way = 1 if k % 2 == 0 else -1
        wires.arrived(relay[p].at[k], (p, "relay", k), here.near(s, -way))
        theirs = slots_of(slots, order, b_index, here.along(s, -way), here.core, start, size)
        for other in (0, 1):
            core = 1 - here.core if other else here.core
            wires.send(
                relay[p].at[k, core], theirs, here.near(s, way, other), (p, "far", other, k)
            )

    def received(p, k, b_step):
        order = ORDERS[p]
        a, b, s = order
        start, size = parts[p]
        b_index = here.along(b, b_step)
        way = 1 if k % 2 == 0 else -1
        for other in (0, 1):
            core = 1 - here.core if other else here.core
            for step in (1, -1):
                wires.arrived(
                    slots_of(slots, order, b_index, here.along(s, -step), core, start, size),
                    (p, "near", step, other, k),
                    here.near(s, -step, other),
                )
            wires.arrived(
                slots_of(slots, order, b_index, here.along(s, 2), core, start, size),
                (p, "far", other, k),
                here.near(s, -way, other),
            )
        wires.arrived(
            slots_of(slots, order, b_index, here.at[s], 1 - here.core, start, size),
            (p, "chip", k),
            here.partner(),
        )

    def batch_copy(p, k):
        start, size = parts[p]
        b_index = here.along(ORDERS[p][1], turns[k])
        slot = (k * 3 + p) % 2
        return pltpu.make_async_copy(
            slots.at[(*fixed_b(ORDERS[p], b_index), slice(None), slice(None), pl.ds(start, size))],
            batch.at[slot, :, :, :, :, pl.ds(0, size)],
            bs.at[slot],
        )

    def ready(p, k):
        received(p, k, turns[k])
        local[6 + k * 3 + p].wait()
        batch_copy(p, k).start()

    def project(p, k):
        start, size = parts[p]
        b_index = here.along(ORDERS[p][1], turns[k])
        slot = (k * 3 + p) % 2
        batch_copy(p, k).wait()
        where = fixed_b(ORDERS[p], b_index)

        def tile(n, carry):
            units = pl.ds(pl.multiple_of(n * 256, 256), 256)
            term = lax.dot_general(
                batch[slot, :, :, :, :, pl.ds(0, size)].reshape(512, size),
                weight[units, pl.ds(start, size)],
                (((1,), (1,)), ((), ())),
                preferred_element_type=jnp.float32,
            )
            there = (*where, slice(None), slice(None), units)
            upstream[there] = upstream[there] + term.reshape(RING, RING, 2, 16, 256)
            return carry

        lax.fori_loop(0, 3, tile, 0)

    turns = (0, -1, 1, 2)
    for p in range(3):
        relay_on(p, 0, 0)
    for p in range(3):
        select(p, 0, 0)
        deliver(p, 0, 0)
    for k, step in ((1, -1), (2, 1), (3, 2)):
        for p in range(3):
            relay_on(p, k, step)
    for k in (1, 2):
        for p in range(3):
            select(p, k, turns[k])
            deliver(p, k, turns[k])
    for p in range(3):
        forward(p, 0, 0)
    for p in range(3):
        for k, step in ((0, 0), (1, -1), (2, 1), (3, 2)):
            far_in(p, k, step)
    for p, (a, b, s) in enumerate(ORDERS):
        wires.arrived(seen.at[p, here.along(b, 2)], (p, "t2far"), here.near(b, -1))
    for p in range(3):
        select(p, 3, 2)
        deliver(p, 3, 2)
    maps_out[...] = seen[...]
    upstream[...] = jnp.zeros_like(upstream)
    fetch.wait()
    for p in range(3):
        forward(p, 1, turns[1])
    work = [(k, p) for k in range(4) for p in range(3)]
    ready(work[0][1], work[0][0])
    for turn, (k, p) in enumerate(work):
        if turn + 1 < len(work):
            after_k, after_p = work[turn + 1]
            if after_p == 0 and after_k < 3:
                for q in range(3):
                    forward(q, after_k + 1, turns[after_k + 1])
            ready(after_p, after_k)
        project(p, k)
    wires.drain()


def dispatch(parts, grad, maps, down):
    tokens, width = grad.shape
    rows = [pltpu.VMEM((RING, RING, tokens, size), jnp.bfloat16) for _, size in parts]
    outs = [pltpu.VMEM((RING, 8, RING, 16, size), jnp.bfloat16) for _, size in parts]
    relays = [pltpu.VMEM((RING, 2, RING, 16, size), jnp.bfloat16) for _, size in parts]
    table = (3, RING, RING, 32, LANES)
    units = down.shape[0]
    return pl.pallas_call(
        functools.partial(dispatch_kernel, parts),
        out_shape=(
            jax.ShapeDtypeStruct((RING, RING, RING, 2, 16, width), jnp.bfloat16),
            jax.ShapeDtypeStruct(table, jnp.bfloat16),
            jax.ShapeDtypeStruct((RING, RING, RING, 2, 16, units), jnp.float32),
        ),
        in_specs=[pl.BlockSpec(memory_space=pltpu.HBM)] * 3,
        out_specs=(
            pl.BlockSpec(memory_space=pltpu.HBM),
            pl.BlockSpec(memory_space=pltpu.VMEM),
            pl.BlockSpec(memory_space=pltpu.VMEM),
        ),
        scratch_shapes=rows
        + outs
        + relays
        + [
            pltpu.VMEM(table, jnp.bfloat16),
            pltpu.VMEM((units, width), jnp.bfloat16),
            pltpu.VMEM((2, RING, RING, 2, 16, parts[0][1]), jnp.bfloat16),
            pltpu.SemaphoreType.DMA((192,)),
            pltpu.SemaphoreType.DMA((192,)),
            pltpu.SemaphoreType.DMA((32,)),
            pltpu.SemaphoreType.DMA((3,)),
        ],
        compiler_params=pltpu.CompilerParams(
            collective_id=0, has_side_effects=True, vmem_limit_bytes=60 * 2**20
        ),
    )(grad, maps, down)


def combine_kernel(
    parts, grad_first, grad_second, w_gate, w_up, tables, out, back,
    q0, q1, q2, l0, l1, l2, x0, x1, x2, y0, y1, y2, u0, u1, u2, v0, v1, v2,
    gate, up, stage, ss, rs, ls, bs,
):
    rows, relay = (q0, q1, q2), (l0, l1, l2)
    halves2, whole2 = (x0, x1, x2), (y0, y1, y2)
    halves1, whole1 = (u0, u1, u2), (v0, v1, v2)
    here = Place()
    wires = Wires(ss, rs)
    tokens = out.shape[0]
    local = []
    fetches = []
    for p, (start, size) in enumerate(parts):
        for n, (src, dst) in enumerate(((w_gate, gate), (w_up, up))):
            span = pl.ds(start, size)
            copy = pltpu.make_async_copy(src.at[span], dst.at[span], bs.at[2 + 2 * p + n])
            copy.start()
            fetches.append(copy)
    here.greet()

    def stage_copy(p, k, b_step):
        start, size = parts[p]
        b_index = here.along(ORDERS[p][1], b_step)
        slot = (k * 3 + p) % 2
        return pltpu.make_async_copy(
            stage.at[slot, :, :, :, :, pl.ds(0, size)],
            back.at[(*fixed_b(ORDERS[p], b_index), slice(None), slice(None), pl.ds(start, size))],
            bs.at[slot],
        )

    def produce(p, k, b_step):
        start, size = parts[p]
        b_index = here.along(ORDERS[p][1], b_step)
        slot = (k * 3 + p) % 2
        where = fixed_b(ORDERS[p], b_index)
        units = grad_first.shape[-1]
        if k == 0:
            fetches[2 * p].wait()
            fetches[2 * p + 1].wait()

        def columns(offset, width):
            span = pl.ds(start + offset, width)
            total = 0.0
            for grads, weight in ((grad_first, gate), (grad_second, up)):
                total = total + lax.dot_general(
                    grads[where].reshape(512, units),
                    weight[span],
                    (((1,), (1,)), ((), ())),
                    preferred_element_type=jnp.float32,
                )
            stage[slot, :, :, :, :, pl.ds(offset, width)] = total.astype(jnp.bfloat16).reshape(
                RING, RING, 2, 16, width
            )

        def tile(n, carry):
            columns(pl.multiple_of(n * 256, 256), 256)
            return carry

        lax.fori_loop(0, size // 256, tile, 0)
        if size % 256:
            columns(size // 256 * 256, size % 256)
        stage_copy(p, k, b_step).start()

    def pieces(p, b_index, s_index, c_index):
        start, size = parts[p]
        return slots_of(back, ORDERS[p], b_index, s_index, c_index, start, size)

    def give(p, k, b_step):
        a, b, s = ORDERS[p]
        b_index = here.along(b, b_step)
        mine = rows[p].at[b_index, :, here.at[s] * 2 + here.core]
        way = 1 if k % 2 == 0 else -1
        wires.send(
            pieces(p, b_index, here.along(s, 2), slice(None)),
            relay[p].at[k],
            here.near(s, way),
            (p, "relay", k),
        )
        for step in (1, -1):
            for other in (0, 1):
                core = 1 - here.core if other else here.core
                wires.send(
                    pieces(p, b_index, here.along(s, step), core),
                    mine,
                    here.near(s, step, other),
                    (p, "near", step, other, k),
                )
        wires.send(
            pieces(p, b_index, here.at[s], 1 - here.core), mine, here.partner(), (p, "chip", k)
        )
        copy = pltpu.make_async_copy(
            pieces(p, b_index, here.at[s], here.core), mine, ls.at[len(local)]
        )
        copy.start()
        local.append(copy)

    def forward(p, k, b_step):
        a, b, s = ORDERS[p]
        b_index = here.along(b, b_step)
        way = 1 if k % 2 == 0 else -1
        wires.arrived(relay[p].at[k], (p, "relay", k), here.near(s, -way))
        theirs = rows[p].at[b_index, :, here.along(s, -way) * 2 + here.core]
        for other in (0, 1):
            core = 1 - here.core if other else here.core
            wires.send(
                relay[p].at[k, :, core], theirs, here.near(s, way, other), (p, "far", other, k)
            )

    def gathered(p, k, b_step):
        a, b, s = ORDERS[p]
        b_index = here.along(b, b_step)
        way = 1 if k % 2 == 0 else -1
        for other in (0, 1):
            core = 1 - here.core if other else here.core
            for step in (1, -1):
                wires.arrived(
                    rows[p].at[b_index, :, here.along(s, -step) * 2 + core],
                    (p, "near", step, other, k),
                    here.near(s, -step, other),
                )
            wires.arrived(
                rows[p].at[b_index, :, here.along(s, 2) * 2 + core],
                (p, "far", other, k),
                here.near(s, -way, other),
            )
        wires.arrived(
            rows[p].at[b_index, :, here.at[s] * 2 + (1 - here.core)],
            (p, "chip", k),
            here.partner(),
        )
        local[k * 3 + p].wait()

    def add_up(p, b_step):
        a, b, s = ORDERS[p]
        b_index = here.along(b, b_step)
        line = here.at[b] * RING + here.at[a]
        size = parts[p][1]

        def one(a_index, carry):
            token_of = line_row(tables[p, b_index, a_index, pl.ds(0, 16), :], line)
            gate_of = line_row(tables[p, b_index, a_index, pl.ds(16, 16), :], line)
            token = lax.broadcasted_iota(jnp.int32, (tokens, LANES), 0).astype(jnp.float32)
            weigh = jnp.where(token == token_of, gate_of, 0.0).astype(jnp.bfloat16)
            total = jnp.dot(
                weigh,
                rows[p][b_index, a_index].reshape(LANES, size),
                preferred_element_type=jnp.float32,
            )
            rows[p][b_index, a_index] = total.astype(jnp.bfloat16).reshape(8, 16, size)
            return carry

        lax.fori_loop(0, RING, one, 0)

    def plus(*terms):
        total = terms[0].astype(jnp.float32)
        for term in terms[1:]:
            total = total + term.astype(jnp.float32)
        return total

    def fold2(p, way):
        a, b, s = ORDERS[p]
        b_index = here.along(b, way)
        slot = 0 if way == 1 else 1
        groups = pl.ds(0, 4) if way == 1 else pl.ds(4, 4)
        wires.arrived(halves2[p].at[slot], (p, "half2", way), here.near(b, -way))

        def one(a_index, carry):
            rows[p][b_index, a_index, groups] = plus(
                rows[p][b_index, a_index, groups], halves2[p][slot, a_index]
            ).astype(jnp.bfloat16)
            return carry

        lax.fori_loop(0, RING, one, 0)
        for k, step in enumerate((2, 1, -1, 0)):
            wires.send(
                rows[p].at[b_index, here.along(a, step)],
                whole2[p].at[slot, k],
                here.near(b, way),
                (p, "whole2", way, k),
            )

    def settle2(p, k, step):
        a, b, s = ORDERS[p]
        for way in (1, -1):
            slot = 0 if way == 1 else 1
            wires.arrived(whole2[p].at[slot, k], (p, "whole2", way, k), here.near(b, -way))
        own = rows[p].at[here.at[b], here.along(a, step)]
        return plus(own[...], whole2[p][0, k], whole2[p][1, k])

    order = (2, 1, -1, 0)
    work = [(k, p) for k in range(4) for p in range(3)]
    for turn in range(len(work) + 1):
        if turn < len(work):
            k, p = work[turn]
            produce(p, k, order[k])
        if turn > 0:
            k, p = work[turn - 1]
            stage_copy(p, k, order[k]).wait()
            give(p, k, order[k])
            if p == 2 and k > 0:
                for q in range(3):
                    forward(q, k - 1, order[k - 1])
    for p, (a, b, s) in enumerate(ORDERS):
        gathered(p, 0, 2)
        add_up(p, 2)
        far = here.along(b, 2)
        for way, groups in ((1, pl.ds(0, 4)), (-1, pl.ds(4, 4))):
            wires.send(
                rows[p].at[far, :, groups],
                halves2[p].at[0 if way == 1 else 1],
                here.near(b, way),
                (p, "half2", way),
            )
    for q in range(3):
        forward(q, 3, order[3])
    for k, way in ((1, 1), (2, -1)):
        for p in range(3):
            gathered(p, k, way)
            add_up(p, way)
            fold2(p, way)
    for p in range(3):
        gathered(p, 3, 0)
        add_up(p, 0)
    for p, (a, b, s) in enumerate(ORDERS):
        block = rows[p].at[here.at[b], here.along(a, 2)]
        block[...] = settle2(p, 0, 2).astype(jnp.bfloat16)
        for way, groups in ((1, pl.ds(0, 4)), (-1, pl.ds(4, 4))):
            wires.send(
                rows[p].at[here.at[b], here.along(a, 2), groups],
                halves1[p].at[0 if way == 1 else 1],
                here.near(a, way),
                (p, "half1", way),
            )
    for k, way in ((1, 1), (2, -1)):
        for p, (a, b, s) in enumerate(ORDERS):
            slot = 0 if way == 1 else 1
            groups = pl.ds(0, 4) if way == 1 else pl.ds(4, 4)
            block = rows[p].at[here.at[b], here.along(a, way)]
            block[...] = settle2(p, k, way).astype(jnp.bfloat16)
            wires.arrived(halves1[p].at[slot], (p, "half1", way), here.near(a, -way))
            part = rows[p].at[here.at[b], here.along(a, way), groups]
            part[...] = plus(part[...], halves1[p][slot]).astype(jnp.bfloat16)
            wires.send(block, whole1[p].at[slot], here.near(a, way), (p, "whole1", way))
    for p, (a, b, s) in enumerate(ORDERS):
        start, size = parts[p]
        total = settle2(p, 3, 0)
        for way in (1, -1):
            slot = 0 if way == 1 else 1
            wires.arrived(whole1[p].at[slot], (p, "whole1", way), here.near(a, -way))
        total = plus(total, whole1[p][0], whole1[p][1])
        out[:, pl.ds(start, size)] = total.reshape(tokens, size)
    wires.drain()


def combine(parts, grad_first, grad_second, w_gate, w_up, tables, tokens):
    width, units = w_gate.shape

    def buffers(*lead):
        return [pltpu.VMEM((*lead, size), jnp.bfloat16) for _, size in parts]

    return pl.pallas_call(
        functools.partial(combine_kernel, parts),
        out_shape=(
            jax.ShapeDtypeStruct((tokens, width), jnp.float32),
            jax.ShapeDtypeStruct((RING, RING, RING, 2, 16, width), jnp.bfloat16),
        ),
        in_specs=[
            pl.BlockSpec(memory_space=pltpu.VMEM),
            pl.BlockSpec(memory_space=pltpu.VMEM),
            pl.BlockSpec(memory_space=pltpu.HBM),
            pl.BlockSpec(memory_space=pltpu.HBM),
            pl.BlockSpec(memory_space=pltpu.VMEM),
        ],
        out_specs=(
            pl.BlockSpec(memory_space=pltpu.VMEM),
            pl.BlockSpec(memory_space=pltpu.HBM),
        ),
        scratch_shapes=buffers(RING, RING, 8, 16)
        + buffers(RING, RING, 2, 16)
        + buffers(2, RING, 4, 16)
        + buffers(2, RING, 8, 16)
        + buffers(2, 4, 16)
        + buffers(2, 8, 16)
        + [
            pltpu.VMEM((width, units), jnp.bfloat16),
            pltpu.VMEM((width, units), jnp.bfloat16),
            pltpu.VMEM((2, RING, RING, 2, 16, parts[0][1]), jnp.bfloat16),
            pltpu.SemaphoreType.DMA((192,)),
            pltpu.SemaphoreType.DMA((192,)),
            pltpu.SemaphoreType.DMA((16,)),
            pltpu.SemaphoreType.DMA((8,)),
        ],
        compiler_params=pltpu.CompilerParams(
            collective_id=1, has_side_effects=True, vmem_limit_bytes=63 * 2**20
        ),
    )(grad_first, grad_second, w_gate, w_up, tables)[0]


def in_blocks(shard, dim, size):
    shape = shard.shape
    parts = shard.reshape(*shape[:dim], size, shape[dim] // size, *shape[dim + 1 :])
    return jnp.moveaxis(parts, dim, 0)


def summed_on_arrival(shard, axis, dim):
    size = lax.axis_size(axis)
    parts = lax.all_to_all(in_blocks(shard, dim, size), axis, 0, 0, tiled=True)
    return jnp.sum(parts, axis=0)


def hidden_backward(upstream, pre_gate, pre_up):
    first = pre_gate.astype(jnp.float32)
    second = pre_up.astype(jnp.float32)
    gate_sig = jax.nn.sigmoid(first)
    gate_act = first * gate_sig
    hidden = gate_act * second
    slot_combine = jnp.sum(upstream * hidden, axis=-1).astype(jnp.bfloat16)
    grad_first = (upstream * second * gate_sig * (1.0 + first * (1.0 - gate_sig))).astype(
        jnp.bfloat16
    )
    grad_second = (upstream * gate_act).astype(jnp.bfloat16)
    return grad_first, grad_second, slot_combine


def shards(
    tokens,
    out_grad,
    router_weight,
    gate_weight,
    up_weight,
    down_weight,
    saved_gate,
    saved_up,
    expert_ids,
    aux_weight,
):
    devices = lax.axis_size(AXES)
    seq_size = lax.axis_size(SEQ)
    inputs, upstream_grad, chosen_ids = tokens[0], out_grad[0], expert_ids[0]
    tok_rows, top_count = chosen_ids.shape
    model_width = inputs.shape[1]
    experts = router_weight.shape[1]
    capacity = saved_gate.shape[1] // devices
    parts = column_parts(model_width)

    logits = jnp.dot(inputs, router_weight, preferred_element_type=jnp.float32)
    probs = jax.nn.softmax(logits, axis=-1)
    expert = jnp.arange(experts, dtype=jnp.int32)
    mask = jnp.sum((chosen_ids[:, :, None] == expert).astype(jnp.float32), axis=1)
    chosen_sum = jnp.sum(probs * mask, axis=1, keepdims=True)
    gates = probs * mask / chosen_sum
    position = jnp.arange(tok_rows)
    before = (position[:, None] > position[None, :]).astype(jnp.bfloat16)
    slot_pos = jnp.dot(before, mask.astype(jnp.bfloat16), preferred_element_type=jnp.float32)
    slot = jnp.arange(capacity, dtype=jnp.float32)
    filled = jnp.where(
        (slot_pos[:, None, :] == slot[None, :, None]) & (mask[:, None, :] > 0), 1.0, 0.0
    )
    offset = (position - tok_rows).astype(jnp.float32)
    slot_token = jnp.sum(filled * offset[:, None, None], axis=0) + tok_rows
    slot_gate = jnp.sum(filled * gates[:, None, :], axis=0)
    tables = []
    for a, b, s in ORDERS:
        both = jnp.stack([slot_token, slot_gate]).reshape(2, capacity, RING, RING, RING, 2)
        both = both.transpose(0, 2 + b, 2 + a, 2 + s, 5, 1)
        tables.append(both.reshape(2 * RING * RING, LANES))
    tables = jnp.stack(tables).astype(jnp.bfloat16)

    _, seen, upstream = dispatch(parts, upstream_grad, tables, down_weight[0])
    grad_first, grad_second, slot_combine = hidden_backward(
        upstream,
        saved_gate[0].reshape(upstream.shape),
        saved_up[0].reshape(upstream.shape),
    )
    combine_back = lax.all_to_all(
        slot_combine.reshape(1, devices, capacity), AXES, split_axis=1, concat_axis=0, tiled=True
    ).reshape(experts, capacity)
    expert_sum = combine(
        parts, grad_first, grad_second, gate_weight[0], up_weight[0], seen, tok_rows
    )

    in_seq = seen[0, :, :, : RING * RING].astype(jnp.float32)
    used = jnp.sum((in_seq < tok_rows).astype(jnp.float32), axis=(0, 1))
    used = jnp.sum(used.reshape(RING, RING, RING, 2, capacity), axis=-1)
    seq_counts = used.transpose(1, 0, 2, 3).reshape(experts)

    combine_dense = jnp.sum(filled * combine_back.T.astype(jnp.float32)[None], axis=1)
    combine_grad = jnp.sum(
        jnp.where(chosen_ids[:, :, None] == expert, combine_dense[:, None, :], 0.0), axis=-1
    )
    prob_sel = (
        combine_dense - jnp.sum(gates * combine_dense, axis=1, keepdims=True)
    ) / chosen_sum
    fraction = experts * seq_counts / (top_count * tok_rows * seq_size)
    prob_grad = prob_sel * mask + aux_weight[0] * fraction[None, :]
    dlogits = probs * (prob_grad - jnp.sum(probs * prob_grad, axis=1, keepdims=True))
    logit_grad = dlogits.astype(jnp.bfloat16)
    token_grad = expert_sum + jnp.einsum(
        "te,de->td", logit_grad, router_weight, preferred_element_type=jnp.float32
    )
    router = jnp.einsum("td,te->de", inputs, logit_grad, preferred_element_type=jnp.float32)
    for axis in AXES:
        router = summed_on_arrival(router, axis, 0)
    return (token_grad.astype(jnp.bfloat16)[None], combine_grad[None], router)


def solution(mesh):
    torus = Mesh(mesh.devices.reshape(RING, RING, RING, 2), AXES)
    return jax.shard_map(
        shards,
        mesh=torus,
        in_specs=(
            P(EXP, SEQ, None),
            P(EXP, SEQ, None),
            P(),
            P(AXES, None, None),
            P(AXES, None, None),
            P(AXES, None, None),
            P(AXES, None, None),
            P(AXES, None, None),
            P(EXP, SEQ, None),
            P(),
        ),
        out_specs=(P(EXP, SEQ, None), P(EXP, SEQ, None), P(AXES, None)),
        check_vma=False,
    )
```

```python
import functools

import jax
import jax.numpy as jnp
from jax import lax
from jax.experimental import pallas as pl
from jax.experimental.pallas import tpu as pltpu
from jax.sharding import Mesh
from jax.sharding import PartitionSpec as P

SEQ = ("seq_0", "seq_1")
EXP = ("exp_0", "exp_1")
AXES = ("seq_0", "seq_1", "exp_0", "exp_1")
MESH = pl.DeviceIdType.MESH
RING = 4
LANES = 128
ORDERS = ((0, 1, 2), (1, 2, 0), (2, 0, 1))


def column_parts(width):
    tiles = width // LANES
    sizes = [(tiles + 2 - p) // 3 * LANES for p in range(3)]
    starts = [0, sizes[0], sizes[0] + sizes[1]]
    return list(zip(starts, sizes))


class Wires:
    def __init__(self, send_sems, recv_sems):
        self.send_sems, self.recv_sems = send_sems, recv_sems
        self.sent, self.names = [], {}

    def slot(self, name):
        return self.recv_sems.at[self.names.setdefault(name, len(self.names))]

    def send(self, src, dst, device, name):
        copy = pltpu.make_async_remote_copy(
            src, dst, self.send_sems.at[len(self.sent)], self.slot(name), device, MESH
        )
        copy.start()
        self.sent.append(copy)

    def arrived(self, ref, name, device):
        pltpu.make_async_remote_copy(
            ref, ref, self.send_sems.at[0], self.slot(name), device, MESH
        ).wait_recv()

    def drain(self):
        for copy in self.sent:
            copy.wait_send()


class Place:
    def __init__(self):
        self.at = [lax.axis_index(name) for name in AXES]
        self.core = self.at[3]

    def along(self, axis, step):
        return lax.rem(self.at[axis] + (step + RING), RING)

    def near(self, axis, step, other_core=0):
        coords = list(self.at)
        coords[axis] = self.along(axis, step)
        if other_core:
            coords[3] = 1 - self.core
        return tuple(coords)

    def partner(self):
        return (self.at[0], self.at[1], self.at[2], 1 - self.core)

    def greet(self, steps=(1, -1)):
        barrier = pltpu.get_barrier_semaphore()
        peers = [self.partner()]
        for axis in range(3):
            for step in steps:
                for other in (0, 1):
                    peers.append(self.near(axis, step, other))
        for peer in peers:
            pl.semaphore_signal(barrier, inc=1, device_id=peer, device_id_type=MESH)
        pl.semaphore_wait(barrier, len(peers))


def slots_of(ref, order, b_index, s_index, c_index, start, size):
    a, b, s = order
    where = [None] * 3
    where[a], where[b], where[s] = slice(None), b_index, s_index
    return ref.at[where[0], where[1], where[2], c_index, :, pl.ds(start, size)]


def line_row(table, line):
    rows = table.astype(jnp.float32)
    index = lax.broadcasted_iota(jnp.int32, rows.shape, 0)
    return jnp.sum(jnp.where(index == line, rows, 0.0), axis=0, keepdims=True)


def fixed_b(order, b_index):
    where = [slice(None)] * 3
    where[order[1]] = b_index
    return tuple(where)


def dispatch_kernel(
    parts, grad, maps, down, slots, maps_out, upstream,
    g0, g1, g2, o0, o1, o2, l0, l1, l2, seen, weight, batch, ss, rs, ls, bs,
):
    held, outgoing, relay = (g0, g1, g2), (o0, o1, o2), (l0, l1, l2)
    here = Place()
    wires = Wires(ss, rs)
    tokens = grad.shape[0]
    half = tokens // 2
    local = []

    def keep(src, dst):
        copy = pltpu.make_async_copy(src, dst, ls.at[len(local)])
        copy.start()
        local.append(copy)

    for p, (a, b, s) in enumerate(ORDERS):
        start, size = parts[p]
        keep(grad.at[:, pl.ds(start, size)], held[p].at[here.at[b], here.at[a]])
        keep(maps.at[p], seen.at[p, here.at[b], here.at[a]])
    fetch = pltpu.make_async_copy(down, weight, bs.at[2])
    fetch.start()
    here.greet()
    for copy in local:
        copy.wait()

    def pass_on(p, k, step):
        a, b, s = ORDERS[p]
        block = held[p].at[here.at[b], here.along(a, step)]
        wires.send(block, block, here.near(b, 1), (p, "m2", 1, k))
        wires.send(block, block, here.near(b, -1), (p, "m2", -1, k))

    def relay_on(p, k, step):
        a, b, s = ORDERS[p]
        for way, rows in ((1, pl.ds(0, half)), (-1, pl.ds(half, half))):
            block = held[p].at[here.along(b, -way), here.along(a, step)]
            wires.arrived(block, (p, "m2", way, k), here.near(b, -way))
            piece = held[p].at[here.along(b, -way), here.along(a, step), rows]
            wires.send(piece, piece, here.near(b, way), (p, "m2far", way, k))

    def far_in(p, k, step):
        a, b, s = ORDERS[p]
        for way, rows in ((1, pl.ds(0, half)), (-1, pl.ds(half, half))):
            piece = held[p].at[here.along(b, 2), here.along(a, step), rows]
            wires.arrived(piece, (p, "m2far", way, k), here.near(b, -way))

    for p, (a, b, s) in enumerate(ORDERS):
        table = seen.at[p, here.at[b], here.at[a]]
        block = held[p].at[here.at[b], here.at[a]]
        for way in (1, -1):
            wires.send(table, table, here.near(a, way), (p, "t1", way))
        for way in (1, -1):
            wires.send(block, block, here.near(a, way), (p, "m1", way))
    for p in range(3):
        pass_on(p, 0, 0)
    for p, (a, b, s) in enumerate(ORDERS):
        table = seen.at[p, here.at[b], here.along(a, -1)]
        wires.arrived(table, (p, "t1", 1), here.near(a, -1))
        wires.send(table, table, here.near(a, 1), (p, "t1far"))
        wires.arrived(
            seen.at[p, here.at[b], here.along(a, 1)], (p, "t1", -1), here.near(a, 1)
        )
    for p, (a, b, s) in enumerate(ORDERS):
        for way, rows in ((1, pl.ds(0, half)), (-1, pl.ds(half, half))):
            block = held[p].at[here.at[b], here.along(a, -way)]
            wires.arrived(block, (p, "m1", way), here.near(a, -way))
            piece = held[p].at[here.at[b], here.along(a, -way), rows]
            wires.send(piece, piece, here.near(a, way), (p, "m1far", way))
    for p, (a, b, s) in enumerate(ORDERS):
        wires.arrived(
            seen.at[p, here.at[b], here.along(a, 2)], (p, "t1far"), here.near(a, -1)
        )
        table = seen.at[p, here.at[b]]
        for way in (1, -1):
            wires.send(table, table, here.near(b, way), (p, "t2", way))
    for p in range(3):
        pass_on(p, 1, -1)
        pass_on(p, 2, 1)
    for p, (a, b, s) in enumerate(ORDERS):
        table = seen.at[p, here.along(b, -1)]
        wires.arrived(table, (p, "t2", 1), here.near(b, -1))
        wires.send(table, table, here.near(b, 1), (p, "t2far"))
        wires.arrived(seen.at[p, here.along(b, 1)], (p, "t2", -1), here.near(b, 1))
    for p, (a, b, s) in enumerate(ORDERS):
        for way, rows in ((1, pl.ds(0, half)), (-1, pl.ds(half, half))):
            piece = held[p].at[here.at[b], here.along(a, 2), rows]
            wires.arrived(piece, (p, "m1far", way), here.near(a, -way))
        pass_on(p, 3, 2)

    def select(p, k, b_step):
        a, b, s = ORDERS[p]
        b_index = here.along(b, b_step)
        line = here.at[b] * RING + here.at[a]
        size = parts[p][1]

        def one(a_index, carry):
            token_of = line_row(seen[p, b_index, a_index, pl.ds(0, 16), :], line)
            token = lax.broadcasted_iota(jnp.int32, (tokens, LANES), 0).astype(jnp.float32)
            pick = jnp.where(token == token_of, 1.0, 0.0).astype(jnp.bfloat16)
            rows = lax.dot_general(
                pick,
                held[p][b_index, a_index],
                (((0,), (0,)), ((), ())),
                preferred_element_type=jnp.float32,
            )
            outgoing[p][k, :, a_index] = rows.astype(jnp.bfloat16).reshape(8, 16, size)
            return carry

        lax.fori_loop(0, RING, one, 0)

    def deliver(p, k, b_step):
        order = ORDERS[p]
        a, b, s = order
        start, size = parts[p]
        b_index = here.along(b, b_step)
        mine = slots_of(slots, order, b_index, here.at[s], here.core, start, size)
        way = 1 if k % 2 == 0 else -1
        wires.send(
            outgoing[p].at[k, pl.ds(here.along(s, 2) * 2, 2)],
            relay[p].at[k],
            here.near(s, way),
            (p, "relay", k),
        )
        for step in (1, -1):
            for other in (0, 1):
                core = 1 - here.core if other else here.core
                wires.send(
                    outgoing[p].at[k, here.along(s, step) * 2 + core],
                    mine,
                    here.near(s, step, other),
                    (p, "near", step, other, k),
                )
        wires.send(
            outgoing[p].at[k, here.at[s] * 2 + (1 - here.core)],
            mine,
            here.partner(),
            (p, "chip", k),
        )
        keep(outgoing[p].at[k, here.at[s] * 2 + here.core], mine)

    def forward(p, k, b_step):
        order = ORDERS[p]
        a, b, s = order
        start, size = parts[p]
        b_index = here.along(b, b_step)
        way = 1 if k % 2 == 0 else -1
        wires.arrived(relay[p].at[k], (p, "relay", k), here.near(s, -way))
        theirs = slots_of(slots, order, b_index, here.along(s, -way), here.core, start, size)
        for other in (0, 1):
            core = 1 - here.core if other else here.core
            wires.send(
                relay[p].at[k, core], theirs, here.near(s, way, other), (p, "far", other, k)
            )

    def received(p, k, b_step):
        order = ORDERS[p]
        a, b, s = order
        start, size = parts[p]
        b_index = here.along(b, b_step)
        way = 1 if k % 2 == 0 else -1
        for other in (0, 1):
            core = 1 - here.core if other else here.core
            for step in (1, -1):
                wires.arrived(
                    slots_of(slots, order, b_index, here.along(s, -step), core, start, size),
                    (p, "near", step, other, k),
                    here.near(s, -step, other),
                )
            wires.arrived(
                slots_of(slots, order, b_index, here.along(s, 2), core, start, size),
                (p, "far", other, k),
                here.near(s, -way, other),
            )
        wires.arrived(
            slots_of(slots, order, b_index, here.at[s], 1 - here.core, start, size),
            (p, "chip", k),
            here.partner(),
        )

    def batch_copy(p, k):
        start, size = parts[p]
        b_index = here.along(ORDERS[p][1], turns[k])
        slot = (k * 3 + p) % 2
        return pltpu.make_async_copy(
            slots.at[(*fixed_b(ORDERS[p], b_index), slice(None), slice(None), pl.ds(start, size))],
            batch.at[slot, :, :, :, :, pl.ds(0, size)],
            bs.at[slot],
        )

    def ready(p, k):
        received(p, k, turns[k])
        local[6 + k * 3 + p].wait()
        batch_copy(p, k).start()

    def project(p, k):
        start, size = parts[p]
        b_index = here.along(ORDERS[p][1], turns[k])
        slot = (k * 3 + p) % 2
        batch_copy(p, k).wait()
        where = fixed_b(ORDERS[p], b_index)

        def tile(n, carry):
            units = pl.ds(pl.multiple_of(n * 256, 256), 256)
            term = lax.dot_general(
                batch[slot, :, :, :, :, pl.ds(0, size)].reshape(512, size),
                weight[units, pl.ds(start, size)],
                (((1,), (1,)), ((), ())),
                preferred_element_type=jnp.float32,
            )
            there = (*where, slice(None), slice(None), units)
            upstream[there] = upstream[there] + term.reshape(RING, RING, 2, 16, 256)
            return carry

        lax.fori_loop(0, 3, tile, 0)

    turns = (0, -1, 1, 2)
    for p in range(3):
        relay_on(p, 0, 0)
    for p in range(3):
        select(p, 0, 0)
        deliver(p, 0, 0)
    for k, step in ((1, -1), (2, 1), (3, 2)):
        for p in range(3):
            relay_on(p, k, step)
    for k in (1, 2):
        for p in range(3):
            select(p, k, turns[k])
            deliver(p, k, turns[k])
    for p in range(3):
        forward(p, 0, 0)
    for p in range(3):
        for k, step in ((0, 0), (1, -1), (2, 1), (3, 2)):
            far_in(p, k, step)
    for p, (a, b, s) in enumerate(ORDERS):
        wires.arrived(seen.at[p, here.along(b, 2)], (p, "t2far"), here.near(b, -1))
    for p in range(3):
        select(p, 3, 2)
        deliver(p, 3, 2)
    maps_out[...] = seen[...]
    upstream[...] = jnp.zeros_like(upstream)
    fetch.wait()
    for p in range(3):
        forward(p, 1, turns[1])
    work = [(k, p) for k in range(4) for p in range(3)]
    ready(work[0][1], work[0][0])
    for turn, (k, p) in enumerate(work):
        if turn + 1 < len(work):
            after_k, after_p = work[turn + 1]
            if after_p == 0 and after_k < 3:
                for q in range(3):
                    forward(q, after_k + 1, turns[after_k + 1])
            ready(after_p, after_k)
        project(p, k)
    wires.drain()


def dispatch(parts, grad, maps, down):
    tokens, width = grad.shape
    rows = [pltpu.VMEM((RING, RING, tokens, size), jnp.bfloat16) for _, size in parts]
    outs = [pltpu.VMEM((RING, 8, RING, 16, size), jnp.bfloat16) for _, size in parts]
    relays = [pltpu.VMEM((RING, 2, RING, 16, size), jnp.bfloat16) for _, size in parts]
    table = (3, RING, RING, maps.shape[1], LANES)
    units = down.shape[0]
    return pl.pallas_call(
        functools.partial(dispatch_kernel, parts),
        out_shape=(
            jax.ShapeDtypeStruct((RING, RING, RING, 2, 16, width), jnp.bfloat16),
            jax.ShapeDtypeStruct(table, jnp.bfloat16),
            jax.ShapeDtypeStruct((RING, RING, RING, 2, 16, units), jnp.float32),
        ),
        in_specs=[pl.BlockSpec(memory_space=pltpu.HBM)] * 3,
        out_specs=(
            pl.BlockSpec(memory_space=pltpu.HBM),
            pl.BlockSpec(memory_space=pltpu.VMEM),
            pl.BlockSpec(memory_space=pltpu.VMEM),
        ),
        scratch_shapes=rows
        + outs
        + relays
        + [
            pltpu.VMEM(table, jnp.bfloat16),
            pltpu.VMEM((units, width), jnp.bfloat16),
            pltpu.VMEM((2, RING, RING, 2, 16, parts[0][1]), jnp.bfloat16),
            pltpu.SemaphoreType.DMA((192,)),
            pltpu.SemaphoreType.DMA((192,)),
            pltpu.SemaphoreType.DMA((32,)),
            pltpu.SemaphoreType.DMA((3,)),
        ],
        compiler_params=pltpu.CompilerParams(
            collective_id=0, has_side_effects=True, vmem_limit_bytes=60 * 2**20
        ),
    )(grad, maps, down)


def combine_kernel(
    parts, values, grad_first, grad_second, w_gate, w_up, tables, inputs, router,
    probs, gates, place, scale, ids, aux,
    out, combine_grad, router_grad, back,
    q0, q1, q2, l0, l1, l2, x0, x1, x2, y0, y1, y2, u0, u1, u2, v0, v1, v2,
    gate, up, stage, given, h1, h2, h3, flat, logit_grad, terms, other_terms,
    e10, e11, e12, e20, e21, e22, e30, e31, e32, ss, rs, ls, bs,
):
    rows, relay = (q0, q1, q2), (l0, l1, l2)
    halves2, whole2 = (x0, x1, x2), (y0, y1, y2)
    halves1, whole1 = (u0, u1, u2), (v0, v1, v2)
    sums = ((e10, e11, e12), (e20, e21, e22), (e30, e31, e32))
    bands = ((0, 16), (16, 8), (24, 8))
    steps = (1, -1, 2)
    here = Place()
    wires = Wires(ss, rs)
    tokens = out.shape[0]
    local = []
    fetches = []
    for p, (start, size) in enumerate(parts):
        for n, (src, dst) in enumerate(((w_gate, gate), (w_up, up))):
            span = pl.ds(start, size)
            copy = pltpu.make_async_copy(src.at[span], dst.at[span], bs.at[6 + 2 * p + n])
            copy.start()
            fetches.append(copy)

    def given_copies(p, k, b_step):
        slot = (k * 3 + p) % 2
        where = fixed_b(ORDERS[p], here.along(ORDERS[p][1], b_step))
        return [
            pltpu.make_async_copy(src.at[where], given.at[slot, n], bs.at[2 + 2 * slot + n])
            for n, src in enumerate((grad_first, grad_second))
        ]

    for copy in given_copies(0, 0, 2):
        copy.start()
    here.greet(steps)

    def values_line():
        mine = here.at[2] * 2 + here.core
        h1[mine] = values[:, :, here.at[2], here.core]
        for step in (0, *steps):
            for other in (0, 1):
                if step or other:
                    core = 1 - here.core if other else here.core
                    wires.send(
                        values.at[:, :, here.along(2, step), core],
                        h1.at[mine],
                        here.near(2, step, other),
                        ("v1", step, other),
                    )

    def values_x():
        for step in (0, *steps):
            for other in (0, 1):
                if step or other:
                    core = 1 - here.core if other else here.core
                    wires.arrived(
                        h1.at[here.along(2, -step) * 2 + core],
                        ("v1", step, other),
                        here.near(2, -step, other),
                    )
        h2[here.at[1]] = h1[:, :, here.at[1]]
        for step in steps:
            wires.send(
                h1.at[:, :, here.along(1, step)],
                h2.at[here.at[1]],
                here.near(1, step),
                ("v2", step),
            )

    def values_z():
        for step in steps:
            wires.arrived(h2.at[here.along(1, -step)], ("v2", step), here.near(1, -step))
        h3[here.at[0]] = h2[:, :, here.at[0]]
        for step in steps:
            wires.send(
                h2.at[:, :, here.along(0, step)],
                h3.at[here.at[0]],
                here.near(0, step),
                ("v3", step),
            )

    def router_back():
        for step in steps:
            wires.arrived(h3.at[here.along(0, -step)], ("v3", step), here.near(0, -step))

        def one_expert(e, carry):
            flat[pl.ds(e, 1), :] = h3[e // 32, (e // 8) % 4, e % 8]
            return carry

        lax.fori_loop(0, flat.shape[0], one_expert, 0)
        by_slot = flat[...].T
        dense = jnp.zeros_like(by_slot)
        for j in range(16):
            dense = dense + jnp.where(place[...] == j, by_slot[j : j + 1], 0.0)
        lane = lax.broadcasted_iota(jnp.int32, dense.shape, 1)
        column = lax.broadcasted_iota(jnp.int32, combine_grad.shape, 1)
        picked = jnp.zeros(combine_grad.shape, jnp.float32)
        for k in range(combine_grad.shape[1]):
            value = jnp.sum(
                jnp.where(lane == ids[:, k : k + 1], dense, 0.0), axis=1, keepdims=True
            )
            picked = picked + jnp.where(column == k, value, 0.0)
        combine_grad[...] = picked
        inner = jnp.sum(gates[...] * dense, axis=1, keepdims=True)
        prob_grad = jnp.where(place[...] >= 0, (dense - inner) / scale[...], 0.0)
        counts = jnp.sum(tables[0, :, :, pl.ds(32, 16), :].astype(jnp.float32), axis=(0, 1))
        counts = jnp.sum(counts, axis=0, keepdims=True)
        top = combine_grad.shape[1]
        fraction = dense.shape[1] * counts / (top * tokens * RING * RING)
        prob_grad = prob_grad + aux[0] * fraction
        mean = jnp.sum(probs[...] * prob_grad, axis=1, keepdims=True)
        logit_grad[...] = (probs[...] * (prob_grad - mean)).astype(jnp.bfloat16)

        def one_tile(n, carry):
            columns = pl.ds(pl.multiple_of(n * LANES, LANES), LANES)
            term = lax.dot_general(
                inputs[:, columns],
                logit_grad[...],
                (((0,), (0,)), ((), ())),
                preferred_element_type=jnp.float32,
            )
            for m in range(2):
                for core in range(2):
                    terms[core, n // 8, (n // 2) % 4, 2 * (n % 2) + m] = term[
                        64 * m + 32 * core : 64 * m + 32 * core + 32
                    ]
            return carry

        lax.fori_loop(0, inputs.shape[1] // LANES, one_tile, 0)
        wires.send(terms.at[1 - here.core], other_terms, here.partner(), ("r0",))

    def chip_sum():
        wires.arrived(other_terms, ("r0",), here.partner())

        def one(n, carry):
            z, x = n // RING, n % RING
            terms[here.core, z, x] = terms[here.core, z, x] + other_terms[z, x]
            return carry

        lax.fori_loop(0, RING * RING, one, 0)

    def band_of(q, level, coordinate):
        where = [slice(None)] * 3
        for axis in ORDERS[q][:level]:
            where[axis] = here.at[axis]
        where[ORDERS[q][level]] = coordinate
        return (here.core, *where, pl.ds(*bands[q]), slice(None))

    def sum_send(level):
        for q in range(3):
            axis = ORDERS[q][level]
            for n, step in enumerate(steps):
                wires.send(
                    terms.at[band_of(q, level, here.along(axis, step))],
                    sums[level][q].at[n],
                    here.near(axis, step),
                    ("r", level, q, step),
                )

    def sum_in(level):
        for q in range(3):
            axis = ORDERS[q][level]
            for n, step in enumerate(steps):
                wires.arrived(
                    sums[level][q].at[n], ("r", level, q, step), here.near(axis, -step)
                )
            own = band_of(q, level, here.at[axis])
            landed = sums[level][q]
            terms[own] = terms[own] + landed[0] + landed[1] + landed[2]

    def sum_out():
        for q in range(3):
            span = pl.ds(*bands[q])
            router_grad[span] = terms[here.core, here.at[0], here.at[1], here.at[2], span]

    def stage_copy(p, k, b_step):
        start, size = parts[p]
        b_index = here.along(ORDERS[p][1], b_step)
        slot = (k * 3 + p) % 2
        return pltpu.make_async_copy(
            stage.at[slot, :, :, :, :, pl.ds(0, size)],
            back.at[(*fixed_b(ORDERS[p], b_index), slice(None), slice(None), pl.ds(start, size))],
            bs.at[slot],
        )

    def produce(p, k, b_step):
        start, size = parts[p]
        b_index = here.along(ORDERS[p][1], b_step)
        slot = (k * 3 + p) % 2
        units = grad_first.shape[-1]
        if k == 0:
            fetches[2 * p].wait()
            fetches[2 * p + 1].wait()
        for copy in given_copies(p, k, b_step):
            copy.wait()

        def columns(offset, width):
            span = pl.ds(start + offset, width)
            total = 0.0
            for n, weight in enumerate((gate, up)):
                total = total + lax.dot_general(
                    given[slot, n].reshape(512, units),
                    weight[span],
                    (((1,), (1,)), ((), ())),
                    preferred_element_type=jnp.float32,
                )
            stage[slot, :, :, :, :, pl.ds(offset, width)] = total.astype(jnp.bfloat16).reshape(
                RING, RING, 2, 16, width
            )

        def tile(n, carry):
            columns(pl.multiple_of(n * 256, 256), 256)
            return carry

        lax.fori_loop(0, size // 256, tile, 0)
        if size % 256:
            columns(size // 256 * 256, size % 256)
        stage_copy(p, k, b_step).start()

    def pieces(p, b_index, s_index, c_index):
        start, size = parts[p]
        return slots_of(back, ORDERS[p], b_index, s_index, c_index, start, size)

    def give(p, k, b_step):
        a, b, s = ORDERS[p]
        b_index = here.along(b, b_step)
        mine = rows[p].at[b_index, :, here.at[s] * 2 + here.core]
        way = 1 if k % 2 == 0 else -1
        wires.send(
            pieces(p, b_index, here.along(s, 2), slice(None)),
            relay[p].at[k],
            here.near(s, way),
            (p, "relay", k),
        )
        for step in (1, -1):
            for other in (0, 1):
                core = 1 - here.core if other else here.core
                wires.send(
                    pieces(p, b_index, here.along(s, step), core),
                    mine,
                    here.near(s, step, other),
                    (p, "near", step, other, k),
                )
        wires.send(
            pieces(p, b_index, here.at[s], 1 - here.core), mine, here.partner(), (p, "chip", k)
        )
        copy = pltpu.make_async_copy(
            pieces(p, b_index, here.at[s], here.core), mine, ls.at[len(local)]
        )
        copy.start()
        local.append(copy)

    def forward(p, k, b_step):
        a, b, s = ORDERS[p]
        b_index = here.along(b, b_step)
        way = 1 if k % 2 == 0 else -1
        wires.arrived(relay[p].at[k], (p, "relay", k), here.near(s, -way))
        theirs = rows[p].at[b_index, :, here.along(s, -way) * 2 + here.core]
        for other in (0, 1):
            core = 1 - here.core if other else here.core
            wires.send(
                relay[p].at[k, :, core], theirs, here.near(s, way, other), (p, "far", other, k)
            )

    def gathered(p, k, b_step):
        a, b, s = ORDERS[p]
        b_index = here.along(b, b_step)
        way = 1 if k % 2 == 0 else -1
        for other in (0, 1):
            core = 1 - here.core if other else here.core
            for step in (1, -1):
                wires.arrived(
                    rows[p].at[b_index, :, here.along(s, -step) * 2 + core],
                    (p, "near", step, other, k),
                    here.near(s, -step, other),
                )
            wires.arrived(
                rows[p].at[b_index, :, here.along(s, 2) * 2 + core],
                (p, "far", other, k),
                here.near(s, -way, other),
            )
        wires.arrived(
            rows[p].at[b_index, :, here.at[s] * 2 + (1 - here.core)],
            (p, "chip", k),
            here.partner(),
        )
        local[k * 3 + p].wait()

    def add_up(p, b_step):
        a, b, s = ORDERS[p]
        b_index = here.along(b, b_step)
        line = here.at[b] * RING + here.at[a]
        size = parts[p][1]

        def one(a_index, carry):
            token_of = line_row(tables[p, b_index, a_index, pl.ds(0, 16), :], line)
            gate_of = line_row(tables[p, b_index, a_index, pl.ds(16, 16), :], line)
            token = lax.broadcasted_iota(jnp.int32, (tokens, LANES), 0).astype(jnp.float32)
            weigh = jnp.where(token == token_of, gate_of, 0.0).astype(jnp.bfloat16)
            total = jnp.dot(
                weigh,
                rows[p][b_index, a_index].reshape(LANES, size),
                preferred_element_type=jnp.float32,
            )
            rows[p][b_index, a_index] = total.astype(jnp.bfloat16).reshape(8, 16, size)
            return carry

        lax.fori_loop(0, RING, one, 0)

    def plus(*terms):
        total = terms[0].astype(jnp.float32)
        for term in terms[1:]:
            total = total + term.astype(jnp.float32)
        return total

    def fold2(p, way):
        a, b, s = ORDERS[p]
        b_index = here.along(b, way)
        slot = 0 if way == 1 else 1
        groups = pl.ds(0, 4) if way == 1 else pl.ds(4, 4)
        wires.arrived(halves2[p].at[slot], (p, "half2", way), here.near(b, -way))

        def one(a_index, carry):
            rows[p][b_index, a_index, groups] = plus(
                rows[p][b_index, a_index, groups], halves2[p][slot, a_index]
            ).astype(jnp.bfloat16)
            return carry

        lax.fori_loop(0, RING, one, 0)
        for k, step in enumerate((2, 1, -1, 0)):
            wires.send(
                rows[p].at[b_index, here.along(a, step)],
                whole2[p].at[slot, k],
                here.near(b, way),
                (p, "whole2", way, k),
            )

    def settle2(p, k, step):
        a, b, s = ORDERS[p]
        for way in (1, -1):
            slot = 0 if way == 1 else 1
            wires.arrived(whole2[p].at[slot, k], (p, "whole2", way, k), here.near(b, -way))
        own = rows[p].at[here.at[b], here.along(a, step)]
        return plus(own[...], whole2[p][0, k], whole2[p][1, k])

    order = (2, 1, -1, 0)
    work = [(k, p) for k in range(4) for p in range(3)]
    values_line()
    between = {2: values_x, 4: values_z, 6: router_back, 8: chip_sum}
    for turn in range(len(work) + 1):
        if turn < len(work):
            k, p = work[turn]
            if turn + 1 < len(work):
                after_k, after_p = work[turn + 1]
                for copy in given_copies(after_p, after_k, order[after_k]):
                    copy.start()
            produce(p, k, order[k])
        if turn > 0:
            k, p = work[turn - 1]
            stage_copy(p, k, order[k]).wait()
            give(p, k, order[k])
            if p == 2 and k > 0:
                for q in range(3):
                    forward(q, k - 1, order[k - 1])
        if turn in between:
            between[turn]()
        if turn == 8:
            sum_send(0)
    for p, (a, b, s) in enumerate(ORDERS):
        gathered(p, 0, 2)
        add_up(p, 2)
        far = here.along(b, 2)
        for way, groups in ((1, pl.ds(0, 4)), (-1, pl.ds(4, 4))):
            wires.send(
                rows[p].at[far, :, groups],
                halves2[p].at[0 if way == 1 else 1],
                here.near(b, way),
                (p, "half2", way),
            )
    for q in range(3):
        forward(q, 3, order[3])
    for k, way in ((1, 1), (2, -1)):
        for p in range(3):
            gathered(p, k, way)
            add_up(p, way)
            fold2(p, way)
        sum_in(k - 1)
        sum_send(k)
    for p in range(3):
        gathered(p, 3, 0)
        add_up(p, 0)
    for p, (a, b, s) in enumerate(ORDERS):
        block = rows[p].at[here.at[b], here.along(a, 2)]
        block[...] = settle2(p, 0, 2).astype(jnp.bfloat16)
        for way, groups in ((1, pl.ds(0, 4)), (-1, pl.ds(4, 4))):
            wires.send(
                rows[p].at[here.at[b], here.along(a, 2), groups],
                halves1[p].at[0 if way == 1 else 1],
                here.near(a, way),
                (p, "half1", way),
            )
    for k, way in ((1, 1), (2, -1)):
        for p, (a, b, s) in enumerate(ORDERS):
            slot = 0 if way == 1 else 1
            groups = pl.ds(0, 4) if way == 1 else pl.ds(4, 4)
            block = rows[p].at[here.at[b], here.along(a, way)]
            block[...] = settle2(p, k, way).astype(jnp.bfloat16)
            wires.arrived(halves1[p].at[slot], (p, "half1", way), here.near(a, -way))
            part = rows[p].at[here.at[b], here.along(a, way), groups]
            part[...] = plus(part[...], halves1[p][slot]).astype(jnp.bfloat16)
            wires.send(block, whole1[p].at[slot], here.near(a, way), (p, "whole1", way))
    for p, (a, b, s) in enumerate(ORDERS):
        start, size = parts[p]
        total = settle2(p, 3, 0)
        for way in (1, -1):
            slot = 0 if way == 1 else 1
            wires.arrived(whole1[p].at[slot], (p, "whole1", way), here.near(a, -way))
        total = plus(total, whole1[p][0], whole1[p][1]).reshape(tokens, size)
        total = total + lax.dot_general(
            logit_grad[...],
            router[pl.ds(start, size)],
            (((1,), (1,)), ((), ())),
            preferred_element_type=jnp.float32,
        )
        out[:, pl.ds(start, size)] = total.astype(out.dtype)
    sum_in(2)
    sum_out()
    wires.drain()


def combine(parts, values, grads, weights, tables, inputs, router, probs, gates, place, scale, ids, aux):
    width, units = weights[0].shape
    tokens, top = ids.shape
    experts = probs.shape[1]

    def buffers(*lead):
        return [pltpu.VMEM((*lead, size), jnp.bfloat16) for _, size in parts]

    def floats(*shape):
        return pltpu.VMEM(shape, jnp.float32)

    hbm, vmem = pl.BlockSpec(memory_space=pltpu.HBM), pl.BlockSpec(memory_space=pltpu.VMEM)
    bands = (16, 8, 8)
    return pl.pallas_call(
        functools.partial(combine_kernel, parts),
        out_shape=(
            jax.ShapeDtypeStruct((tokens, width), jnp.bfloat16),
            jax.ShapeDtypeStruct((tokens, top), jnp.float32),
            jax.ShapeDtypeStruct((width // (2 * RING**3), experts), jnp.float32),
            jax.ShapeDtypeStruct((RING, RING, RING, 2, 16, width), jnp.bfloat16),
        ),
        in_specs=[vmem, hbm, hbm, hbm, hbm]
        + [vmem] * 8
        + [pl.BlockSpec(memory_space=pltpu.SMEM)],
        out_specs=(vmem, vmem, vmem, hbm),
        scratch_shapes=buffers(RING, RING, 8, 16)
        + buffers(RING, RING, 2, 16)
        + buffers(2, RING, 4, 16)
        + buffers(2, RING, 8, 16)
        + buffers(2, 4, 16)
        + buffers(2, 8, 16)
        + [
            pltpu.VMEM((width, units), jnp.bfloat16),
            pltpu.VMEM((width, units), jnp.bfloat16),
            pltpu.VMEM((2, RING, RING, 2, 16, parts[0][1]), jnp.bfloat16),
            pltpu.VMEM((2, 2, RING, RING, 2, 16, units), jnp.bfloat16),
            floats(8, RING, RING, 1, LANES),
            floats(RING, 8, RING, 1, LANES),
            floats(RING, RING, 8, 1, LANES),
            floats(experts, LANES),
            pltpu.VMEM((tokens, experts), jnp.bfloat16),
            floats(2, RING, RING, RING, 32, experts),
            floats(RING, RING, RING, 32, experts),
        ]
        + [floats(3, RING, RING, band, experts) for band in bands]
        + [floats(3, RING, band, experts) for band in bands]
        + [floats(3, band, experts) for band in bands]
        + [
            pltpu.SemaphoreType.DMA((224,)),
            pltpu.SemaphoreType.DMA((224,)),
            pltpu.SemaphoreType.DMA((16,)),
            pltpu.SemaphoreType.DMA((12,)),
        ],
        compiler_params=pltpu.CompilerParams(
            collective_id=1, has_side_effects=True, vmem_limit_bytes=67043328
        ),
    )(values, *grads, *weights, tables, inputs, router, probs, gates, place, scale, ids, aux)[:3]


def hidden_backward(upstream, pre_gate, pre_up):
    first = pre_gate.astype(jnp.float32)
    second = pre_up.astype(jnp.float32)
    gate_sig = jax.nn.sigmoid(first)
    gate_act = first * gate_sig
    hidden = gate_act * second
    slot_combine = jnp.sum(upstream * hidden, axis=-1).astype(jnp.bfloat16)
    grad_first = (upstream * second * gate_sig * (1.0 + first * (1.0 - gate_sig))).astype(
        jnp.bfloat16
    )
    grad_second = (upstream * gate_act).astype(jnp.bfloat16)
    return grad_first, grad_second, slot_combine


def shards(
    tokens,
    out_grad,
    router_weight,
    gate_weight,
    up_weight,
    down_weight,
    saved_gate,
    saved_up,
    expert_ids,
    aux_weight,
):
    devices = lax.axis_size(AXES)
    inputs, upstream_grad, chosen_ids = tokens[0], out_grad[0], expert_ids[0]
    tok_rows = chosen_ids.shape[0]
    model_width = inputs.shape[1]
    experts = router_weight.shape[1]
    capacity = saved_gate.shape[1] // devices
    parts = column_parts(model_width)

    logits = jnp.dot(inputs, router_weight, preferred_element_type=jnp.float32)
    probs = jax.nn.softmax(logits, axis=-1)
    expert = jnp.arange(experts, dtype=jnp.int32)
    mask = jnp.sum((chosen_ids[:, :, None] == expert).astype(jnp.float32), axis=1)
    chosen_sum = jnp.sum(probs * mask, axis=1, keepdims=True)
    gates = probs * mask / chosen_sum
    position = jnp.arange(tok_rows)
    before = (position[:, None] > position[None, :]).astype(jnp.bfloat16)
    slot_pos = jnp.dot(before, mask.astype(jnp.bfloat16), preferred_element_type=jnp.float32)
    slot = jnp.arange(capacity, dtype=jnp.float32)
    filled = jnp.where(
        (slot_pos[:, None, :] == slot[None, :, None]) & (mask[:, None, :] > 0), 1.0, 0.0
    )
    offset = (position - tok_rows).astype(jnp.float32)
    slot_token = jnp.sum(filled * offset[:, None, None], axis=0) + tok_rows
    slot_gate = jnp.sum(filled * gates[:, None, :], axis=0)
    counts = jnp.pad(jnp.sum(mask, axis=0, keepdims=True), ((0, capacity - 1), (0, 0)))
    tables = []
    for a, b, s in ORDERS:
        both = jnp.stack([slot_token, slot_gate]).reshape(2, capacity, RING, RING, RING, 2)
        both = both.transpose(0, 2 + b, 2 + a, 2 + s, 5, 1)
        tables.append(jnp.concatenate([both.reshape(2 * RING * RING, LANES), counts]))
    tables = jnp.stack(tables).astype(jnp.bfloat16)

    _, seen, upstream = dispatch(parts, upstream_grad, tables, down_weight[0])
    grad_first, grad_second, slot_combine = hidden_backward(
        upstream,
        saved_gate[0].reshape(upstream.shape),
        saved_up[0].reshape(upstream.shape),
    )
    values = slot_combine.astype(jnp.float32).reshape(*upstream.shape[:4], 1, capacity)
    values = jnp.pad(values, [(0, 0)] * 5 + [(0, LANES - capacity)])
    token_grad, combine_grad, router_grad = combine(
        parts,
        values,
        (grad_first, grad_second),
        (gate_weight[0], up_weight[0]),
        seen,
        inputs,
        router_weight,
        probs,
        gates,
        jnp.where(mask > 0, slot_pos, -1.0),
        chosen_sum,
        chosen_ids,
        aux_weight,
    )
    return (token_grad[None], combine_grad[None], router_grad)


def solution(mesh):
    torus = Mesh(mesh.devices.reshape(RING, RING, RING, 2), AXES)
    return jax.shard_map(
        shards,
        mesh=torus,
        in_specs=(
            P(EXP, SEQ, None),
            P(EXP, SEQ, None),
            P(),
            P(AXES, None, None),
            P(AXES, None, None),
            P(AXES, None, None),
            P(AXES, None, None),
            P(AXES, None, None),
            P(EXP, SEQ, None),
            P(),
        ),
        out_specs=(P(EXP, SEQ, None), P(EXP, SEQ, None), P(AXES, None)),
        check_vma=False,
    )
```

```python
import functools

import jax
import jax.numpy as jnp
from jax import lax
from jax.experimental import pallas as pl
from jax.experimental.pallas import tpu as pltpu
from jax.sharding import Mesh
from jax.sharding import PartitionSpec as P

SEQ = ("seq_0", "seq_1")
EXP = ("exp_0", "exp_1")
AXES = ("seq_0", "seq_1", "exp_0", "exp_1")
MESH = pl.DeviceIdType.MESH
RING = 4
LANES = 128
ORDERS = ((0, 1, 2), (1, 2, 0), (2, 0, 1))
STRIDES = (32, 8, 2)


def column_parts(width):
    tiles = width // LANES
    sizes = [(tiles + 2 - p) // 3 * LANES for p in range(3)]
    starts = [0, sizes[0], sizes[0] + sizes[1]]
    return list(zip(starts, sizes))


class Wires:
    def __init__(self, send_sems, recv_sems):
        self.send_sems, self.recv_sems = send_sems, recv_sems
        self.sent, self.names = [], {}

    def slot(self, name):
        return self.recv_sems.at[self.names.setdefault(name, len(self.names))]

    def send(self, src, dst, device, name):
        copy = pltpu.make_async_remote_copy(
            src, dst, self.send_sems.at[len(self.sent)], self.slot(name), device, MESH
        )
        copy.start()
        self.sent.append(copy)

    def arrived(self, ref, name, device):
        pltpu.make_async_remote_copy(
            ref, ref, self.send_sems.at[0], self.slot(name), device, MESH
        ).wait_recv()

    def drain(self):
        for copy in self.sent:
            copy.wait_send()


class Place:
    def __init__(self):
        self.at = [lax.axis_index(name) for name in AXES]
        self.core = self.at[3]

    def along(self, axis, step):
        return lax.rem(self.at[axis] + (step + RING), RING)

    def near(self, axis, step, other_core=0):
        coords = list(self.at)
        coords[axis] = self.along(axis, step)
        if other_core:
            coords[3] = 1 - self.core
        return tuple(coords)

    def partner(self):
        return (self.at[0], self.at[1], self.at[2], 1 - self.core)

    def greet(self, steps=(1, -1)):
        barrier = pltpu.get_barrier_semaphore()
        peers = [self.partner()]
        for axis in range(3):
            for step in steps:
                for other in (0, 1):
                    peers.append(self.near(axis, step, other))
        for peer in peers:
            pl.semaphore_signal(barrier, inc=1, device_id=peer, device_id_type=MESH)
        pl.semaphore_wait(barrier, len(peers))


def slots_of(ref, order, b_index, s_index, c_index, start, size):
    a, b, s = order
    where = [None] * 3
    where[a], where[b], where[s] = slice(None), b_index, s_index
    return ref.at[where[0], where[1], where[2], c_index, :, pl.ds(start, size)]


def fixed_b(order, b_index):
    where = [slice(None)] * 3
    where[order[1]] = b_index
    return tuple(where)


def dispatch_kernel(
    parts, grad, inputs, router, ids, down,
    slots, upstream, lines, counts, probs, gates, place, scale,
    g0, g1, g2, o0, o1, o2, l0, l1, l2, seen, picks, tokens_in, router_in, weight, batch,
    ss, rs, ls, bs,
):
    held, outgoing, relay = (g0, g1, g2), (o0, o1, o2), (l0, l1, l2)
    here = Place()
    wires = Wires(ss, rs)
    tokens = grad.shape[0]
    half = tokens // 2
    local = []

    def keep(src, dst):
        copy = pltpu.make_async_copy(src, dst, ls.at[len(local)])
        copy.start()
        local.append(copy)

    for p, (a, b, s) in enumerate(ORDERS):
        start, size = parts[p]
        keep(grad.at[:, pl.ds(start, size)], held[p].at[here.at[b], here.at[a]])
    fetches = [
        pltpu.make_async_copy(src, dst, bs.at[2 + n])
        for n, (src, dst) in enumerate(((inputs, tokens_in), (router, router_in), (down, weight)))
    ]
    for copy in fetches:
        copy.start()
    here.greet()
    for copy in local:
        copy.wait()

    def pass_on(p, k, step):
        a, b, s = ORDERS[p]
        block = held[p].at[here.at[b], here.along(a, step)]
        wires.send(block, block, here.near(b, 1), (p, "m2", 1, k))
        wires.send(block, block, here.near(b, -1), (p, "m2", -1, k))

    def relay_on(p, k, step):
        a, b, s = ORDERS[p]
        for way, rows in ((1, pl.ds(0, half)), (-1, pl.ds(half, half))):
            block = held[p].at[here.along(b, -way), here.along(a, step)]
            wires.arrived(block, (p, "m2", way, k), here.near(b, -way))
            piece = held[p].at[here.along(b, -way), here.along(a, step), rows]
            wires.send(piece, piece, here.near(b, way), (p, "m2far", way, k))

    def far_in(p, k, step):
        a, b, s = ORDERS[p]
        for way, rows in ((1, pl.ds(0, half)), (-1, pl.ds(half, half))):
            piece = held[p].at[here.along(b, 2), here.along(a, step), rows]
            wires.arrived(piece, (p, "m2far", way, k), here.near(b, -way))

    def route():
        experts = router.shape[1]
        row = lax.broadcasted_iota(jnp.int32, (tokens, experts), 0)
        lane = lax.broadcasted_iota(jnp.int32, (tokens, experts), 1)
        mask = jnp.zeros((tokens, experts), jnp.float32)
        for k in range(ids.shape[1]):
            mask = mask + jnp.where(lane == ids[:, k : k + 1], 1.0, 0.0)
        before = jnp.where(row > lane, 1.0, 0.0).astype(jnp.bfloat16)
        rank = jnp.dot(before, mask.astype(jnp.bfloat16), preferred_element_type=jnp.float32)
        place[...] = jnp.where(mask > 0, rank, -1.0)
        logits = jnp.dot(tokens_in[...], router_in[...], preferred_element_type=jnp.float32)
        powers = jnp.exp(logits - jnp.max(logits, axis=1, keepdims=True))
        probs[...] = powers / jnp.sum(powers, axis=1, keepdims=True)
        chosen = probs[...] * mask
        scale[...] = jnp.sum(chosen, axis=1, keepdims=True)
        gates[...] = chosen / scale[...]
        slot = lax.broadcasted_iota(jnp.int32, (16, experts), 0)
        token_of = jnp.zeros((16, experts), jnp.float32)
        gate_of = jnp.zeros((16, experts), jnp.float32)
        offset = (row - tokens).astype(jnp.float32)
        for j in range(16):
            hit = place[...] == j
            token = jnp.sum(jnp.where(hit, offset, 0.0), axis=0, keepdims=True) + tokens
            gate = jnp.sum(jnp.where(hit, gates[...], 0.0), axis=0, keepdims=True)
            token_of = jnp.where(slot == j, token, token_of)
            gate_of = jnp.where(slot == j, gate, gate_of)
        count = jnp.where(slot == 0, jnp.sum(mask, axis=0, keepdims=True), 0.0)
        for p, (a, b, s) in enumerate(ORDERS):
            for n, part in enumerate((token_of, gate_of, count)):
                seen[p, here.at[b], here.at[a], pl.ds(16 * n, 16), :] = part.astype(jnp.bfloat16)
        for p, (a, b, s) in enumerate(ORDERS):
            first = here.at[a] * STRIDES[a] + here.at[b] * STRIDES[b]
            expert = first + lane // 32 * STRIDES[s] + lane // 16 % 2
            picks[p] = jnp.where(row == expert, 1.0, 0.0).astype(jnp.bfloat16)

    for p, (a, b, s) in enumerate(ORDERS):
        block = held[p].at[here.at[b], here.at[a]]
        for way in (1, -1):
            wires.send(block, block, here.near(a, way), (p, "m1", way))
    for copy in fetches[:2]:
        copy.wait()
    route()
    for p, (a, b, s) in enumerate(ORDERS):
        table = seen.at[p, here.at[b], here.at[a]]
        for way in (1, -1):
            wires.send(table, table, here.near(a, way), (p, "t1", way))
    for p in range(3):
        pass_on(p, 0, 0)
    for p, (a, b, s) in enumerate(ORDERS):
        table = seen.at[p, here.at[b], here.along(a, -1)]
        wires.arrived(table, (p, "t1", 1), here.near(a, -1))
        wires.send(table, table, here.near(a, 1), (p, "t1far"))
        wires.arrived(
            seen.at[p, here.at[b], here.along(a, 1)], (p, "t1", -1), here.near(a, 1)
        )
    for p, (a, b, s) in enumerate(ORDERS):
        for way, rows in ((1, pl.ds(0, half)), (-1, pl.ds(half, half))):
            block = held[p].at[here.at[b], here.along(a, -way)]
            wires.arrived(block, (p, "m1", way), here.near(a, -way))
            piece = held[p].at[here.at[b], here.along(a, -way), rows]
            wires.send(piece, piece, here.near(a, way), (p, "m1far", way))
    for p, (a, b, s) in enumerate(ORDERS):
        wires.arrived(
            seen.at[p, here.at[b], here.along(a, 2)], (p, "t1far"), here.near(a, -1)
        )
        table = seen.at[p, here.at[b]]
        for way in (1, -1):
            wires.send(table, table, here.near(b, way), (p, "t2", way))
    for p in range(3):
        pass_on(p, 1, -1)
        pass_on(p, 2, 1)
    for p, (a, b, s) in enumerate(ORDERS):
        table = seen.at[p, here.along(b, -1)]
        wires.arrived(table, (p, "t2", 1), here.near(b, -1))
        wires.send(table, table, here.near(b, 1), (p, "t2far"))
        wires.arrived(seen.at[p, here.along(b, 1)], (p, "t2", -1), here.near(b, 1))
    for p, (a, b, s) in enumerate(ORDERS):
        for way, rows in ((1, pl.ds(0, half)), (-1, pl.ds(half, half))):
            piece = held[p].at[here.at[b], here.along(a, 2), rows]
            wires.arrived(piece, (p, "m1far", way), here.near(a, -way))
        pass_on(p, 3, 2)

    def select(p, k, b_step):
        a, b, s = ORDERS[p]
        b_index = here.along(b, b_step)
        size = parts[p][1]
        found = jnp.dot(
            seen[p, b_index].reshape(RING * 48, LANES),
            picks[p],
            preferred_element_type=jnp.float32,
        ).reshape(RING, 3, 16, LANES)
        slot = lax.broadcasted_iota(jnp.int32, found.shape, 2)
        lane = lax.broadcasted_iota(jnp.int32, found.shape, 3)
        found = jnp.sum(jnp.where(slot == lane % 16, found, 0.0), axis=2)
        for a_index in range(RING):
            for n in range(2):
                lines[p, b_index, a_index, pl.ds(n, 1), :] = found[a_index, n : n + 1]

        def one(a_index, carry):
            token_of = lines[p, b_index, a_index, pl.ds(0, 1), :]
            token = lax.broadcasted_iota(jnp.int32, (tokens, LANES), 0).astype(jnp.float32)
            pick = jnp.where(token == token_of, 1.0, 0.0).astype(jnp.bfloat16)
            rows = lax.dot_general(
                pick,
                held[p][b_index, a_index],
                (((0,), (0,)), ((), ())),
                preferred_element_type=jnp.float32,
            )
            outgoing[p][k, :, a_index] = rows.astype(jnp.bfloat16).reshape(8, 16, size)
            return carry

        lax.fori_loop(0, RING, one, 0)

    def deliver(p, k, b_step):
        order = ORDERS[p]
        a, b, s = order
        start, size = parts[p]
        b_index = here.along(b, b_step)
        mine = slots_of(slots, order, b_index, here.at[s], here.core, start, size)
        way = 1 if k % 2 == 0 else -1
        wires.send(
            outgoing[p].at[k, pl.ds(here.along(s, 2) * 2, 2)],
            relay[p].at[k],
            here.near(s, way),
            (p, "relay", k),
        )
        for step in (1, -1):
            for other in (0, 1):
                core = 1 - here.core if other else here.core
                wires.send(
                    outgoing[p].at[k, here.along(s, step) * 2 + core],
                    mine,
                    here.near(s, step, other),
                    (p, "near", step, other, k),
                )
        wires.send(
            outgoing[p].at[k, here.at[s] * 2 + (1 - here.core)],
            mine,
            here.partner(),
            (p, "chip", k),
        )
        keep(outgoing[p].at[k, here.at[s] * 2 + here.core], mine)

    def forward(p, k, b_step):
        order = ORDERS[p]
        a, b, s = order
        start, size = parts[p]
        b_index = here.along(b, b_step)
        way = 1 if k % 2 == 0 else -1
        wires.arrived(relay[p].at[k], (p, "relay", k), here.near(s, -way))
        theirs = slots_of(slots, order, b_index, here.along(s, -way), here.core, start, size)
        for other in (0, 1):
            core = 1 - here.core if other else here.core
            wires.send(
                relay[p].at[k, core], theirs, here.near(s, way, other), (p, "far", other, k)
            )

    def received(p, k, b_step):
        order = ORDERS[p]
        a, b, s = order
        start, size = parts[p]
        b_index = here.along(b, b_step)
        way = 1 if k % 2 == 0 else -1
        for other in (0, 1):
            core = 1 - here.core if other else here.core
            for step in (1, -1):
                wires.arrived(
                    slots_of(slots, order, b_index, here.along(s, -step), core, start, size),
                    (p, "near", step, other, k),
                    here.near(s, -step, other),
                )
            wires.arrived(
                slots_of(slots, order, b_index, here.along(s, 2), core, start, size),
                (p, "far", other, k),
                here.near(s, -way, other),
            )
        wires.arrived(
            slots_of(slots, order, b_index, here.at[s], 1 - here.core, start, size),
            (p, "chip", k),
            here.partner(),
        )

    def batch_copy(p, k):
        start, size = parts[p]
        b_index = here.along(ORDERS[p][1], turns[k])
        slot = (k * 3 + p) % 2
        return pltpu.make_async_copy(
            slots.at[(*fixed_b(ORDERS[p], b_index), slice(None), slice(None), pl.ds(start, size))],
            batch.at[slot, :, :, :, :, pl.ds(0, size)],
            bs.at[slot],
        )

    def ready(p, k):
        received(p, k, turns[k])
        local[3 + k * 3 + p].wait()
        batch_copy(p, k).start()

    def project(p, k):
        start, size = parts[p]
        b_index = here.along(ORDERS[p][1], turns[k])
        slot = (k * 3 + p) % 2
        batch_copy(p, k).wait()
        where = fixed_b(ORDERS[p], b_index)

        def tile(n, carry):
            units = pl.ds(pl.multiple_of(n * 256, 256), 256)
            term = lax.dot_general(
                batch[slot, :, :, :, :, pl.ds(0, size)].reshape(512, size),
                weight[units, pl.ds(start, size)],
                (((1,), (1,)), ((), ())),
                preferred_element_type=jnp.float32,
            )
            there = (*where, slice(None), slice(None), units)
            upstream[there] = upstream[there] + term.reshape(RING, RING, 2, 16, 256)
            return carry

        lax.fori_loop(0, 3, tile, 0)

    turns = (0, -1, 1, 2)
    for p in range(3):
        relay_on(p, 0, 0)
    for p in range(3):
        select(p, 0, 0)
        deliver(p, 0, 0)
    for k, step in ((1, -1), (2, 1), (3, 2)):
        for p in range(3):
            relay_on(p, k, step)
    for k in (1, 2):
        for p in range(3):
            select(p, k, turns[k])
            deliver(p, k, turns[k])
    for p in range(3):
        forward(p, 0, 0)
    for p in range(3):
        for k, step in ((0, 0), (1, -1), (2, 1), (3, 2)):
            far_in(p, k, step)
    for p, (a, b, s) in enumerate(ORDERS):
        wires.arrived(seen.at[p, here.along(b, 2)], (p, "t2far"), here.near(b, -1))
    for p in range(3):
        select(p, 3, 2)
        deliver(p, 3, 2)
    total = jnp.sum(seen[0, :, :, pl.ds(32, 16), :].astype(jnp.float32), axis=(0, 1))
    counts[...] = jnp.sum(total, axis=0, keepdims=True)
    upstream[...] = jnp.zeros_like(upstream)
    fetches[2].wait()
    for p in range(3):
        forward(p, 1, turns[1])
    work = [(k, p) for k in range(4) for p in range(3)]
    ready(work[0][1], work[0][0])
    for turn, (k, p) in enumerate(work):
        if turn + 1 < len(work):
            after_k, after_p = work[turn + 1]
            if after_p == 0 and after_k < 3:
                for q in range(3):
                    forward(q, after_k + 1, turns[after_k + 1])
            ready(after_p, after_k)
        project(p, k)
    wires.drain()


def dispatch(parts, grad, inputs, router, ids, down):
    tokens, width = grad.shape
    units, experts = down.shape[0], router.shape[1]
    rows = [pltpu.VMEM((RING, RING, tokens, size), jnp.bfloat16) for _, size in parts]
    outs = [pltpu.VMEM((RING, 8, RING, 16, size), jnp.bfloat16) for _, size in parts]
    relays = [pltpu.VMEM((RING, 2, RING, 16, size), jnp.bfloat16) for _, size in parts]
    hbm, vmem = pl.BlockSpec(memory_space=pltpu.HBM), pl.BlockSpec(memory_space=pltpu.VMEM)
    square = jax.ShapeDtypeStruct((tokens, experts), jnp.float32)
    return pl.pallas_call(
        functools.partial(dispatch_kernel, parts),
        out_shape=(
            jax.ShapeDtypeStruct((RING, RING, RING, 2, 16, width), jnp.bfloat16),
            jax.ShapeDtypeStruct((RING, RING, RING, 2, 16, units), jnp.float32),
            jax.ShapeDtypeStruct((3, RING, RING, 8, LANES), jnp.float32),
            jax.ShapeDtypeStruct((1, experts), jnp.float32),
            square,
            square,
            square,
            jax.ShapeDtypeStruct((tokens, 1), jnp.float32),
        ),
        in_specs=[hbm, hbm, hbm, vmem, hbm],
        out_specs=(hbm,) + (vmem,) * 7,
        scratch_shapes=rows
        + outs
        + relays
        + [
            pltpu.VMEM((3, RING, RING, 48, LANES), jnp.bfloat16),
            pltpu.VMEM((3, experts, LANES), jnp.bfloat16),
            pltpu.VMEM((tokens, width), jnp.bfloat16),
            pltpu.VMEM((width, experts), jnp.bfloat16),
            pltpu.VMEM((units, width), jnp.bfloat16),
            pltpu.VMEM((2, RING, RING, 2, 16, parts[0][1]), jnp.bfloat16),
            pltpu.SemaphoreType.DMA((192,)),
            pltpu.SemaphoreType.DMA((192,)),
            pltpu.SemaphoreType.DMA((32,)),
            pltpu.SemaphoreType.DMA((5,)),
        ],
        compiler_params=pltpu.CompilerParams(
            collective_id=0, has_side_effects=True, vmem_limit_bytes=62 * 2**20
        ),
    )(grad, inputs, router, ids, down)[1:]


def combine_kernel(
    parts, values, grad_first, grad_second, w_gate, w_up, lines, counts, inputs, router,
    probs, gates, place, scale, ids, aux,
    out, combine_grad, router_grad, back,
    q0, q1, q2, l0, l1, l2, x0, x1, x2, y0, y1, y2, u0, u1, u2, v0, v1, v2,
    gate, up, stage, given, h1, h2, h3, flat, logit_grad, terms, other_terms,
    e10, e11, e12, e20, e21, e22, e30, e31, e32, ss, rs, ls, bs,
):
    rows, relay = (q0, q1, q2), (l0, l1, l2)
    halves2, whole2 = (x0, x1, x2), (y0, y1, y2)
    halves1, whole1 = (u0, u1, u2), (v0, v1, v2)
    sums = ((e10, e11, e12), (e20, e21, e22), (e30, e31, e32))
    bands = ((0, 16), (16, 8), (24, 8))
    steps = (1, -1, 2)
    here = Place()
    wires = Wires(ss, rs)
    tokens = out.shape[0]
    local = []
    fetches = []
    for p, (start, size) in enumerate(parts):
        for n, (src, dst) in enumerate(((w_gate, gate), (w_up, up))):
            span = pl.ds(start, size)
            copy = pltpu.make_async_copy(src.at[span], dst.at[span], bs.at[6 + 2 * p + n])
            copy.start()
            fetches.append(copy)

    def given_copies(p, k, b_step):
        slot = (k * 3 + p) % 2
        where = fixed_b(ORDERS[p], here.along(ORDERS[p][1], b_step))
        return [
            pltpu.make_async_copy(src.at[where], given.at[slot, n], bs.at[2 + 2 * slot + n])
            for n, src in enumerate((grad_first, grad_second))
        ]

    for copy in given_copies(0, 0, 2):
        copy.start()
    here.greet(steps)

    def values_line():
        mine = here.at[2] * 2 + here.core
        h1[mine] = values[:, :, here.at[2], here.core]
        for step in (0, *steps):
            for other in (0, 1):
                if step or other:
                    core = 1 - here.core if other else here.core
                    wires.send(
                        values.at[:, :, here.along(2, step), core],
                        h1.at[mine],
                        here.near(2, step, other),
                        ("v1", step, other),
                    )

    def values_x():
        for step in (0, *steps):
            for other in (0, 1):
                if step or other:
                    core = 1 - here.core if other else here.core
                    wires.arrived(
                        h1.at[here.along(2, -step) * 2 + core],
                        ("v1", step, other),
                        here.near(2, -step, other),
                    )
        h2[here.at[1]] = h1[:, :, here.at[1]]
        for step in steps:
            wires.send(
                h1.at[:, :, here.along(1, step)],
                h2.at[here.at[1]],
                here.near(1, step),
                ("v2", step),
            )

    def values_z():
        for step in steps:
            wires.arrived(h2.at[here.along(1, -step)], ("v2", step), here.near(1, -step))
        h3[here.at[0]] = h2[:, :, here.at[0]]
        for step in steps:
            wires.send(
                h2.at[:, :, here.along(0, step)],
                h3.at[here.at[0]],
                here.near(0, step),
                ("v3", step),
            )

    def router_back():
        for step in steps:
            wires.arrived(h3.at[here.along(0, -step)], ("v3", step), here.near(0, -step))

        def one_expert(e, carry):
            flat[pl.ds(e, 1), :] = h3[e // 32, (e // 8) % 4, e % 8]
            return carry

        lax.fori_loop(0, flat.shape[0], one_expert, 0)
        by_slot = flat[...].T
        dense = jnp.zeros_like(by_slot)
        for j in range(16):
            dense = dense + jnp.where(place[...] == j, by_slot[j : j + 1], 0.0)
        lane = lax.broadcasted_iota(jnp.int32, dense.shape, 1)
        column = lax.broadcasted_iota(jnp.int32, combine_grad.shape, 1)
        picked = jnp.zeros(combine_grad.shape, jnp.float32)
        for k in range(combine_grad.shape[1]):
            value = jnp.sum(
                jnp.where(lane == ids[:, k : k + 1], dense, 0.0), axis=1, keepdims=True
            )
            picked = picked + jnp.where(column == k, value, 0.0)
        combine_grad[...] = picked
        inner = jnp.sum(gates[...] * dense, axis=1, keepdims=True)
        prob_grad = jnp.where(place[...] >= 0, (dense - inner) / scale[...], 0.0)
        top = combine_grad.shape[1]
        fraction = dense.shape[1] * counts[...] / (top * tokens * RING * RING)
        prob_grad = prob_grad + aux[0] * fraction
        mean = jnp.sum(probs[...] * prob_grad, axis=1, keepdims=True)
        logit_grad[...] = (probs[...] * (prob_grad - mean)).astype(jnp.bfloat16)

        def one_tile(n, carry):
            columns = pl.ds(pl.multiple_of(n * LANES, LANES), LANES)
            term = lax.dot_general(
                inputs[:, columns],
                logit_grad[...],
                (((0,), (0,)), ((), ())),
                preferred_element_type=jnp.float32,
            )
            for m in range(2):
                for core in range(2):
                    terms[core, n // 8, (n // 2) % 4, 2 * (n % 2) + m] = term[
                        64 * m + 32 * core : 64 * m + 32 * core + 32
                    ]
            return carry

        lax.fori_loop(0, inputs.shape[1] // LANES, one_tile, 0)
        wires.send(terms.at[1 - here.core], other_terms, here.partner(), ("r0",))

    def chip_sum():
        wires.arrived(other_terms, ("r0",), here.partner())

        def one(n, carry):
            z, x = n // RING, n % RING
            terms[here.core, z, x] = terms[here.core, z, x] + other_terms[z, x]
            return carry

        lax.fori_loop(0, RING * RING, one, 0)

    def band_of(q, level, coordinate):
        where = [slice(None)] * 3
        for axis in ORDERS[q][:level]:
            where[axis] = here.at[axis]
        where[ORDERS[q][level]] = coordinate
        return (here.core, *where, pl.ds(*bands[q]), slice(None))

    def sum_send(level):
        for q in range(3):
            axis = ORDERS[q][level]
            for n, step in enumerate(steps):
                wires.send(
                    terms.at[band_of(q, level, here.along(axis, step))],
                    sums[level][q].at[n],
                    here.near(axis, step),
                    ("r", level, q, step),
                )

    def sum_in(level):
        for q in range(3):
            axis = ORDERS[q][level]
            for n, step in enumerate(steps):
                wires.arrived(
                    sums[level][q].at[n], ("r", level, q, step), here.near(axis, -step)
                )
            own = band_of(q, level, here.at[axis])
            landed = sums[level][q]
            terms[own] = terms[own] + landed[0] + landed[1] + landed[2]

    def sum_out():
        for q in range(3):
            span = pl.ds(*bands[q])
            router_grad[span] = terms[here.core, here.at[0], here.at[1], here.at[2], span]

    def stage_copy(p, k, b_step):
        start, size = parts[p]
        b_index = here.along(ORDERS[p][1], b_step)
        slot = (k * 3 + p) % 2
        return pltpu.make_async_copy(
            stage.at[slot, :, :, :, :, pl.ds(0, size)],
            back.at[(*fixed_b(ORDERS[p], b_index), slice(None), slice(None), pl.ds(start, size))],
            bs.at[slot],
        )

    def produce(p, k, b_step):
        start, size = parts[p]
        b_index = here.along(ORDERS[p][1], b_step)
        slot = (k * 3 + p) % 2
        units = grad_first.shape[-1]
        if k == 0:
            fetches[2 * p].wait()
            fetches[2 * p + 1].wait()
        for copy in given_copies(p, k, b_step):
            copy.wait()

        def columns(offset, width):
            span = pl.ds(start + offset, width)
            total = 0.0
            for n, weight in enumerate((gate, up)):
                total = total + lax.dot_general(
                    given[slot, n].reshape(512, units),
                    weight[span],
                    (((1,), (1,)), ((), ())),
                    preferred_element_type=jnp.float32,
                )
            stage[slot, :, :, :, :, pl.ds(offset, width)] = total.astype(jnp.bfloat16).reshape(
                RING, RING, 2, 16, width
            )

        def tile(n, carry):
            columns(pl.multiple_of(n * 256, 256), 256)
            return carry

        lax.fori_loop(0, size // 256, tile, 0)
        if size % 256:
            columns(size // 256 * 256, size % 256)
        stage_copy(p, k, b_step).start()

    def pieces(p, b_index, s_index, c_index):
        start, size = parts[p]
        return slots_of(back, ORDERS[p], b_index, s_index, c_index, start, size)

    def give(p, k, b_step):
        a, b, s = ORDERS[p]
        b_index = here.along(b, b_step)
        mine = rows[p].at[b_index, :, here.at[s] * 2 + here.core]
        way = 1 if k % 2 == 0 else -1
        wires.send(
            pieces(p, b_index, here.along(s, 2), slice(None)),
            relay[p].at[k],
            here.near(s, way),
            (p, "relay", k),
        )
        for step in (1, -1):
            for other in (0, 1):
                core = 1 - here.core if other else here.core
                wires.send(
                    pieces(p, b_index, here.along(s, step), core),
                    mine,
                    here.near(s, step, other),
                    (p, "near", step, other, k),
                )
        wires.send(
            pieces(p, b_index, here.at[s], 1 - here.core), mine, here.partner(), (p, "chip", k)
        )
        copy = pltpu.make_async_copy(
            pieces(p, b_index, here.at[s], here.core), mine, ls.at[len(local)]
        )
        copy.start()
        local.append(copy)

    def forward(p, k, b_step):
        a, b, s = ORDERS[p]
        b_index = here.along(b, b_step)
        way = 1 if k % 2 == 0 else -1
        wires.arrived(relay[p].at[k], (p, "relay", k), here.near(s, -way))
        theirs = rows[p].at[b_index, :, here.along(s, -way) * 2 + here.core]
        for other in (0, 1):
            core = 1 - here.core if other else here.core
            wires.send(
                relay[p].at[k, :, core], theirs, here.near(s, way, other), (p, "far", other, k)
            )

    def gathered(p, k, b_step):
        a, b, s = ORDERS[p]
        b_index = here.along(b, b_step)
        way = 1 if k % 2 == 0 else -1
        for other in (0, 1):
            core = 1 - here.core if other else here.core
            for step in (1, -1):
                wires.arrived(
                    rows[p].at[b_index, :, here.along(s, -step) * 2 + core],
                    (p, "near", step, other, k),
                    here.near(s, -step, other),
                )
            wires.arrived(
                rows[p].at[b_index, :, here.along(s, 2) * 2 + core],
                (p, "far", other, k),
                here.near(s, -way, other),
            )
        wires.arrived(
            rows[p].at[b_index, :, here.at[s] * 2 + (1 - here.core)],
            (p, "chip", k),
            here.partner(),
        )
        local[k * 3 + p].wait()

    def add_up(p, b_step):
        a, b, s = ORDERS[p]
        b_index = here.along(b, b_step)
        size = parts[p][1]

        def one(a_index, carry):
            token_of = lines[p, b_index, a_index, pl.ds(0, 1), :]
            gate_of = lines[p, b_index, a_index, pl.ds(1, 1), :]
            token = lax.broadcasted_iota(jnp.int32, (tokens, LANES), 0).astype(jnp.float32)
            weigh = jnp.where(token == token_of, gate_of, 0.0).astype(jnp.bfloat16)
            total = jnp.dot(
                weigh,
                rows[p][b_index, a_index].reshape(LANES, size),
                preferred_element_type=jnp.float32,
            )
            rows[p][b_index, a_index] = total.astype(jnp.bfloat16).reshape(8, 16, size)
            return carry

        lax.fori_loop(0, RING, one, 0)

    def plus(*terms):
        total = terms[0].astype(jnp.float32)
        for term in terms[1:]:
            total = total + term.astype(jnp.float32)
        return total

    def fold2(p, way, k, step):
        a, b, s = ORDERS[p]
        b_index, a_index = here.along(b, way), here.along(a, step)
        slot = 0 if way == 1 else 1
        groups = pl.ds(0, 4) if way == 1 else pl.ds(4, 4)
        wires.arrived(halves2[p].at[slot, k], (p, "half2", way, k), here.near(b, -way))
        rows[p][b_index, a_index, groups] = plus(
            rows[p][b_index, a_index, groups], halves2[p][slot, k]
        ).astype(jnp.bfloat16)
        wires.send(
            rows[p].at[b_index, a_index],
            whole2[p].at[slot, k],
            here.near(b, way),
            (p, "whole2", way, k),
        )

    def settle2(p, k, step):
        a, b, s = ORDERS[p]
        for way in (1, -1):
            slot = 0 if way == 1 else 1
            wires.arrived(whole2[p].at[slot, k], (p, "whole2", way, k), here.near(b, -way))
        own = rows[p].at[here.at[b], here.along(a, step)]
        return plus(own[...], whole2[p][0, k], whole2[p][1, k])

    order = (2, 1, -1, 0)
    work = [(k, p) for k in range(4) for p in range(3)]
    values_line()
    between = {2: values_x, 4: values_z, 6: router_back, 8: chip_sum}
    for turn in range(len(work) + 1):
        if turn < len(work):
            k, p = work[turn]
            if turn + 1 < len(work):
                after_k, after_p = work[turn + 1]
                for copy in given_copies(after_p, after_k, order[after_k]):
                    copy.start()
            produce(p, k, order[k])
        if turn > 0:
            k, p = work[turn - 1]
            stage_copy(p, k, order[k]).wait()
            give(p, k, order[k])
            if p == 2 and k > 0:
                for q in range(3):
                    forward(q, k - 1, order[k - 1])
        if turn in between:
            between[turn]()
        if turn == 8:
            sum_send(0)
    for p, (a, b, s) in enumerate(ORDERS):
        gathered(p, 0, 2)
        add_up(p, 2)
        far = here.along(b, 2)
        for k, step in enumerate(order):
            for way, groups in ((1, pl.ds(0, 4)), (-1, pl.ds(4, 4))):
                wires.send(
                    rows[p].at[far, here.along(a, step), groups],
                    halves2[p].at[0 if way == 1 else 1, k],
                    here.near(b, way),
                    (p, "half2", way, k),
                )
    for q in range(3):
        forward(q, 3, order[3])
    for k in (1, 2, 3):
        for p in range(3):
            gathered(p, k, order[k])
            add_up(p, order[k])
    sum_in(0)
    sum_send(1)
    for k, step in enumerate(order):
        for way in (1, -1):
            for p in range(3):
                fold2(p, way, k, step)
    sum_in(1)
    sum_send(2)
    for p, (a, b, s) in enumerate(ORDERS):
        block = rows[p].at[here.at[b], here.along(a, 2)]
        block[...] = settle2(p, 0, 2).astype(jnp.bfloat16)
        for way, groups in ((1, pl.ds(0, 4)), (-1, pl.ds(4, 4))):
            wires.send(
                rows[p].at[here.at[b], here.along(a, 2), groups],
                halves1[p].at[0 if way == 1 else 1],
                here.near(a, way),
                (p, "half1", way),
            )
    for k, way in ((1, 1), (2, -1)):
        for p, (a, b, s) in enumerate(ORDERS):
            slot = 0 if way == 1 else 1
            groups = pl.ds(0, 4) if way == 1 else pl.ds(4, 4)
            block = rows[p].at[here.at[b], here.along(a, way)]
            block[...] = settle2(p, k, way).astype(jnp.bfloat16)
            wires.arrived(halves1[p].at[slot], (p, "half1", way), here.near(a, -way))
            part = rows[p].at[here.at[b], here.along(a, way), groups]
            part[...] = plus(part[...], halves1[p][slot]).astype(jnp.bfloat16)
            wires.send(block, whole1[p].at[slot], here.near(a, way), (p, "whole1", way))
    for p, (a, b, s) in enumerate(ORDERS):
        start, size = parts[p]
        total = settle2(p, 3, 0)
        for way in (1, -1):
            slot = 0 if way == 1 else 1
            wires.arrived(whole1[p].at[slot], (p, "whole1", way), here.near(a, -way))
        total = plus(total, whole1[p][0], whole1[p][1]).reshape(tokens, size)
        total = total + lax.dot_general(
            logit_grad[...],
            router[pl.ds(start, size)],
            (((1,), (1,)), ((), ())),
            preferred_element_type=jnp.float32,
        )
        out[:, pl.ds(start, size)] = total.astype(out.dtype)
    sum_in(2)
    sum_out()
    wires.drain()


def combine(parts, values, grads, weights, lines, counts, inputs, router, probs, gates, place, scale, ids, aux):
    width, units = weights[0].shape
    tokens, top = ids.shape
    experts = probs.shape[1]

    def buffers(*lead):
        return [pltpu.VMEM((*lead, size), jnp.bfloat16) for _, size in parts]

    def floats(*shape):
        return pltpu.VMEM(shape, jnp.float32)

    hbm, vmem = pl.BlockSpec(memory_space=pltpu.HBM), pl.BlockSpec(memory_space=pltpu.VMEM)
    bands = (16, 8, 8)
    return pl.pallas_call(
        functools.partial(combine_kernel, parts),
        out_shape=(
            jax.ShapeDtypeStruct((tokens, width), jnp.bfloat16),
            jax.ShapeDtypeStruct((tokens, top), jnp.float32),
            jax.ShapeDtypeStruct((width // (2 * RING**3), experts), jnp.float32),
            jax.ShapeDtypeStruct((RING, RING, RING, 2, 16, width), jnp.bfloat16),
        ),
        in_specs=[vmem, hbm, hbm, hbm, hbm]
        + [vmem] * 9
        + [pl.BlockSpec(memory_space=pltpu.SMEM)],
        out_specs=(vmem, vmem, vmem, hbm),
        scratch_shapes=buffers(RING, RING, 8, 16)
        + buffers(RING, RING, 2, 16)
        + buffers(2, RING, 4, 16)
        + buffers(2, RING, 8, 16)
        + buffers(2, 4, 16)
        + buffers(2, 8, 16)
        + [
            pltpu.VMEM((width, units), jnp.bfloat16),
            pltpu.VMEM((width, units), jnp.bfloat16),
            pltpu.VMEM((2, RING, RING, 2, 16, parts[0][1]), jnp.bfloat16),
            pltpu.VMEM((2, 2, RING, RING, 2, 16, units), jnp.bfloat16),
            floats(8, RING, RING, 1, LANES),
            floats(RING, 8, RING, 1, LANES),
            floats(RING, RING, 8, 1, LANES),
            floats(experts, LANES),
            pltpu.VMEM((tokens, experts), jnp.bfloat16),
            floats(2, RING, RING, RING, 32, experts),
            floats(RING, RING, RING, 32, experts),
        ]
        + [floats(3, RING, RING, band, experts) for band in bands]
        + [floats(3, RING, band, experts) for band in bands]
        + [floats(3, band, experts) for band in bands]
        + [
            pltpu.SemaphoreType.DMA((224,)),
            pltpu.SemaphoreType.DMA((224,)),
            pltpu.SemaphoreType.DMA((16,)),
            pltpu.SemaphoreType.DMA((12,)),
        ],
        compiler_params=pltpu.CompilerParams(
            collective_id=1, has_side_effects=True, vmem_limit_bytes=67043328
        ),
    )(values, *grads, *weights, lines, counts, inputs, router, probs, gates, place, scale, ids, aux)[:3]


def hidden_backward(upstream, pre_gate, pre_up):
    first = pre_gate.astype(jnp.float32)
    second = pre_up.astype(jnp.float32)
    gate_sig = jax.nn.sigmoid(first)
    gate_act = first * gate_sig
    hidden = gate_act * second
    slot_combine = jnp.sum(upstream * hidden, axis=-1).astype(jnp.bfloat16)
    grad_first = (upstream * second * gate_sig * (1.0 + first * (1.0 - gate_sig))).astype(
        jnp.bfloat16
    )
    grad_second = (upstream * gate_act).astype(jnp.bfloat16)
    return grad_first, grad_second, slot_combine


def shards(
    tokens,
    out_grad,
    router_weight,
    gate_weight,
    up_weight,
    down_weight,
    saved_gate,
    saved_up,
    expert_ids,
    aux_weight,
):
    devices = lax.axis_size(AXES)
    inputs, upstream_grad, chosen_ids = tokens[0], out_grad[0], expert_ids[0]
    model_width = inputs.shape[1]
    capacity = saved_gate.shape[1] // devices
    parts = column_parts(model_width)

    upstream, lines, counts, probs, gates, place, chosen_sum = dispatch(
        parts, upstream_grad, inputs, router_weight, chosen_ids, down_weight[0]
    )
    grad_first, grad_second, slot_combine = hidden_backward(
        upstream,
        saved_gate[0].reshape(upstream.shape),
        saved_up[0].reshape(upstream.shape),
    )
    values = slot_combine.astype(jnp.float32).reshape(*upstream.shape[:4], 1, capacity)
    values = jnp.pad(values, [(0, 0)] * 5 + [(0, LANES - capacity)])
    token_grad, combine_grad, router_grad = combine(
        parts,
        values,
        (grad_first, grad_second),
        (gate_weight[0], up_weight[0]),
        lines,
        counts,
        inputs,
        router_weight,
        probs,
        gates,
        place,
        chosen_sum,
        chosen_ids,
        aux_weight,
    )
    return (token_grad[None], combine_grad[None], router_grad)


def solution(mesh):
    torus = Mesh(mesh.devices.reshape(RING, RING, RING, 2), AXES)
    return jax.shard_map(
        shards,
        mesh=torus,
        in_specs=(
            P(EXP, SEQ, None),
            P(EXP, SEQ, None),
            P(),
            P(AXES, None, None),
            P(AXES, None, None),
            P(AXES, None, None),
            P(AXES, None, None),
            P(AXES, None, None),
            P(EXP, SEQ, None),
            P(),
        ),
        out_specs=(P(EXP, SEQ, None), P(EXP, SEQ, None), P(AXES, None)),
        check_vma=False,
    )
```

```python
import functools

import jax
import jax.numpy as jnp
from jax import lax
from jax.experimental import pallas as pl
from jax.experimental.pallas import tpu as pltpu
from jax.sharding import Mesh
from jax.sharding import PartitionSpec as P

SEQ = ("seq_0", "seq_1")
EXP = ("exp_0", "exp_1")
AXES = ("seq_0", "seq_1", "exp_0", "exp_1")
MESH = pl.DeviceIdType.MESH
RING = 4
LANES = 128
ORDERS = ((0, 1, 2), (1, 2, 0), (2, 0, 1))
STRIDES = (32, 8, 2)
DISPATCH_PLAN = (
    ("relay", 0), ("choose", 0), ("relay", 1), ("relay", 2), ("relay", 3), ("choose", 1), ("pass", 0),
    ("choose", 2), ("far",), ("pass", 1), ("choose", 3), ("clear",),
    ("near", 0), ("pass", 2), ("near", 1), ("distant", 0), ("pass", 3), ("near", 2),
    ("distant", 1), ("near", 3), ("distant", 2), ("distant", 3),
)
COMBINE_PLAN = (
    ("line",), ("make", 0), ("post", 0), ("make", 1), ("post", 1), ("make", 2), ("post", 2), ("x",),
    ("make", 3), ("post", 3), ("make", 4), ("post", 4), ("pass", 0), ("make", 5), ("post", 5), ("z",),
    ("make", 6), ("post", 6), ("make", 7), ("post", 7), ("pass", 1), ("make", 8), ("post", 8),
    ("total", 0), ("halve",), ("router",), ("make", 9), ("post", 9), ("pass", 2), ("make", 10), ("post", 10),
    ("make", 11), ("post", 11), ("chip",), ("send", 0), ("pass", 3),
    ("total", 1), ("fold", 1), ("in", 0), ("send", 1),
    ("total", 2), ("fold", -1), ("in", 1), ("send", 2), ("total", 3),
)


def column_parts(width):
    tiles = width // LANES
    sizes = [(tiles + 2 - p) // 3 * LANES for p in range(3)]
    starts = [0, sizes[0], sizes[0] + sizes[1]]
    return list(zip(starts, sizes))


class Wires:
    def __init__(self, send_sems, recv_sems):
        self.send_sems, self.recv_sems = send_sems, recv_sems
        self.sent, self.names = [], {}

    def slot(self, name):
        return self.recv_sems.at[self.names.setdefault(name, len(self.names))]

    def send(self, src, dst, device, name):
        copy = pltpu.make_async_remote_copy(
            src, dst, self.send_sems.at[len(self.sent)], self.slot(name), device, MESH
        )
        copy.start()
        self.sent.append(copy)

    def arrived(self, ref, name, device):
        pltpu.make_async_remote_copy(
            ref, ref, self.send_sems.at[0], self.slot(name), device, MESH
        ).wait_recv()

    def drain(self):
        for copy in self.sent:
            copy.wait_send()


class Place:
    def __init__(self):
        self.at = [lax.axis_index(name) for name in AXES]
        self.core = self.at[3]

    def along(self, axis, step):
        return lax.rem(self.at[axis] + (step + RING), RING)

    def near(self, axis, step, other_core=0):
        coords = list(self.at)
        coords[axis] = self.along(axis, step)
        if other_core:
            coords[3] = 1 - self.core
        return tuple(coords)

    def partner(self):
        return (self.at[0], self.at[1], self.at[2], 1 - self.core)

    def greet(self, steps=(1, -1)):
        barrier = pltpu.get_barrier_semaphore()
        peers = [self.partner()]
        for axis in range(3):
            for step in steps:
                for other in (0, 1):
                    peers.append(self.near(axis, step, other))
        for peer in peers:
            pl.semaphore_signal(barrier, inc=1, device_id=peer, device_id_type=MESH)
        pl.semaphore_wait(barrier, len(peers))


def slots_of(ref, order, b_index, s_index, c_index, start, size):
    a, b, s = order
    where = [None] * 3
    where[a], where[b], where[s] = slice(None), b_index, s_index
    return ref.at[where[0], where[1], where[2], c_index, :, pl.ds(start, size)]


def fixed_b(order, b_index):
    where = [slice(None)] * 3
    where[order[1]] = b_index
    return tuple(where)


def dispatch_kernel(
    parts, grad, inputs, router, ids, down,
    slots, upstream, lines, counts, probs, gates, place, scale,
    g0, g1, g2, o0, o1, o2, l0, l1, l2, seen, picks, tokens_in, router_in, weight, batch, last,
    ss, rs, ls, bs,
):
    held, outgoing, relay = (g0, g1, g2), (o0, o1, o2), (l0, l1, l2)
    here = Place()
    wires = Wires(ss, rs)
    tokens = grad.shape[0]
    half = tokens // 2
    local = []

    def keep(src, dst):
        copy = pltpu.make_async_copy(src, dst, ls.at[len(local)])
        copy.start()
        local.append(copy)

    for p, (a, b, s) in enumerate(ORDERS):
        start, size = parts[p]
        keep(grad.at[:, pl.ds(start, size)], held[p].at[here.at[b], here.at[a]])
    fetches = [
        pltpu.make_async_copy(src, dst, bs.at[8 + n])
        for n, (src, dst) in enumerate(((inputs, tokens_in), (router, router_in), (down, weight)))
    ]
    for copy in fetches:
        copy.start()
    here.greet()
    for copy in local:
        copy.wait()

    def pass_on(p, k, step):
        a, b, s = ORDERS[p]
        block = held[p].at[here.at[b], here.along(a, step)]
        wires.send(block, block, here.near(b, 1), (p, "m2", 1, k))
        wires.send(block, block, here.near(b, -1), (p, "m2", -1, k))

    def relay_on(p, k, step):
        a, b, s = ORDERS[p]
        for way, rows in ((1, pl.ds(0, half)), (-1, pl.ds(half, half))):
            block = held[p].at[here.along(b, -way), here.along(a, step)]
            wires.arrived(block, (p, "m2", way, k), here.near(b, -way))
            piece = held[p].at[here.along(b, -way), here.along(a, step), rows]
            wires.send(piece, piece, here.near(b, way), (p, "m2far", way, k))

    def far_in(p, k, step):
        a, b, s = ORDERS[p]
        for way, rows in ((1, pl.ds(0, half)), (-1, pl.ds(half, half))):
            piece = held[p].at[here.along(b, 2), here.along(a, step), rows]
            wires.arrived(piece, (p, "m2far", way, k), here.near(b, -way))

    def route():
        experts = router.shape[1]
        row = lax.broadcasted_iota(jnp.int32, (tokens, experts), 0)
        lane = lax.broadcasted_iota(jnp.int32, (tokens, experts), 1)
        mask = jnp.zeros((tokens, experts), jnp.float32)
        by_token = ids[...].T
        for k in range(ids.shape[0]):
            mask = mask + jnp.where(lane == by_token[:, k : k + 1], 1.0, 0.0)
        before = jnp.where(row > lane, 1.0, 0.0).astype(jnp.bfloat16)
        rank = jnp.dot(before, mask.astype(jnp.bfloat16), preferred_element_type=jnp.float32)
        place[...] = jnp.where(mask > 0, rank, -1.0)
        logits = jnp.dot(tokens_in[...], router_in[...], preferred_element_type=jnp.float32)
        powers = jnp.exp(logits - jnp.max(logits, axis=1, keepdims=True))
        probs[...] = powers / jnp.sum(powers, axis=1, keepdims=True)
        chosen = probs[...] * mask
        scale[...] = jnp.sum(chosen, axis=1, keepdims=True)
        gates[...] = chosen / scale[...]
        slot = lax.broadcasted_iota(jnp.int32, (16, experts), 0)
        token_of = jnp.zeros((16, experts), jnp.float32)
        gate_of = jnp.zeros((16, experts), jnp.float32)
        offset = (row - tokens).astype(jnp.float32)
        for j in range(16):
            hit = place[...] == j
            token = jnp.sum(jnp.where(hit, offset, 0.0), axis=0, keepdims=True) + tokens
            gate = jnp.sum(jnp.where(hit, gates[...], 0.0), axis=0, keepdims=True)
            token_of = jnp.where(slot == j, token, token_of)
            gate_of = jnp.where(slot == j, gate, gate_of)
        count = jnp.where(slot == 0, jnp.sum(mask, axis=0, keepdims=True), 0.0)
        for p, (a, b, s) in enumerate(ORDERS):
            for n, part in enumerate((token_of, gate_of, count)):
                seen[p, here.at[b], here.at[a], pl.ds(16 * n, 16), :] = part.astype(jnp.bfloat16)
        for p, (a, b, s) in enumerate(ORDERS):
            first = here.at[a] * STRIDES[a] + here.at[b] * STRIDES[b]
            expert = first + lane // 32 * STRIDES[s] + lane // 16 % 2
            picks[p] = jnp.where(row == expert, 1.0, 0.0).astype(jnp.bfloat16)

    for p, (a, b, s) in enumerate(ORDERS):
        block = held[p].at[here.at[b], here.at[a]]
        for way in (1, -1):
            wires.send(block, block, here.near(a, way), (p, "m1", way))
    for copy in fetches[:2]:
        copy.wait()
    route()
    for p, (a, b, s) in enumerate(ORDERS):
        table = seen.at[p, here.at[b], here.at[a]]
        for way in (1, -1):
            wires.send(table, table, here.near(a, way), (p, "t1", way))
    for p in range(3):
        pass_on(p, 0, 0)
    for p, (a, b, s) in enumerate(ORDERS):
        table = seen.at[p, here.at[b], here.along(a, -1)]
        wires.arrived(table, (p, "t1", 1), here.near(a, -1))
        wires.send(table, table, here.near(a, 1), (p, "t1far"))
        wires.arrived(
            seen.at[p, here.at[b], here.along(a, 1)], (p, "t1", -1), here.near(a, 1)
        )
    for p, (a, b, s) in enumerate(ORDERS):
        for way, rows in ((1, pl.ds(0, half)), (-1, pl.ds(half, half))):
            block = held[p].at[here.at[b], here.along(a, -way)]
            wires.arrived(block, (p, "m1", way), here.near(a, -way))
            piece = held[p].at[here.at[b], here.along(a, -way), rows]
            wires.send(piece, piece, here.near(a, way), (p, "m1far", way))
    for p, (a, b, s) in enumerate(ORDERS):
        wires.arrived(
            seen.at[p, here.at[b], here.along(a, 2)], (p, "t1far"), here.near(a, -1)
        )
        table = seen.at[p, here.at[b]]
        for way in (1, -1):
            wires.send(table, table, here.near(b, way), (p, "t2", way))
    for p in range(3):
        pass_on(p, 1, -1)
        pass_on(p, 2, 1)
    for p, (a, b, s) in enumerate(ORDERS):
        table = seen.at[p, here.along(b, -1)]
        wires.arrived(table, (p, "t2", 1), here.near(b, -1))
        wires.send(table, table, here.near(b, 1), (p, "t2far"))
        wires.arrived(seen.at[p, here.along(b, 1)], (p, "t2", -1), here.near(b, 1))
    for p, (a, b, s) in enumerate(ORDERS):
        for way, rows in ((1, pl.ds(0, half)), (-1, pl.ds(half, half))):
            piece = held[p].at[here.at[b], here.along(a, 2), rows]
            wires.arrived(piece, (p, "m1far", way), here.near(a, -way))
        pass_on(p, 3, 2)

    def select(p, k, b_step):
        a, b, s = ORDERS[p]
        b_index = here.along(b, b_step)
        size = parts[p][1]
        found = jnp.dot(
            seen[p, b_index].reshape(RING * 48, LANES),
            picks[p],
            preferred_element_type=jnp.float32,
        ).reshape(RING, 3, 16, LANES)
        slot = lax.broadcasted_iota(jnp.int32, found.shape, 2)
        lane = lax.broadcasted_iota(jnp.int32, found.shape, 3)
        found = jnp.sum(jnp.where(slot == lane % 16, found, 0.0), axis=2)
        for a_index in range(RING):
            for n in range(2):
                lines[p, b_index, a_index, pl.ds(n, 1), :] = found[a_index, n : n + 1]

        def one(a_index, carry):
            token_of = lines[p, b_index, a_index, pl.ds(0, 1), :]
            token = lax.broadcasted_iota(jnp.int32, (tokens, LANES), 0).astype(jnp.float32)
            pick = jnp.where(token == token_of, 1.0, 0.0).astype(jnp.bfloat16)
            rows = lax.dot_general(
                pick,
                held[p][b_index, a_index],
                (((0,), (0,)), ((), ())),
                preferred_element_type=jnp.float32,
            )
            outgoing[p][k, :, a_index] = rows.astype(jnp.bfloat16).reshape(8, 16, size)
            return carry

        lax.fori_loop(0, RING, one, 0)

    def deliver(p, k, b_step):
        order = ORDERS[p]
        a, b, s = order
        start, size = parts[p]
        b_index = here.along(b, b_step)
        mine = slots_of(slots, order, b_index, here.at[s], here.core, start, size)
        way = 1 if k % 2 == 0 else -1
        wires.send(
            outgoing[p].at[k, pl.ds(here.along(s, 2) * 2, 2)],
            relay[p].at[k],
            here.near(s, way),
            (p, "relay", k),
        )
        for step in (1, -1):
            for other in (0, 1):
                core = 1 - here.core if other else here.core
                wires.send(
                    outgoing[p].at[k, here.along(s, step) * 2 + core],
                    mine,
                    here.near(s, step, other),
                    (p, "near", step, other, k),
                )
        wires.send(
            outgoing[p].at[k, here.at[s] * 2 + (1 - here.core)],
            mine,
            here.partner(),
            (p, "chip", k),
        )
        keep(outgoing[p].at[k, here.at[s] * 2 + here.core], mine)

    def forward(p, k, b_step):
        order = ORDERS[p]
        a, b, s = order
        start, size = parts[p]
        b_index = here.along(b, b_step)
        way = 1 if k % 2 == 0 else -1
        wires.arrived(relay[p].at[k], (p, "relay", k), here.near(s, -way))
        theirs = slots_of(slots, order, b_index, here.along(s, -way), here.core, start, size)
        for other in (0, 1):
            core = 1 - here.core if other else here.core
            wires.send(
                relay[p].at[k, core], theirs, here.near(s, way, other), (p, "far", other, k)
            )

    def near_in(p, k):
        order = ORDERS[p]
        a, b, s = order
        start, size = parts[p]
        b_index = here.along(b, turns[k])
        for other in (0, 1):
            core = 1 - here.core if other else here.core
            for step in (1, -1):
                wires.arrived(
                    slots_of(slots, order, b_index, here.along(s, -step), core, start, size),
                    (p, "near", step, other, k),
                    here.near(s, -step, other),
                )
        wires.arrived(
            slots_of(slots, order, b_index, here.at[s], 1 - here.core, start, size),
            (p, "chip", k),
            here.partner(),
        )
        local[3 + k * 3 + p].wait()

    def distant_in(p, k):
        order = ORDERS[p]
        a, b, s = order
        start, size = parts[p]
        b_index = here.along(b, turns[k])
        way = 1 if k % 2 == 0 else -1
        for other in (0, 1):
            core = 1 - here.core if other else here.core
            wires.arrived(
                slots_of(slots, order, b_index, here.along(s, 2), core, start, size),
                (p, "far", other, k),
                here.near(s, -way, other),
            )

    def copies(p, k, senders):
        order = ORDERS[p]
        start, size = parts[p]
        b_index = here.along(order[1], turns[k])
        slot = (k * 3 + p) % 2
        target, first = (batch, 3 * slot) if len(senders) == 3 else (last, 6 + slot)
        return [
            pltpu.make_async_copy(
                slots_of(
                    slots, order, b_index, here.along(order[2], step), slice(None), start, size
                ),
                target.at[slot, n, :, :, :, pl.ds(0, size)],
                bs.at[first + n],
            )
            for n, step in enumerate(senders)
        ]

    def project(p, k, senders):
        a, b, s = ORDERS[p]
        start, size = parts[p]
        b_index = here.along(b, turns[k])
        slot = (k * 3 + p) % 2
        source = batch if len(senders) == 3 else last
        for copy in copies(p, k, senders):
            copy.wait()

        def tile(n, carry):
            units = pl.ds(pl.multiple_of(n * 256, 256), 256)
            term = lax.dot_general(
                source[slot, :, :, :, :, pl.ds(0, size)].reshape(len(senders) * LANES, size),
                weight[units, pl.ds(start, size)],
                (((1,), (1,)), ((), ())),
                preferred_element_type=jnp.float32,
            ).reshape(len(senders), RING, 2, 16, 256)
            for m, step in enumerate(senders):
                where = [slice(None)] * 3
                where[b], where[s] = b_index, here.along(s, step)
                there = (*where, slice(None), slice(None), units)
                upstream[there] = upstream[there] + term[m]
            return carry

        lax.fori_loop(0, 3, tile, 0)

    turns = (0, -1, 1, 2)
    joined = (0, -1, 1, 2)

    def relays(k):
        for p in range(3):
            relay_on(p, k, joined[k])

    def choose(k):
        for p in range(3):
            select(p, k, turns[k])
            deliver(p, k, turns[k])

    def far_rows():
        for p, (a, b, s) in enumerate(ORDERS):
            for k in range(RING):
                far_in(p, k, joined[k])
            wires.arrived(seen.at[p, here.along(b, 2)], (p, "t2far"), here.near(b, -1))

    def pass_far(k):
        for p in range(3):
            forward(p, k, turns[k])

    def clear():
        total = jnp.sum(seen[0, :, :, pl.ds(32, 16), :].astype(jnp.float32), axis=(0, 1))
        counts[...] = jnp.sum(total, axis=0, keepdims=True)
        upstream[...] = jnp.zeros_like(upstream)
        fetches[2].wait()

    def multiply(k, arrive, senders):
        def fetch(p):
            arrive(p, k)
            for copy in copies(p, k, senders):
                copy.start()

        fetch(0)
        for p in range(3):
            if p < 2:
                fetch(p + 1)
            project(p, k, senders)

    actions = {
        "relay": relays,
        "choose": choose,
        "far": far_rows,
        "pass": pass_far,
        "clear": clear,
        "near": lambda k: multiply(k, near_in, (0, 1, -1)),
        "distant": lambda k: multiply(k, distant_in, (2,)),
    }
    for name, *given_to in DISPATCH_PLAN:
        actions[name](*given_to)
    wires.drain()


def dispatch(parts, grad, inputs, router, ids, down):
    tokens, width = grad.shape
    units, experts = down.shape[0], router.shape[1]
    rows = [pltpu.VMEM((RING, RING, tokens, size), jnp.bfloat16) for _, size in parts]
    outs = [pltpu.VMEM((RING, 8, RING, 16, size), jnp.bfloat16) for _, size in parts]
    relays = [pltpu.VMEM((RING, 2, RING, 16, size), jnp.bfloat16) for _, size in parts]
    hbm, vmem = pl.BlockSpec(memory_space=pltpu.HBM), pl.BlockSpec(memory_space=pltpu.VMEM)
    square = jax.ShapeDtypeStruct((tokens, experts), jnp.float32)
    return pl.pallas_call(
        functools.partial(dispatch_kernel, parts),
        out_shape=(
            jax.ShapeDtypeStruct((RING, RING, RING, 2, 16, width), jnp.bfloat16),
            jax.ShapeDtypeStruct((RING, RING, RING, 2, 16, units), jnp.float32),
            jax.ShapeDtypeStruct((3, RING, RING, 8, LANES), jnp.float32),
            jax.ShapeDtypeStruct((1, experts), jnp.float32),
            square,
            square,
            square,
            jax.ShapeDtypeStruct((tokens, 1), jnp.float32),
        ),
        in_specs=[hbm, hbm, hbm, vmem, hbm],
        out_specs=(hbm,) + (vmem,) * 7,
        scratch_shapes=rows
        + outs
        + relays
        + [
            pltpu.VMEM((3, RING, RING, 48, LANES), jnp.bfloat16),
            pltpu.VMEM((3, experts, LANES), jnp.bfloat16),
            pltpu.VMEM((tokens, width), jnp.bfloat16),
            pltpu.VMEM((width, experts), jnp.bfloat16),
            pltpu.VMEM((units, width), jnp.bfloat16),
            pltpu.VMEM((2, 3, RING, 2, 16, parts[0][1]), jnp.bfloat16),
            pltpu.VMEM((2, 1, RING, 2, 16, parts[0][1]), jnp.bfloat16),
            pltpu.SemaphoreType.DMA((192,)),
            pltpu.SemaphoreType.DMA((192,)),
            pltpu.SemaphoreType.DMA((32,)),
            pltpu.SemaphoreType.DMA((11,)),
        ],
        compiler_params=pltpu.CompilerParams(
            collective_id=0, has_side_effects=True, vmem_limit_bytes=62 * 2**20
        ),
    )(grad, inputs, router, ids, down)[1:]


def combine_kernel(
    parts, values, grad_first, grad_second, w_gate, w_up, lines, counts, inputs, router,
    probs, gates, place, scale, ids, aux,
    out, combine_grad, router_grad, back,
    q0, q1, q2, l0, l1, l2, x0, x1, x2, y0, y1, y2, u0, u1, u2, v0, v1, v2,
    gate, up, stage, given, h1, h2, h3, flat, logit_grad, terms, other_terms,
    e10, e11, e12, e20, e21, e22, e30, e31, e32, ss, rs, ls, bs,
):
    rows, relay = (q0, q1, q2), (l0, l1, l2)
    halves2, whole2 = (x0, x1, x2), (y0, y1, y2)
    halves1, whole1 = (u0, u1, u2), (v0, v1, v2)
    sums = ((e10, e11, e12), (e20, e21, e22), (e30, e31, e32))
    bands = ((0, 16), (16, 8), (24, 8))
    steps = (1, -1, 2)
    here = Place()
    wires = Wires(ss, rs)
    tokens = out.shape[0]
    local = []
    fetches = []
    for p, (start, size) in enumerate(parts):
        for n, (src, dst) in enumerate(((w_gate, gate), (w_up, up))):
            span = pl.ds(start, size)
            copy = pltpu.make_async_copy(src.at[span], dst.at[span], bs.at[6 + 2 * p + n])
            copy.start()
            fetches.append(copy)

    def given_copies(p, k, b_step):
        slot = (k * 3 + p) % 2
        where = fixed_b(ORDERS[p], here.along(ORDERS[p][1], b_step))
        return [
            pltpu.make_async_copy(src.at[where], given.at[slot, n], bs.at[2 + 2 * slot + n])
            for n, src in enumerate((grad_first, grad_second))
        ]

    for copy in given_copies(0, 0, 2):
        copy.start()
    here.greet(steps)

    def values_line():
        mine = here.at[2] * 2 + here.core
        h1[mine] = values[:, :, here.at[2], here.core]
        for step in (0, *steps):
            for other in (0, 1):
                if step or other:
                    core = 1 - here.core if other else here.core
                    wires.send(
                        values.at[:, :, here.along(2, step), core],
                        h1.at[mine],
                        here.near(2, step, other),
                        ("v1", step, other),
                    )

    def values_x():
        for step in (0, *steps):
            for other in (0, 1):
                if step or other:
                    core = 1 - here.core if other else here.core
                    wires.arrived(
                        h1.at[here.along(2, -step) * 2 + core],
                        ("v1", step, other),
                        here.near(2, -step, other),
                    )
        h2[here.at[1]] = h1[:, :, here.at[1]]
        for step in steps:
            wires.send(
                h1.at[:, :, here.along(1, step)],
                h2.at[here.at[1]],
                here.near(1, step),
                ("v2", step),
            )

    def values_z():
        for step in steps:
            wires.arrived(h2.at[here.along(1, -step)], ("v2", step), here.near(1, -step))
        h3[here.at[0]] = h2[:, :, here.at[0]]
        for step in steps:
            wires.send(
                h2.at[:, :, here.along(0, step)],
                h3.at[here.at[0]],
                here.near(0, step),
                ("v3", step),
            )

    def router_back():
        for step in steps:
            wires.arrived(h3.at[here.along(0, -step)], ("v3", step), here.near(0, -step))

        def one_expert(e, carry):
            flat[pl.ds(e, 1), :] = h3[e // 32, (e // 8) % 4, e % 8]
            return carry

        lax.fori_loop(0, flat.shape[0], one_expert, 0)
        by_slot = flat[...].T
        dense = jnp.zeros_like(by_slot)
        for j in range(16):
            dense = dense + jnp.where(place[...] == j, by_slot[j : j + 1], 0.0)
        lane = lax.broadcasted_iota(jnp.int32, dense.shape, 1)
        by_token = ids[...].T
        picked = jnp.zeros_like(dense)
        for k in range(ids.shape[0]):
            value = jnp.sum(
                jnp.where(lane == by_token[:, k : k + 1], dense, 0.0), axis=1, keepdims=True
            )
            picked = picked + jnp.where(lane == k, value, 0.0)
        combine_grad[...] = picked.T[: ids.shape[0]]
        inner = jnp.sum(gates[...] * dense, axis=1, keepdims=True)
        prob_grad = jnp.where(place[...] >= 0, (dense - inner) / scale[...], 0.0)
        top = ids.shape[0]
        fraction = dense.shape[1] * counts[...] / (top * tokens * RING * RING)
        prob_grad = prob_grad + aux[0] * fraction
        mean = jnp.sum(probs[...] * prob_grad, axis=1, keepdims=True)
        logit_grad[...] = (probs[...] * (prob_grad - mean)).astype(jnp.bfloat16)

        def one_tile(n, carry):
            columns = pl.ds(pl.multiple_of(n * LANES, LANES), LANES)
            term = lax.dot_general(
                inputs[:, columns],
                logit_grad[...],
                (((0,), (0,)), ((), ())),
                preferred_element_type=jnp.float32,
            )
            for m in range(2):
                for core in range(2):
                    terms[core, n // 8, (n // 2) % 4, 2 * (n % 2) + m] = term[
                        64 * m + 32 * core : 64 * m + 32 * core + 32
                    ]
            return carry

        lax.fori_loop(0, inputs.shape[1] // LANES, one_tile, 0)
        wires.send(terms.at[1 - here.core], other_terms, here.partner(), ("r0",))

    def chip_sum():
        wires.arrived(other_terms, ("r0",), here.partner())

        def one(n, carry):
            z, x = n // RING, n % RING
            terms[here.core, z, x] = terms[here.core, z, x] + other_terms[z, x]
            return carry

        lax.fori_loop(0, RING * RING, one, 0)

    def band_of(q, level, coordinate):
        where = [slice(None)] * 3
        for axis in ORDERS[q][:level]:
            where[axis] = here.at[axis]
        where[ORDERS[q][level]] = coordinate
        return (here.core, *where, pl.ds(*bands[q]), slice(None))

    def sum_send(level):
        for q in range(3):
            axis = ORDERS[q][level]
            for n, step in enumerate(steps):
                wires.send(
                    terms.at[band_of(q, level, here.along(axis, step))],
                    sums[level][q].at[n],
                    here.near(axis, step),
                    ("r", level, q, step),
                )

    def sum_in(level):
        for q in range(3):
            axis = ORDERS[q][level]
            for n, step in enumerate(steps):
                wires.arrived(
                    sums[level][q].at[n], ("r", level, q, step), here.near(axis, -step)
                )
            own = band_of(q, level, here.at[axis])
            landed = sums[level][q]
            terms[own] = terms[own] + landed[0] + landed[1] + landed[2]

    def sum_out():
        for q in range(3):
            span = pl.ds(*bands[q])
            router_grad[span] = terms[here.core, here.at[0], here.at[1], here.at[2], span]

    def stage_copy(p, k, b_step):
        start, size = parts[p]
        b_index = here.along(ORDERS[p][1], b_step)
        slot = (k * 3 + p) % 2
        return pltpu.make_async_copy(
            stage.at[slot, :, :, :, :, pl.ds(0, size)],
            back.at[(*fixed_b(ORDERS[p], b_index), slice(None), slice(None), pl.ds(start, size))],
            bs.at[slot],
        )

    def produce(p, k, b_step):
        start, size = parts[p]
        b_index = here.along(ORDERS[p][1], b_step)
        slot = (k * 3 + p) % 2
        units = grad_first.shape[-1]
        if k == 0:
            fetches[2 * p].wait()
            fetches[2 * p + 1].wait()
        for copy in given_copies(p, k, b_step):
            copy.wait()

        def columns(offset, width):
            span = pl.ds(start + offset, width)
            total = 0.0
            for n, weight in enumerate((gate, up)):
                total = total + lax.dot_general(
                    given[slot, n].reshape(512, units),
                    weight[span],
                    (((1,), (1,)), ((), ())),
                    preferred_element_type=jnp.float32,
                )
            stage[slot, :, :, :, :, pl.ds(offset, width)] = total.astype(jnp.bfloat16).reshape(
                RING, RING, 2, 16, width
            )

        def tile(n, carry):
            columns(pl.multiple_of(n * 256, 256), 256)
            return carry

        lax.fori_loop(0, size // 256, tile, 0)
        if size % 256:
            columns(size // 256 * 256, size % 256)
        stage_copy(p, k, b_step).start()

    def pieces(p, b_index, s_index, c_index):
        start, size = parts[p]
        return slots_of(back, ORDERS[p], b_index, s_index, c_index, start, size)

    def give(p, k, b_step):
        a, b, s = ORDERS[p]
        b_index = here.along(b, b_step)
        mine = rows[p].at[b_index, :, here.at[s] * 2 + here.core]
        way = 1 if k % 2 == 0 else -1
        wires.send(
            pieces(p, b_index, here.along(s, 2), slice(None)),
            relay[p].at[k],
            here.near(s, way),
            (p, "relay", k),
        )
        for step in (1, -1):
            for other in (0, 1):
                core = 1 - here.core if other else here.core
                wires.send(
                    pieces(p, b_index, here.along(s, step), core),
                    mine,
                    here.near(s, step, other),
                    (p, "near", step, other, k),
                )
        wires.send(
            pieces(p, b_index, here.at[s], 1 - here.core), mine, here.partner(), (p, "chip", k)
        )
        copy = pltpu.make_async_copy(
            pieces(p, b_index, here.at[s], here.core), mine, ls.at[len(local)]
        )
        copy.start()
        local.append(copy)

    def forward(p, k, b_step):
        a, b, s = ORDERS[p]
        b_index = here.along(b, b_step)
        way = 1 if k % 2 == 0 else -1
        wires.arrived(relay[p].at[k], (p, "relay", k), here.near(s, -way))
        theirs = rows[p].at[b_index, :, here.along(s, -way) * 2 + here.core]
        for other in (0, 1):
            core = 1 - here.core if other else here.core
            wires.send(
                relay[p].at[k, :, core], theirs, here.near(s, way, other), (p, "far", other, k)
            )

    def gathered(p, k, b_step):
        a, b, s = ORDERS[p]
        b_index = here.along(b, b_step)
        way = 1 if k % 2 == 0 else -1
        for other in (0, 1):
            core = 1 - here.core if other else here.core
            for step in (1, -1):
                wires.arrived(
                    rows[p].at[b_index, :, here.along(s, -step) * 2 + core],
                    (p, "near", step, other, k),
                    here.near(s, -step, other),
                )
            wires.arrived(
                rows[p].at[b_index, :, here.along(s, 2) * 2 + core],
                (p, "far", other, k),
                here.near(s, -way, other),
            )
        wires.arrived(
            rows[p].at[b_index, :, here.at[s] * 2 + (1 - here.core)],
            (p, "chip", k),
            here.partner(),
        )
        local[k * 3 + p].wait()

    def add_up(p, b_step):
        a, b, s = ORDERS[p]
        b_index = here.along(b, b_step)
        size = parts[p][1]

        def one(a_index, carry):
            token_of = lines[p, b_index, a_index, pl.ds(0, 1), :]
            gate_of = lines[p, b_index, a_index, pl.ds(1, 1), :]
            token = lax.broadcasted_iota(jnp.int32, (tokens, LANES), 0).astype(jnp.float32)
            weigh = jnp.where(token == token_of, gate_of, 0.0).astype(jnp.bfloat16)
            total = jnp.dot(
                weigh,
                rows[p][b_index, a_index].reshape(LANES, size),
                preferred_element_type=jnp.float32,
            )
            rows[p][b_index, a_index] = total.astype(jnp.bfloat16).reshape(8, 16, size)
            return carry

        lax.fori_loop(0, RING, one, 0)

    def plus(*terms):
        total = terms[0].astype(jnp.float32)
        for term in terms[1:]:
            total = total + term.astype(jnp.float32)
        return total

    def fold2(p, way, k, step):
        a, b, s = ORDERS[p]
        b_index, a_index = here.along(b, way), here.along(a, step)
        slot = 0 if way == 1 else 1
        groups = pl.ds(0, 4) if way == 1 else pl.ds(4, 4)
        wires.arrived(halves2[p].at[slot, k], (p, "half2", way, k), here.near(b, -way))
        rows[p][b_index, a_index, groups] = plus(
            rows[p][b_index, a_index, groups], halves2[p][slot, k]
        ).astype(jnp.bfloat16)
        wires.send(
            rows[p].at[b_index, a_index],
            whole2[p].at[slot, k],
            here.near(b, way),
            (p, "whole2", way, k),
        )

    def settle2(p, k, step):
        a, b, s = ORDERS[p]
        for way in (1, -1):
            slot = 0 if way == 1 else 1
            wires.arrived(whole2[p].at[slot, k], (p, "whole2", way, k), here.near(b, -way))
        own = rows[p].at[here.at[b], here.along(a, step)]
        return plus(own[...], whole2[p][0, k], whole2[p][1, k])

    order = (2, 1, -1, 0)
    work = [(k, p) for k in range(4) for p in range(3)]

    def make(turn):
        k, p = work[turn]
        if turn + 1 < len(work):
            after_k, after_p = work[turn + 1]
            for copy in given_copies(after_p, after_k, order[after_k]):
                copy.start()
        produce(p, k, order[k])

    def post(turn):
        k, p = work[turn]
        stage_copy(p, k, order[k]).wait()
        give(p, k, order[k])

    def pass_on(k):
        for p in range(3):
            forward(p, k, order[k])

    def total(k):
        for p in range(3):
            gathered(p, k, order[k])
            add_up(p, order[k])

    def halve():
        for p, (a, b, s) in enumerate(ORDERS):
            far = here.along(b, 2)
            for k, step in enumerate(order):
                for way, groups in ((1, pl.ds(0, 4)), (-1, pl.ds(4, 4))):
                    wires.send(
                        rows[p].at[far, here.along(a, step), groups],
                        halves2[p].at[0 if way == 1 else 1, k],
                        here.near(b, way),
                        (p, "half2", way, k),
                    )

    def fold(way):
        for k, step in enumerate(order):
            for p in range(3):
                fold2(p, way, k, step)

    actions = {
        "make": make,
        "post": post,
        "pass": pass_on,
        "total": total,
        "halve": halve,
        "fold": fold,
        "line": values_line,
        "x": values_x,
        "z": values_z,
        "router": router_back,
        "chip": chip_sum,
        "send": sum_send,
        "in": sum_in,
    }
    for name, *given_to in COMBINE_PLAN:
        actions[name](*given_to)
    for p, (a, b, s) in enumerate(ORDERS):
        block = rows[p].at[here.at[b], here.along(a, 2)]
        block[...] = settle2(p, 0, 2).astype(jnp.bfloat16)
        for way, groups in ((1, pl.ds(0, 4)), (-1, pl.ds(4, 4))):
            wires.send(
                rows[p].at[here.at[b], here.along(a, 2), groups],
                halves1[p].at[0 if way == 1 else 1],
                here.near(a, way),
                (p, "half1", way),
            )
    for k, way in ((1, 1), (2, -1)):
        for p, (a, b, s) in enumerate(ORDERS):
            slot = 0 if way == 1 else 1
            groups = pl.ds(0, 4) if way == 1 else pl.ds(4, 4)
            block = rows[p].at[here.at[b], here.along(a, way)]
            block[...] = settle2(p, k, way).astype(jnp.bfloat16)
            wires.arrived(halves1[p].at[slot], (p, "half1", way), here.near(a, -way))
            part = rows[p].at[here.at[b], here.along(a, way), groups]
            part[...] = plus(part[...], halves1[p][slot]).astype(jnp.bfloat16)
            wires.send(block, whole1[p].at[slot], here.near(a, way), (p, "whole1", way))
    for p, (a, b, s) in enumerate(ORDERS):
        start, size = parts[p]
        total = settle2(p, 3, 0)
        for way in (1, -1):
            slot = 0 if way == 1 else 1
            wires.arrived(whole1[p].at[slot], (p, "whole1", way), here.near(a, -way))
        total = plus(total, whole1[p][0], whole1[p][1]).reshape(tokens, size)
        total = total + lax.dot_general(
            logit_grad[...],
            router[pl.ds(start, size)],
            (((1,), (1,)), ((), ())),
            preferred_element_type=jnp.float32,
        )
        out[:, pl.ds(start, size)] = total.astype(out.dtype)
    if ("in", 2) not in COMBINE_PLAN:
        sum_in(2)
    sum_out()
    wires.drain()


def combine(parts, values, grads, weights, lines, counts, inputs, router, probs, gates, place, scale, ids, aux):
    width, units = weights[0].shape
    top, tokens = ids.shape
    experts = probs.shape[1]

    def buffers(*lead):
        return [pltpu.VMEM((*lead, size), jnp.bfloat16) for _, size in parts]

    def floats(*shape):
        return pltpu.VMEM(shape, jnp.float32)

    hbm, vmem = pl.BlockSpec(memory_space=pltpu.HBM), pl.BlockSpec(memory_space=pltpu.VMEM)
    bands = (16, 8, 8)
    return pl.pallas_call(
        functools.partial(combine_kernel, parts),
        out_shape=(
            jax.ShapeDtypeStruct((tokens, width), jnp.bfloat16),
            jax.ShapeDtypeStruct((top, tokens), jnp.float32),
            jax.ShapeDtypeStruct((width // (2 * RING**3), experts), jnp.float32),
            jax.ShapeDtypeStruct((RING, RING, RING, 2, 16, width), jnp.bfloat16),
        ),
        in_specs=[vmem, hbm, hbm, hbm, hbm]
        + [vmem] * 9
        + [pl.BlockSpec(memory_space=pltpu.SMEM)],
        out_specs=(vmem, vmem, vmem, hbm),
        scratch_shapes=buffers(RING, RING, 8, 16)
        + buffers(RING, RING, 2, 16)
        + buffers(2, RING, 4, 16)
        + buffers(2, RING, 8, 16)
        + buffers(2, 4, 16)
        + buffers(2, 8, 16)
        + [
            pltpu.VMEM((width, units), jnp.bfloat16),
            pltpu.VMEM((width, units), jnp.bfloat16),
            pltpu.VMEM((2, RING, RING, 2, 16, parts[0][1]), jnp.bfloat16),
            pltpu.VMEM((2, 2, RING, RING, 2, 16, units), jnp.bfloat16),
            floats(8, RING, RING, 1, LANES),
            floats(RING, 8, RING, 1, LANES),
            floats(RING, RING, 8, 1, LANES),
            floats(experts, LANES),
            pltpu.VMEM((tokens, experts), jnp.bfloat16),
            floats(2, RING, RING, RING, 32, experts),
            floats(RING, RING, RING, 32, experts),
        ]
        + [floats(3, RING, RING, band, experts) for band in bands]
        + [floats(3, RING, band, experts) for band in bands]
        + [floats(3, band, experts) for band in bands]
        + [
            pltpu.SemaphoreType.DMA((224,)),
            pltpu.SemaphoreType.DMA((224,)),
            pltpu.SemaphoreType.DMA((16,)),
            pltpu.SemaphoreType.DMA((12,)),
        ],
        compiler_params=pltpu.CompilerParams(
            collective_id=1, has_side_effects=True, vmem_limit_bytes=67043328
        ),
    )(values, *grads, *weights, lines, counts, inputs, router, probs, gates, place, scale, ids, aux)[:3]


def hidden_backward(upstream, pre_gate, pre_up):
    first = pre_gate.astype(jnp.float32)
    second = pre_up.astype(jnp.float32)
    gate_sig = jax.nn.sigmoid(first)
    gate_act = first * gate_sig
    hidden = gate_act * second
    slot_combine = jnp.sum(upstream * hidden, axis=-1).astype(jnp.bfloat16)
    grad_first = (upstream * second * gate_sig * (1.0 + first * (1.0 - gate_sig))).astype(
        jnp.bfloat16
    )
    grad_second = (upstream * gate_act).astype(jnp.bfloat16)
    return grad_first, grad_second, slot_combine


def shards(
    tokens,
    out_grad,
    router_weight,
    gate_weight,
    up_weight,
    down_weight,
    saved_gate,
    saved_up,
    expert_ids,
    aux_weight,
):
    devices = lax.axis_size(AXES)
    inputs, upstream_grad, chosen_ids = tokens[0], out_grad[0], expert_ids[0].T
    model_width = inputs.shape[1]
    capacity = saved_gate.shape[1] // devices
    parts = column_parts(model_width)

    upstream, lines, counts, probs, gates, place, chosen_sum = dispatch(
        parts, upstream_grad, inputs, router_weight, chosen_ids, down_weight[0]
    )
    grad_first, grad_second, slot_combine = hidden_backward(
        upstream,
        saved_gate[0].reshape(upstream.shape),
        saved_up[0].reshape(upstream.shape),
    )
    values = slot_combine.astype(jnp.float32).reshape(*upstream.shape[:4], 1, capacity)
    values = jnp.pad(values, [(0, 0)] * 5 + [(0, LANES - capacity)])
    token_grad, combine_grad, router_grad = combine(
        parts,
        values,
        (grad_first, grad_second),
        (gate_weight[0], up_weight[0]),
        lines,
        counts,
        inputs,
        router_weight,
        probs,
        gates,
        place,
        chosen_sum,
        chosen_ids,
        aux_weight,
    )
    return (token_grad[None], combine_grad.T[None], router_grad)


def solution(mesh):
    torus = Mesh(mesh.devices.reshape(RING, RING, RING, 2), AXES)
    return jax.shard_map(
        shards,
        mesh=torus,
        in_specs=(
            P(EXP, SEQ, None),
            P(EXP, SEQ, None),
            P(),
            P(AXES, None, None),
            P(AXES, None, None),
            P(AXES, None, None),
            P(AXES, None, None),
            P(AXES, None, None),
            P(EXP, SEQ, None),
            P(),
        ),
        out_specs=(P(EXP, SEQ, None), P(EXP, SEQ, None), P(AXES, None)),
        check_vma=False,
    )
```

```python
import functools

import jax
import jax.numpy as jnp
from jax import lax
from jax.experimental import pallas as pl
from jax.experimental.pallas import tpu as pltpu
from jax.sharding import Mesh
from jax.sharding import PartitionSpec as P

SEQ = ("seq_0", "seq_1")
EXP = ("exp_0", "exp_1")
AXES = ("seq_0", "seq_1", "exp_0", "exp_1")
MESH = pl.DeviceIdType.MESH
RING = 4
LANES = 128
ORDERS = ((0, 1, 2), (1, 2, 0), (2, 0, 1))
STRIDES = (32, 8, 2)
DISPATCH_PLAN = (
    ("relay", 0), ("choose", 0), ("relay", 1), ("relay", 2), ("relay", 3), ("choose", 1), ("pass", 0),
    ("choose", 2), ("far",), ("pass", 1), ("choose", 3), ("clear",),
    ("near", 0), ("pass", 2), ("near", 1), ("distant", 0), ("pass", 3), ("near", 2),
    ("distant", 1), ("near", 3), ("distant", 2), ("distant", 3),
)
COMBINE_PLAN = (
    ("line",), ("make", 0), ("post", 0), ("make", 1), ("post", 1), ("make", 2), ("post", 2), ("x",),
    ("make", 3), ("post", 3), ("make", 4), ("post", 4), ("pass", 0), ("make", 5), ("post", 5), ("z",),
    ("make", 6), ("post", 6), ("make", 7), ("post", 7), ("pass", 1), ("make", 8), ("post", 8),
    ("total", 0), ("halve",), ("router",), ("make", 9), ("post", 9), ("pass", 2), ("make", 10), ("post", 10),
    ("make", 11), ("post", 11), ("chip",), ("send", 0), ("pass", 3),
    ("total", 1), ("fold", 1), ("in", 0), ("send", 1),
    ("total", 2), ("fold", -1), ("in", 1), ("send", 2), ("total", 3),
)


def column_parts(width):
    tiles = width // LANES
    sizes = [(tiles + 2 - p) // 3 * LANES for p in range(3)]
    starts = [0, sizes[0], sizes[0] + sizes[1]]
    return list(zip(starts, sizes))


class Wires:
    def __init__(self, send_sems, recv_sems):
        self.send_sems, self.recv_sems = send_sems, recv_sems
        self.sent, self.names = [], {}

    def slot(self, name):
        return self.recv_sems.at[self.names.setdefault(name, len(self.names))]

    def send(self, src, dst, device, name):
        copy = pltpu.make_async_remote_copy(
            src, dst, self.send_sems.at[len(self.sent)], self.slot(name), device, MESH
        )
        copy.start()
        self.sent.append(copy)

    def arrived(self, ref, name, device):
        pltpu.make_async_remote_copy(
            ref, ref, self.send_sems.at[0], self.slot(name), device, MESH
        ).wait_recv()

    def drain(self):
        for copy in self.sent:
            copy.wait_send()


class Place:
    def __init__(self):
        self.at = [lax.axis_index(name) for name in AXES]
        self.core = self.at[3]

    def along(self, axis, step):
        return lax.rem(self.at[axis] + (step + RING), RING)

    def near(self, axis, step, other_core=0):
        coords = list(self.at)
        coords[axis] = self.along(axis, step)
        if other_core:
            coords[3] = 1 - self.core
        return tuple(coords)

    def partner(self):
        return (self.at[0], self.at[1], self.at[2], 1 - self.core)

    def greet(self, steps=(1, -1)):
        barrier = pltpu.get_barrier_semaphore()
        peers = [self.partner()]
        for axis in range(3):
            for step in steps:
                for other in (0, 1):
                    peers.append(self.near(axis, step, other))
        for peer in peers:
            pl.semaphore_signal(barrier, inc=1, device_id=peer, device_id_type=MESH)
        pl.semaphore_wait(barrier, len(peers))


def slots_of(ref, order, b_index, s_index, c_index, start, size):
    a, b, s = order
    where = [None] * 3
    where[a], where[b], where[s] = slice(None), b_index, s_index
    return ref.at[where[0], where[1], where[2], c_index, :, pl.ds(start, size)]


def fixed_b(order, b_index):
    where = [slice(None)] * 3
    where[order[1]] = b_index
    return tuple(where)


def dispatch_kernel(
    parts, grad, inputs, router, ids, down, saved_gate, saved_up,
    slots, grad_first, grad_second, values, lines, counts, probs, gates, place, scale,
    g0, g1, g2, o0, o1, o2, l0, l1, l2, seen, picks, tokens_in, router_in, weight, batch, last,
    upstream, before, after, ss, rs, ls, bs, hs,
):
    held, outgoing, relay = (g0, g1, g2), (o0, o1, o2), (l0, l1, l2)
    here = Place()
    wires = Wires(ss, rs)
    tokens = grad.shape[0]
    half = tokens // 2
    local = []

    def keep(src, dst):
        copy = pltpu.make_async_copy(src, dst, ls.at[len(local)])
        copy.start()
        local.append(copy)

    for p, (a, b, s) in enumerate(ORDERS):
        start, size = parts[p]
        keep(grad.at[:, pl.ds(start, size)], held[p].at[here.at[b], here.at[a]])
    fetches = [
        pltpu.make_async_copy(src, dst, bs.at[8 + n])
        for n, (src, dst) in enumerate(((inputs, tokens_in), (router, router_in), (down, weight)))
    ]
    here.greet()
    for copy in local:
        copy.wait()
    for copy in fetches[:2]:
        copy.start()

    def pass_on(p, k, step):
        a, b, s = ORDERS[p]
        block = held[p].at[here.at[b], here.along(a, step)]
        wires.send(block, block, here.near(b, 1), (p, "m2", 1, k))
        wires.send(block, block, here.near(b, -1), (p, "m2", -1, k))

    def relay_on(p, k, step):
        a, b, s = ORDERS[p]
        for way, rows in ((1, pl.ds(0, half)), (-1, pl.ds(half, half))):
            block = held[p].at[here.along(b, -way), here.along(a, step)]
            wires.arrived(block, (p, "m2", way, k), here.near(b, -way))
            piece = held[p].at[here.along(b, -way), here.along(a, step), rows]
            wires.send(piece, piece, here.near(b, way), (p, "m2far", way, k))

    def far_in(p, k, step):
        a, b, s = ORDERS[p]
        for way, rows in ((1, pl.ds(0, half)), (-1, pl.ds(half, half))):
            piece = held[p].at[here.along(b, 2), here.along(a, step), rows]
            wires.arrived(piece, (p, "m2far", way, k), here.near(b, -way))

    def route():
        experts = router.shape[1]
        row = lax.broadcasted_iota(jnp.int32, (tokens, experts), 0)
        lane = lax.broadcasted_iota(jnp.int32, (tokens, experts), 1)
        mask = jnp.zeros((tokens, experts), jnp.float32)
        by_token = ids[...].T
        for k in range(ids.shape[0]):
            mask = mask + jnp.where(lane == by_token[:, k : k + 1], 1.0, 0.0)
        before = jnp.where(row > lane, 1.0, 0.0).astype(jnp.bfloat16)
        rank = jnp.dot(before, mask.astype(jnp.bfloat16), preferred_element_type=jnp.float32)
        place[...] = jnp.where(mask > 0, rank, -1.0)
        logits = jnp.dot(tokens_in[...], router_in[...], preferred_element_type=jnp.float32)
        powers = jnp.exp(logits - jnp.max(logits, axis=1, keepdims=True))
        probs[...] = powers / jnp.sum(powers, axis=1, keepdims=True)
        chosen = probs[...] * mask
        scale[...] = jnp.sum(chosen, axis=1, keepdims=True)
        gates[...] = chosen / scale[...]
        slot = lax.broadcasted_iota(jnp.int32, (16, experts), 0)
        token_of = jnp.zeros((16, experts), jnp.float32)
        gate_of = jnp.zeros((16, experts), jnp.float32)
        offset = (row - tokens).astype(jnp.float32)
        for j in range(16):
            hit = place[...] == j
            token = jnp.sum(jnp.where(hit, offset, 0.0), axis=0, keepdims=True) + tokens
            gate = jnp.sum(jnp.where(hit, gates[...], 0.0), axis=0, keepdims=True)
            token_of = jnp.where(slot == j, token, token_of)
            gate_of = jnp.where(slot == j, gate, gate_of)
        count = jnp.where(slot == 0, jnp.sum(mask, axis=0, keepdims=True), 0.0)
        for p, (a, b, s) in enumerate(ORDERS):
            for n, part in enumerate((token_of, gate_of, count)):
                seen[p, here.at[b], here.at[a], pl.ds(16 * n, 16), :] = part.astype(jnp.bfloat16)
        for p, (a, b, s) in enumerate(ORDERS):
            first = here.at[a] * STRIDES[a] + here.at[b] * STRIDES[b]
            expert = first + lane // 32 * STRIDES[s] + lane // 16 % 2
            picks[p] = jnp.where(row == expert, 1.0, 0.0).astype(jnp.bfloat16)

    for p, (a, b, s) in enumerate(ORDERS):
        block = held[p].at[here.at[b], here.at[a]]
        for way in (1, -1):
            wires.send(block, block, here.near(a, way), (p, "m1", way))
    for copy in fetches[:2]:
        copy.wait()
    fetches[2].start()
    route()
    for p, (a, b, s) in enumerate(ORDERS):
        table = seen.at[p, here.at[b], here.at[a]]
        for way in (1, -1):
            wires.send(table, table, here.near(a, way), (p, "t1", way))
    for p in range(3):
        pass_on(p, 0, 0)
    for p, (a, b, s) in enumerate(ORDERS):
        table = seen.at[p, here.at[b], here.along(a, -1)]
        wires.arrived(table, (p, "t1", 1), here.near(a, -1))
        wires.send(table, table, here.near(a, 1), (p, "t1far"))
        wires.arrived(
            seen.at[p, here.at[b], here.along(a, 1)], (p, "t1", -1), here.near(a, 1)
        )
    for p, (a, b, s) in enumerate(ORDERS):
        for way, rows in ((1, pl.ds(0, half)), (-1, pl.ds(half, half))):
            block = held[p].at[here.at[b], here.along(a, -way)]
            wires.arrived(block, (p, "m1", way), here.near(a, -way))
            piece = held[p].at[here.at[b], here.along(a, -way), rows]
            wires.send(piece, piece, here.near(a, way), (p, "m1far", way))
    for p, (a, b, s) in enumerate(ORDERS):
        wires.arrived(
            seen.at[p, here.at[b], here.along(a, 2)], (p, "t1far"), here.near(a, -1)
        )
        table = seen.at[p, here.at[b]]
        for way in (1, -1):
            wires.send(table, table, here.near(b, way), (p, "t2", way))
    for p in range(3):
        pass_on(p, 1, -1)
        pass_on(p, 2, 1)
    for p, (a, b, s) in enumerate(ORDERS):
        table = seen.at[p, here.along(b, -1)]
        wires.arrived(table, (p, "t2", 1), here.near(b, -1))
        wires.send(table, table, here.near(b, 1), (p, "t2far"))
        wires.arrived(seen.at[p, here.along(b, 1)], (p, "t2", -1), here.near(b, 1))
    for p, (a, b, s) in enumerate(ORDERS):
        for way, rows in ((1, pl.ds(0, half)), (-1, pl.ds(half, half))):
            piece = held[p].at[here.at[b], here.along(a, 2), rows]
            wires.arrived(piece, (p, "m1far", way), here.near(a, -way))
        pass_on(p, 3, 2)

    def select(p, k, b_step):
        a, b, s = ORDERS[p]
        b_index = here.along(b, b_step)
        size = parts[p][1]
        found = jnp.dot(
            seen[p, b_index].reshape(RING * 48, LANES),
            picks[p],
            preferred_element_type=jnp.float32,
        ).reshape(RING, 3, 16, LANES)
        slot = lax.broadcasted_iota(jnp.int32, found.shape, 2)
        lane = lax.broadcasted_iota(jnp.int32, found.shape, 3)
        found = jnp.sum(jnp.where(slot == lane % 16, found, 0.0), axis=2)
        for a_index in range(RING):
            for n in range(2):
                lines[p, b_index, a_index, pl.ds(n, 1), :] = found[a_index, n : n + 1]

        def one(a_index, carry):
            token_of = lines[p, b_index, a_index, pl.ds(0, 1), :]
            token = lax.broadcasted_iota(jnp.int32, (tokens, LANES), 0).astype(jnp.float32)
            pick = jnp.where(token == token_of, 1.0, 0.0).astype(jnp.bfloat16)
            rows = lax.dot_general(
                pick,
                held[p][b_index, a_index],
                (((0,), (0,)), ((), ())),
                preferred_element_type=jnp.float32,
            )
            outgoing[p][k, :, a_index] = rows.astype(jnp.bfloat16).reshape(8, 16, size)
            return carry

        lax.fori_loop(0, RING, one, 0)

    def deliver(p, k, b_step):
        order = ORDERS[p]
        a, b, s = order
        start, size = parts[p]
        b_index = here.along(b, b_step)
        mine = slots_of(slots, order, b_index, here.at[s], here.core, start, size)
        way = 1 if k % 2 == 0 else -1
        wires.send(
            outgoing[p].at[k, pl.ds(here.along(s, 2) * 2, 2)],
            relay[p].at[k],
            here.near(s, way),
            (p, "relay", k),
        )
        for step in (1, -1):
            for other in (0, 1):
                core = 1 - here.core if other else here.core
                wires.send(
                    outgoing[p].at[k, here.along(s, step) * 2 + core],
                    mine,
                    here.near(s, step, other),
                    (p, "near", step, other, k),
                )
        wires.send(
            outgoing[p].at[k, here.at[s] * 2 + (1 - here.core)],
            mine,
            here.partner(),
            (p, "chip", k),
        )
        keep(outgoing[p].at[k, here.at[s] * 2 + here.core], mine)

    def forward(p, k, b_step):
        order = ORDERS[p]
        a, b, s = order
        start, size = parts[p]
        b_index = here.along(b, b_step)
        way = 1 if k % 2 == 0 else -1
        wires.arrived(relay[p].at[k], (p, "relay", k), here.near(s, -way))
        theirs = slots_of(slots, order, b_index, here.along(s, -way), here.core, start, size)
        for other in (0, 1):
            core = 1 - here.core if other else here.core
            wires.send(
                relay[p].at[k, core], theirs, here.near(s, way, other), (p, "far", other, k)
            )

    def near_in(p, k):
        order = ORDERS[p]
        a, b, s = order
        start, size = parts[p]
        b_index = here.along(b, turns[k])
        for other in (0, 1):
            core = 1 - here.core if other else here.core
            for step in (1, -1):
                wires.arrived(
                    slots_of(slots, order, b_index, here.along(s, -step), core, start, size),
                    (p, "near", step, other, k),
                    here.near(s, -step, other),
                )
        wires.arrived(
            slots_of(slots, order, b_index, here.at[s], 1 - here.core, start, size),
            (p, "chip", k),
            here.partner(),
        )
        local[3 + k * 3 + p].wait()

    def distant_in(p, k):
        order = ORDERS[p]
        a, b, s = order
        start, size = parts[p]
        b_index = here.along(b, turns[k])
        way = 1 if k % 2 == 0 else -1
        for other in (0, 1):
            core = 1 - here.core if other else here.core
            wires.arrived(
                slots_of(slots, order, b_index, here.along(s, 2), core, start, size),
                (p, "far", other, k),
                here.near(s, -way, other),
            )

    def copies(p, k, senders):
        order = ORDERS[p]
        start, size = parts[p]
        b_index = here.along(order[1], turns[k])
        slot = (k * 3 + p) % 2
        target, first = (batch, 3 * slot) if len(senders) == 3 else (last, 6 + slot)
        return [
            pltpu.make_async_copy(
                slots_of(
                    slots, order, b_index, here.along(order[2], step), slice(None), start, size
                ),
                target.at[slot, n, :, :, :, pl.ds(0, size)],
                bs.at[first + n],
            )
            for n, step in enumerate(senders)
        ]

    def project(p, k, senders):
        a, b, s = ORDERS[p]
        start, size = parts[p]
        b_index = here.along(b, turns[k])
        slot = (k * 3 + p) % 2
        source = batch if len(senders) == 3 else last
        for copy in copies(p, k, senders):
            copy.wait()

        def tile(n, carry):
            units = pl.ds(pl.multiple_of(n * 256, 256), 256)
            term = lax.dot_general(
                source[slot, :, :, :, :, pl.ds(0, size)].reshape(len(senders) * LANES, size),
                weight[units, pl.ds(start, size)],
                (((1,), (1,)), ((), ())),
                preferred_element_type=jnp.float32,
            ).reshape(len(senders), RING, 2, 16, 256)
            for m, step in enumerate(senders):
                where = [slice(None)] * 3
                where[b], where[s] = b_index, here.along(s, step)
                there = (*where, slice(None), slice(None), units)
                upstream[there] = upstream[there] + term[m]
            return carry

        lax.fori_loop(0, 3, tile, 0)

    turns = (0, -1, 1, 2)
    joined = (0, -1, 1, 2)

    def relays(k):
        for p in range(3):
            relay_on(p, k, joined[k])

    def choose(k):
        for p in range(3):
            select(p, k, turns[k])
            deliver(p, k, turns[k])

    def far_rows():
        for p, (a, b, s) in enumerate(ORDERS):
            for k in range(RING):
                far_in(p, k, joined[k])
            wires.arrived(seen.at[p, here.along(b, 2)], (p, "t2far"), here.near(b, -1))

    def pass_far(k):
        for p in range(3):
            forward(p, k, turns[k])

    def clear():
        total = jnp.sum(seen[0, :, :, pl.ds(32, 16), :].astype(jnp.float32), axis=(0, 1))
        counts[...] = jnp.sum(total, axis=0, keepdims=True)
        upstream[...] = jnp.zeros_like(upstream)
        fetches[2].wait()
        for n in range(2):
            for copy in saved_copies(n):
                copy.start()

    def saved_copies(n):
        return [
            pltpu.make_async_copy(
                src.at[n // RING, n % RING], before.at[n % 2, i], hs.at[2 * (n % 2) + i]
            )
            for i, src in enumerate((saved_gate, saved_up))
        ]

    def grad_copies(n):
        return [
            pltpu.make_async_copy(
                after.at[n % 2, i], dst.at[n // RING, n % RING], hs.at[4 + 2 * (n % 2) + i]
            )
            for i, dst in enumerate((grad_first, grad_second))
        ]

    def units_back():
        rows = RING * RING

        def one_block(n, carry):
            z, x, slot = n // RING, n % RING, n % 2
            for copy in saved_copies(n):
                copy.wait()

            @pl.when(n >= 2)
            def _():
                for copy in grad_copies(n):
                    copy.wait()

            def one_source(m, carry):
                y, core = m // 2, m % 2
                up = upstream[z, x, y, core]
                first = before[slot, 0, y, core].astype(jnp.float32)
                second = before[slot, 1, y, core].astype(jnp.float32)
                sig = jax.nn.sigmoid(first)
                act = first * sig
                total = jnp.sum(up * (act * second), axis=-1, keepdims=True)
                total = total.astype(jnp.bfloat16).astype(jnp.float32)
                row = lax.broadcasted_iota(jnp.int32, (16, LANES), 0)
                lane = lax.broadcasted_iota(jnp.int32, (16, LANES), 1)
                values[z, x, y, core] = jnp.sum(
                    jnp.where(row == lane, total, 0.0), axis=0, keepdims=True
                )
                after[slot, 0, y, core] = (
                    up * second * sig * (1.0 + first * (1.0 - sig))
                ).astype(jnp.bfloat16)
                after[slot, 1, y, core] = (up * act).astype(jnp.bfloat16)
                return carry

            lax.fori_loop(0, 2 * RING, one_source, 0, unroll=8)
            for copy in grad_copies(n):
                copy.start()

            @pl.when(n + 2 < rows)
            def _():
                for copy in saved_copies(n + 2):
                    copy.start()

            return carry

        lax.fori_loop(0, rows, one_block, 0)
        for n in (rows - 2, rows - 1):
            for copy in grad_copies(n):
                copy.wait()

    def multiply(k, arrive, senders):
        def fetch(p):
            arrive(p, k)
            for copy in copies(p, k, senders):
                copy.start()

        fetch(0)
        for p in range(3):
            if p < 2:
                fetch(p + 1)
            project(p, k, senders)

    actions = {
        "relay": relays,
        "choose": choose,
        "far": far_rows,
        "pass": pass_far,
        "clear": clear,
        "near": lambda k: multiply(k, near_in, (0, 1, -1)),
        "distant": lambda k: multiply(k, distant_in, (2,)),
    }
    for name, *given_to in DISPATCH_PLAN:
        actions[name](*given_to)
    units_back()
    wires.drain()


def dispatch(parts, grad, inputs, router, ids, down, saved_gate, saved_up):
    tokens, width = grad.shape
    units, experts = down.shape[0], router.shape[1]
    rows = [pltpu.VMEM((RING, RING, tokens, size), jnp.bfloat16) for _, size in parts]
    outs = [pltpu.VMEM((RING, 8, RING, 16, size), jnp.bfloat16) for _, size in parts]
    relays = [pltpu.VMEM((RING, 2, RING, 16, size), jnp.bfloat16) for _, size in parts]
    hbm, vmem = pl.BlockSpec(memory_space=pltpu.HBM), pl.BlockSpec(memory_space=pltpu.VMEM)
    square = jax.ShapeDtypeStruct((tokens, experts), jnp.float32)
    return pl.pallas_call(
        functools.partial(dispatch_kernel, parts),
        out_shape=(
            jax.ShapeDtypeStruct((RING, RING, RING, 2, 16, width), jnp.bfloat16),
            jax.ShapeDtypeStruct((RING, RING, RING, 2, 16, units), jnp.bfloat16),
            jax.ShapeDtypeStruct((RING, RING, RING, 2, 16, units), jnp.bfloat16),
            jax.ShapeDtypeStruct((RING, RING, RING, 2, 1, LANES), jnp.float32),
            jax.ShapeDtypeStruct((3, RING, RING, 8, LANES), jnp.float32),
            jax.ShapeDtypeStruct((1, experts), jnp.float32),
            square,
            square,
            square,
            jax.ShapeDtypeStruct((tokens, 1), jnp.float32),
        ),
        in_specs=[hbm, hbm, hbm, vmem, hbm, hbm, hbm],
        out_specs=(hbm,) * 3 + (vmem,) * 7,
        scratch_shapes=rows
        + outs
        + relays
        + [
            pltpu.VMEM((3, RING, RING, 48, LANES), jnp.bfloat16),
            pltpu.VMEM((3, experts, LANES), jnp.bfloat16),
            pltpu.VMEM((tokens, width), jnp.bfloat16),
            pltpu.VMEM((width, experts), jnp.bfloat16),
            pltpu.VMEM((units, width), jnp.bfloat16),
            pltpu.VMEM((2, 3, RING, 2, 16, parts[0][1]), jnp.bfloat16),
            pltpu.VMEM((2, 1, RING, 2, 16, parts[0][1]), jnp.bfloat16),
            pltpu.VMEM((RING, RING, RING, 2, 16, units), jnp.float32),
            pltpu.VMEM((2, 2, RING, 2, 16, units), jnp.bfloat16),
            pltpu.VMEM((2, 2, RING, 2, 16, units), jnp.bfloat16),
            pltpu.SemaphoreType.DMA((192,)),
            pltpu.SemaphoreType.DMA((192,)),
            pltpu.SemaphoreType.DMA((32,)),
            pltpu.SemaphoreType.DMA((11,)),
            pltpu.SemaphoreType.DMA((8,)),
        ],
        compiler_params=pltpu.CompilerParams(
            collective_id=0, has_side_effects=True, vmem_limit_bytes=62 * 2**20
        ),
    )(grad, inputs, router, ids, down, saved_gate, saved_up)[1:]


def combine_kernel(
    parts, values, grad_first, grad_second, w_gate, w_up, lines, counts, inputs, router,
    probs, gates, place, scale, ids, aux,
    out, combine_grad, router_grad, back,
    q0, q1, q2, l0, l1, l2, x0, x1, x2, y0, y1, y2, u0, u1, u2, v0, v1, v2,
    gate, up, stage, given, h1, h2, h3, flat, logit_grad, terms, other_terms,
    e10, e11, e12, e20, e21, e22, e30, e31, e32, ss, rs, ls, bs,
):
    rows, relay = (q0, q1, q2), (l0, l1, l2)
    halves2, whole2 = (x0, x1, x2), (y0, y1, y2)
    halves1, whole1 = (u0, u1, u2), (v0, v1, v2)
    sums = ((e10, e11, e12), (e20, e21, e22), (e30, e31, e32))
    bands = ((0, 16), (16, 8), (24, 8))
    steps = (1, -1, 2)
    here = Place()
    wires = Wires(ss, rs)
    tokens = out.shape[0]
    local = []
    fetches = []
    for p, (start, size) in enumerate(parts):
        for n, (src, dst) in enumerate(((w_gate, gate), (w_up, up))):
            span = pl.ds(start, size)
            copy = pltpu.make_async_copy(src.at[span], dst.at[span], bs.at[6 + 2 * p + n])
            fetches.append(copy)
    for copy in fetches[:2]:
        copy.start()

    def given_copies(p, k, b_step):
        slot = (k * 3 + p) % 2
        where = fixed_b(ORDERS[p], here.along(ORDERS[p][1], b_step))
        return [
            pltpu.make_async_copy(src.at[where], given.at[slot, n], bs.at[2 + 2 * slot + n])
            for n, src in enumerate((grad_first, grad_second))
        ]

    for copy in given_copies(0, 0, 2):
        copy.start()
    here.greet(steps)
    for copy in fetches[2:]:
        copy.start()

    def values_line():
        mine = here.at[2] * 2 + here.core
        h1[mine] = values[:, :, here.at[2], here.core]
        for step in (0, *steps):
            for other in (0, 1):
                if step or other:
                    core = 1 - here.core if other else here.core
                    wires.send(
                        values.at[:, :, here.along(2, step), core],
                        h1.at[mine],
                        here.near(2, step, other),
                        ("v1", step, other),
                    )

    def values_x():
        for step in (0, *steps):
            for other in (0, 1):
                if step or other:
                    core = 1 - here.core if other else here.core
                    wires.arrived(
                        h1.at[here.along(2, -step) * 2 + core],
                        ("v1", step, other),
                        here.near(2, -step, other),
                    )
        h2[here.at[1]] = h1[:, :, here.at[1]]
        for step in steps:
            wires.send(
                h1.at[:, :, here.along(1, step)],
                h2.at[here.at[1]],
                here.near(1, step),
                ("v2", step),
            )

    def values_z():
        for step in steps:
            wires.arrived(h2.at[here.along(1, -step)], ("v2", step), here.near(1, -step))
        h3[here.at[0]] = h2[:, :, here.at[0]]
        for step in steps:
            wires.send(
                h2.at[:, :, here.along(0, step)],
                h3.at[here.at[0]],
                here.near(0, step),
                ("v3", step),
            )

    def router_back():
        for step in steps:
            wires.arrived(h3.at[here.along(0, -step)], ("v3", step), here.near(0, -step))

        def one_expert(e, carry):
            flat[pl.ds(e, 1), :] = h3[e // 32, (e // 8) % 4, e % 8]
            return carry

        lax.fori_loop(0, flat.shape[0], one_expert, 0)
        by_slot = flat[...].T
        dense = jnp.zeros_like(by_slot)
        for j in range(16):
            dense = dense + jnp.where(place[...] == j, by_slot[j : j + 1], 0.0)
        lane = lax.broadcasted_iota(jnp.int32, dense.shape, 1)
        by_token = ids[...].T
        picked = jnp.zeros_like(dense)
        for k in range(ids.shape[0]):
            value = jnp.sum(
                jnp.where(lane == by_token[:, k : k + 1], dense, 0.0), axis=1, keepdims=True
            )
            picked = picked + jnp.where(lane == k, value, 0.0)
        combine_grad[...] = picked.T[: ids.shape[0]]
        inner = jnp.sum(gates[...] * dense, axis=1, keepdims=True)
        prob_grad = jnp.where(place[...] >= 0, (dense - inner) / scale[...], 0.0)
        top = ids.shape[0]
        fraction = dense.shape[1] * counts[...] / (top * tokens * RING * RING)
        prob_grad = prob_grad + aux[0] * fraction
        mean = jnp.sum(probs[...] * prob_grad, axis=1, keepdims=True)
        logit_grad[...] = (probs[...] * (prob_grad - mean)).astype(jnp.bfloat16)

        def one_tile(n, carry):
            columns = pl.ds(pl.multiple_of(n * LANES, LANES), LANES)
            term = lax.dot_general(
                inputs[:, columns],
                logit_grad[...],
                (((0,), (0,)), ((), ())),
                preferred_element_type=jnp.float32,
            )
            for m in range(2):
                for core in range(2):
                    terms[core, n // 8, (n // 2) % 4, 2 * (n % 2) + m] = term[
                        64 * m + 32 * core : 64 * m + 32 * core + 32
                    ]
            return carry

        lax.fori_loop(0, inputs.shape[1] // LANES, one_tile, 0)
        wires.send(terms.at[1 - here.core], other_terms, here.partner(), ("r0",))

    def chip_sum():
        wires.arrived(other_terms, ("r0",), here.partner())

        def one(n, carry):
            z, x = n // RING, n % RING
            terms[here.core, z, x] = terms[here.core, z, x] + other_terms[z, x]
            return carry

        lax.fori_loop(0, RING * RING, one, 0)

    def band_of(q, level, coordinate):
        where = [slice(None)] * 3
        for axis in ORDERS[q][:level]:
            where[axis] = here.at[axis]
        where[ORDERS[q][level]] = coordinate
        return (here.core, *where, pl.ds(*bands[q]), slice(None))

    def sum_send(level):
        for q in range(3):
            axis = ORDERS[q][level]
            for n, step in enumerate(steps):
                wires.send(
                    terms.at[band_of(q, level, here.along(axis, step))],
                    sums[level][q].at[n],
                    here.near(axis, step),
                    ("r", level, q, step),
                )

    def sum_in(level):
        for q in range(3):
            axis = ORDERS[q][level]
            for n, step in enumerate(steps):
                wires.arrived(
                    sums[level][q].at[n], ("r", level, q, step), here.near(axis, -step)
                )
            own = band_of(q, level, here.at[axis])
            landed = sums[level][q]
            terms[own] = terms[own] + landed[0] + landed[1] + landed[2]

    def sum_out():
        for q in range(3):
            span = pl.ds(*bands[q])
            router_grad[span] = terms[here.core, here.at[0], here.at[1], here.at[2], span]

    def stage_copy(p, k, b_step):
        start, size = parts[p]
        b_index = here.along(ORDERS[p][1], b_step)
        slot = (k * 3 + p) % 2
        return pltpu.make_async_copy(
            stage.at[slot, :, :, :, :, pl.ds(0, size)],
            back.at[(*fixed_b(ORDERS[p], b_index), slice(None), slice(None), pl.ds(start, size))],
            bs.at[slot],
        )

    def produce(p, k, b_step):
        start, size = parts[p]
        b_index = here.along(ORDERS[p][1], b_step)
        slot = (k * 3 + p) % 2
        units = grad_first.shape[-1]
        if k == 0:
            fetches[2 * p].wait()
            fetches[2 * p + 1].wait()
        for copy in given_copies(p, k, b_step):
            copy.wait()

        def columns(offset, width):
            span = pl.ds(start + offset, width)
            total = 0.0
            for n, weight in enumerate((gate, up)):
                total = total + lax.dot_general(
                    given[slot, n].reshape(512, units),
                    weight[span],
                    (((1,), (1,)), ((), ())),
                    preferred_element_type=jnp.float32,
                )
            stage[slot, :, :, :, :, pl.ds(offset, width)] = total.astype(jnp.bfloat16).reshape(
                RING, RING, 2, 16, width
            )

        def tile(n, carry):
            columns(pl.multiple_of(n * 256, 256), 256)
            return carry

        lax.fori_loop(0, size // 256, tile, 0)
        if size % 256:
            columns(size // 256 * 256, size % 256)
        stage_copy(p, k, b_step).start()

    def pieces(p, b_index, s_index, c_index):
        start, size = parts[p]
        return slots_of(back, ORDERS[p], b_index, s_index, c_index, start, size)

    def give(p, k, b_step):
        a, b, s = ORDERS[p]
        b_index = here.along(b, b_step)
        mine = rows[p].at[b_index, :, here.at[s] * 2 + here.core]
        way = 1 if k % 2 == 0 else -1
        wires.send(
            pieces(p, b_index, here.along(s, 2), slice(None)),
            relay[p].at[k],
            here.near(s, way),
            (p, "relay", k),
        )
        for step in (1, -1):
            for other in (0, 1):
                core = 1 - here.core if other else here.core
                wires.send(
                    pieces(p, b_index, here.along(s, step), core),
                    mine,
                    here.near(s, step, other),
                    (p, "near", step, other, k),
                )
        wires.send(
            pieces(p, b_index, here.at[s], 1 - here.core), mine, here.partner(), (p, "chip", k)
        )
        copy = pltpu.make_async_copy(
            pieces(p, b_index, here.at[s], here.core), mine, ls.at[len(local)]
        )
        copy.start()
        local.append(copy)

    def forward(p, k, b_step):
        a, b, s = ORDERS[p]
        b_index = here.along(b, b_step)
        way = 1 if k % 2 == 0 else -1
        wires.arrived(relay[p].at[k], (p, "relay", k), here.near(s, -way))
        theirs = rows[p].at[b_index, :, here.along(s, -way) * 2 + here.core]
        for other in (0, 1):
            core = 1 - here.core if other else here.core
            wires.send(
                relay[p].at[k, :, core], theirs, here.near(s, way, other), (p, "far", other, k)
            )

    def gathered(p, k, b_step):
        a, b, s = ORDERS[p]
        b_index = here.along(b, b_step)
        way = 1 if k % 2 == 0 else -1
        for other in (0, 1):
            core = 1 - here.core if other else here.core
            for step in (1, -1):
                wires.arrived(
                    rows[p].at[b_index, :, here.along(s, -step) * 2 + core],
                    (p, "near", step, other, k),
                    here.near(s, -step, other),
                )
            wires.arrived(
                rows[p].at[b_index, :, here.along(s, 2) * 2 + core],
                (p, "far", other, k),
                here.near(s, -way, other),
            )
        wires.arrived(
            rows[p].at[b_index, :, here.at[s] * 2 + (1 - here.core)],
            (p, "chip", k),
            here.partner(),
        )
        local[k * 3 + p].wait()

    def add_up(p, b_step):
        a, b, s = ORDERS[p]
        b_index = here.along(b, b_step)
        size = parts[p][1]

        def one(a_index, carry):
            token_of = lines[p, b_index, a_index, pl.ds(0, 1), :]
            gate_of = lines[p, b_index, a_index, pl.ds(1, 1), :]
            token = lax.broadcasted_iota(jnp.int32, (tokens, LANES), 0).astype(jnp.float32)
            weigh = jnp.where(token == token_of, gate_of, 0.0).astype(jnp.bfloat16)
            total = jnp.dot(
                weigh,
                rows[p][b_index, a_index].reshape(LANES, size),
                preferred_element_type=jnp.float32,
            )
            rows[p][b_index, a_index] = total.astype(jnp.bfloat16).reshape(8, 16, size)
            return carry

        lax.fori_loop(0, RING, one, 0)

    def plus(*terms):
        total = terms[0].astype(jnp.float32)
        for term in terms[1:]:
            total = total + term.astype(jnp.float32)
        return total

    def fold2(p, way, k, step):
        a, b, s = ORDERS[p]
        b_index, a_index = here.along(b, way), here.along(a, step)
        slot = 0 if way == 1 else 1
        groups = pl.ds(0, 4) if way == 1 else pl.ds(4, 4)
        wires.arrived(halves2[p].at[slot, k], (p, "half2", way, k), here.near(b, -way))
        rows[p][b_index, a_index, groups] = plus(
            rows[p][b_index, a_index, groups], halves2[p][slot, k]
        ).astype(jnp.bfloat16)
        wires.send(
            rows[p].at[b_index, a_index],
            whole2[p].at[slot, k],
            here.near(b, way),
            (p, "whole2", way, k),
        )

    def settle2(p, k, step):
        a, b, s = ORDERS[p]
        for way in (1, -1):
            slot = 0 if way == 1 else 1
            wires.arrived(whole2[p].at[slot, k], (p, "whole2", way, k), here.near(b, -way))
        own = rows[p].at[here.at[b], here.along(a, step)]
        return plus(own[...], whole2[p][0, k], whole2[p][1, k])

    order = (2, 1, -1, 0)
    work = [(k, p) for k in range(4) for p in range(3)]

    def make(turn):
        k, p = work[turn]
        if turn + 1 < len(work):
            after_k, after_p = work[turn + 1]
            for copy in given_copies(after_p, after_k, order[after_k]):
                copy.start()
        produce(p, k, order[k])

    def post(turn):
        k, p = work[turn]
        stage_copy(p, k, order[k]).wait()
        give(p, k, order[k])

    def pass_on(k):
        for p in range(3):
            forward(p, k, order[k])

    def total(k):
        for p in range(3):
            gathered(p, k, order[k])
            add_up(p, order[k])

    def halve():
        for p, (a, b, s) in enumerate(ORDERS):
            far = here.along(b, 2)
            for k, step in enumerate(order):
                for way, groups in ((1, pl.ds(0, 4)), (-1, pl.ds(4, 4))):
                    wires.send(
                        rows[p].at[far, here.along(a, step), groups],
                        halves2[p].at[0 if way == 1 else 1, k],
                        here.near(b, way),
                        (p, "half2", way, k),
                    )

    def fold(way):
        for k, step in enumerate(order):
            for p in range(3):
                fold2(p, way, k, step)

    actions = {
        "make": make,
        "post": post,
        "pass": pass_on,
        "total": total,
        "halve": halve,
        "fold": fold,
        "line": values_line,
        "x": values_x,
        "z": values_z,
        "router": router_back,
        "chip": chip_sum,
        "send": sum_send,
        "in": sum_in,
    }
    for name, *given_to in COMBINE_PLAN:
        actions[name](*given_to)
    for p, (a, b, s) in enumerate(ORDERS):
        block = rows[p].at[here.at[b], here.along(a, 2)]
        block[...] = settle2(p, 0, 2).astype(jnp.bfloat16)
        for way, groups in ((1, pl.ds(0, 4)), (-1, pl.ds(4, 4))):
            wires.send(
                rows[p].at[here.at[b], here.along(a, 2), groups],
                halves1[p].at[0 if way == 1 else 1],
                here.near(a, way),
                (p, "half1", way),
            )
    for k, way in ((1, 1), (2, -1)):
        for p, (a, b, s) in enumerate(ORDERS):
            slot = 0 if way == 1 else 1
            groups = pl.ds(0, 4) if way == 1 else pl.ds(4, 4)
            block = rows[p].at[here.at[b], here.along(a, way)]
            block[...] = settle2(p, k, way).astype(jnp.bfloat16)
            wires.arrived(halves1[p].at[slot], (p, "half1", way), here.near(a, -way))
            part = rows[p].at[here.at[b], here.along(a, way), groups]
            part[...] = plus(part[...], halves1[p][slot]).astype(jnp.bfloat16)
            wires.send(block, whole1[p].at[slot], here.near(a, way), (p, "whole1", way))
    for p, (a, b, s) in enumerate(ORDERS):
        start, size = parts[p]
        total = settle2(p, 3, 0)
        for way in (1, -1):
            slot = 0 if way == 1 else 1
            wires.arrived(whole1[p].at[slot], (p, "whole1", way), here.near(a, -way))
        total = plus(total, whole1[p][0], whole1[p][1]).reshape(tokens, size)
        total = total + lax.dot_general(
            logit_grad[...],
            router[pl.ds(start, size)],
            (((1,), (1,)), ((), ())),
            preferred_element_type=jnp.float32,
        )
        out[:, pl.ds(start, size)] = total.astype(out.dtype)
    if ("in", 2) not in COMBINE_PLAN:
        sum_in(2)
    sum_out()
    wires.drain()


def combine(parts, values, grads, weights, lines, counts, inputs, router, probs, gates, place, scale, ids, aux):
    width, units = weights[0].shape
    top, tokens = ids.shape
    experts = probs.shape[1]

    def buffers(*lead):
        return [pltpu.VMEM((*lead, size), jnp.bfloat16) for _, size in parts]

    def floats(*shape):
        return pltpu.VMEM(shape, jnp.float32)

    hbm, vmem = pl.BlockSpec(memory_space=pltpu.HBM), pl.BlockSpec(memory_space=pltpu.VMEM)
    bands = (16, 8, 8)
    return pl.pallas_call(
        functools.partial(combine_kernel, parts),
        out_shape=(
            jax.ShapeDtypeStruct((tokens, width), jnp.bfloat16),
            jax.ShapeDtypeStruct((top, tokens), jnp.float32),
            jax.ShapeDtypeStruct((width // (2 * RING**3), experts), jnp.float32),
            jax.ShapeDtypeStruct((RING, RING, RING, 2, 16, width), jnp.bfloat16),
        ),
        in_specs=[vmem, hbm, hbm, hbm, hbm]
        + [vmem] * 9
        + [pl.BlockSpec(memory_space=pltpu.SMEM)],
        out_specs=(vmem, vmem, vmem, hbm),
        scratch_shapes=buffers(RING, RING, 8, 16)
        + buffers(RING, RING, 2, 16)
        + buffers(2, RING, 4, 16)
        + buffers(2, RING, 8, 16)
        + buffers(2, 4, 16)
        + buffers(2, 8, 16)
        + [
            pltpu.VMEM((width, units), jnp.bfloat16),
            pltpu.VMEM((width, units), jnp.bfloat16),
            pltpu.VMEM((2, RING, RING, 2, 16, parts[0][1]), jnp.bfloat16),
            pltpu.VMEM((2, 2, RING, RING, 2, 16, units), jnp.bfloat16),
            floats(8, RING, RING, 1, LANES),
            floats(RING, 8, RING, 1, LANES),
            floats(RING, RING, 8, 1, LANES),
            floats(experts, LANES),
            pltpu.VMEM((tokens, experts), jnp.bfloat16),
            floats(2, RING, RING, RING, 32, experts),
            floats(RING, RING, RING, 32, experts),
        ]
        + [floats(3, RING, RING, band, experts) for band in bands]
        + [floats(3, RING, band, experts) for band in bands]
        + [floats(3, band, experts) for band in bands]
        + [
            pltpu.SemaphoreType.DMA((224,)),
            pltpu.SemaphoreType.DMA((224,)),
            pltpu.SemaphoreType.DMA((16,)),
            pltpu.SemaphoreType.DMA((12,)),
        ],
        compiler_params=pltpu.CompilerParams(
            collective_id=1, has_side_effects=True, vmem_limit_bytes=67043328
        ),
    )(values, *grads, *weights, lines, counts, inputs, router, probs, gates, place, scale, ids, aux)[:3]


def shards(
    tokens,
    out_grad,
    router_weight,
    gate_weight,
    up_weight,
    down_weight,
    saved_gate,
    saved_up,
    expert_ids,
    aux_weight,
):
    devices = lax.axis_size(AXES)
    inputs, upstream_grad, chosen_ids = tokens[0], out_grad[0], expert_ids[0].T
    model_width = inputs.shape[1]
    parts = column_parts(model_width)

    by_source = (RING, RING, RING, 2, saved_gate.shape[1] // devices, saved_gate.shape[2])
    grad_first, grad_second, values, lines, counts, probs, gates, place, chosen_sum = dispatch(
        parts,
        upstream_grad,
        inputs,
        router_weight,
        chosen_ids,
        down_weight[0],
        saved_gate[0].reshape(by_source),
        saved_up[0].reshape(by_source),
    )
    token_grad, combine_grad, router_grad = combine(
        parts,
        values,
        (grad_first, grad_second),
        (gate_weight[0], up_weight[0]),
        lines,
        counts,
        inputs,
        router_weight,
        probs,
        gates,
        place,
        chosen_sum,
        chosen_ids,
        aux_weight,
    )
    return (token_grad[None], combine_grad.T[None], router_grad)


def solution(mesh):
    torus = Mesh(mesh.devices.reshape(RING, RING, RING, 2), AXES)
    return jax.shard_map(
        shards,
        mesh=torus,
        in_specs=(
            P(EXP, SEQ, None),
            P(EXP, SEQ, None),
            P(),
            P(AXES, None, None),
            P(AXES, None, None),
            P(AXES, None, None),
            P(AXES, None, None),
            P(AXES, None, None),
            P(EXP, SEQ, None),
            P(),
        ),
        out_specs=(P(EXP, SEQ, None), P(EXP, SEQ, None), P(AXES, None)),
        check_vma=False,
    )
```
